32 devices in a mesh: kpt: 2 (over y), row: 4 (over x, core), col: 4 (over z).
Axes of the slice: x: 2, y: 2, z: 4, core: 2. Of those that a mesh axis runs over, the one named last changes fastest.
Arguments:
- left_blocks: bfloat16 [8, 64, 2, 2, 128, 128], P(('kpt', 'row'), 'col'), parts along dimension 0, may hold values from -0.5 to 0.5
- left_rows: int32 [8, 64, 2], P(('kpt', 'row'), 'col'), parts along dimension 0, may hold values from 0 to 7, as said below
- left_count: int32 [8, 64], P(('kpt', 'row'), 'col'), parts along dimension 0, may hold values from 1 to 2, as said below
- left_level: int32 [8, 64, 2], P(('kpt', 'row'), 'col'), parts along dimension 0, may hold values from 0 to 7
- right_blocks: bfloat16 [2, 64, 4, 4, 2, 128, 128], P('kpt', 'row', 'col'), parts along dimension 0, may hold values from -6 to 6
- right_cols: int32 [2, 64, 4, 4], P('kpt', 'row', 'col'), parts along dimension 0, may hold values from 0 to 15, as said below
- right_count: int32 [2, 64, 4], P('kpt', 'row', 'col'), parts along dimension 0, may hold values from 1 to 4, as said below
- right_level: int32 [2, 64, 4, 4], P('kpt', 'row', 'col'), parts along dimension 0, may hold values from 0 to 7
Outputs:
- product_blocks: bfloat16 [64, 64, 2, 128, 128], P(('kpt', 'row'), 'col'), parts along dimension 0
The draws below stay inside these ranges and needn't reach their ends.
There are 2 independent parts, one for each index of `kpt`. The reference program is written for one: setup_inputs(seed, part) draws one part's arguments, and reference() takes and returns one part's arrays. A program takes and returns all parts, laid end to end along the dimension named above; each array names one. Nothing has to cross between parts.
Inputs may be any that keep to these rules, and one draw needn't show every extreme that they name: `left_rows`: the 2 slots of one row group and block column name distinct block rows. `left_count`: in every row group some block column has all 2 slots live. `right_cols`: the 4 slots of one block row and column group name distinct block columns. `right_count`: in every column group some block row has all 4 slots live.
All inputs are finite; a program needn't handle non-finite values.
Results may differ from the reference program's by a relative error of at most 0.001.
Values may be sent and summed in bfloat16 or wider, within the bound.
A program may use at most 256 MiB of HBM per device.

```python
import jax
import jax.numpy as jnp
from jax import lax

BS = 128
GR = 8
LEVEL_CUT = 7
NB = 64
KB = 16
MA = 2
MB = 4
SETS = 1
N_ROW = 4
N_COL = 4


def distinct_slots(key, count, choices, taken):
    keys = jax.random.split(key, count)
    orders = jax.vmap(lambda single: jax.random.permutation(single, choices))(keys)
    return orders[:, :taken].astype(jnp.int32)


def filled_counts(key, groups, length, most):
    base = jax.random.randint(jax.random.fold_in(key, 1), (groups, length), 1, most + 1)
    chosen = jax.random.randint(jax.random.fold_in(key, 2), (groups, 1), 0, length)
    position = jnp.arange(length, dtype=jnp.int32)[None, :]
    return jnp.where(position == chosen, most, base).astype(jnp.int32)


def draw_left_rows(key, part):
    slots = distinct_slots(jax.random.fold_in(key, 101), N_ROW * NB, GR, MA)
    return slots.reshape(N_ROW, NB, MA)


def draw_left_count(key, part):
    return filled_counts(jax.random.fold_in(key, 202), N_ROW, NB, MA)


def draw_right_cols(key, part):
    slots = distinct_slots(jax.random.fold_in(key, 303), NB * N_COL, KB, MB)
    return slots.reshape(N_COL // N_ROW, N_ROW * KB, N_COL, MB)


def draw_right_count(key, part):
    counts = filled_counts(jax.random.fold_in(key, 404), N_COL, NB, MB)
    return counts.T.reshape(N_COL // N_ROW, N_ROW * KB, N_COL)


def set_ends(array, key, low, top_value):
    longest = array.shape.index(max(array.shape))
    spots = []
    for shift in (0, 1):
        where = [jax.random.randint(jax.random.fold_in(key, axis), (), 0, length) for axis, length in enumerate(array.shape)]
        where[longest] = (where[longest] + shift) % array.shape[longest]
        spots.append(tuple(where))
    return array.at[spots[0]].set(low).at[spots[1]].set(top_value)


def shard_levels(rng, dims, cuts, least, high):
    factor_of, own = 1.0, jax.random.fold_in(rng, 6)
    for axis_at, parts in cuts:
        steps = jnp.exp(jax.random.uniform(jax.random.fold_in(own, axis_at), (parts,), jnp.float32, least / len(cuts), high / len(cuts)))
        factor_of = factor_of * jnp.repeat(steps, dims[axis_at] // parts).reshape([-1 if axis == axis_at else 1 for axis in range(len(dims))])
    return factor_of


def gaussian(rng, shape, width, limit, pieces=(), kind=jnp.bfloat16):
    values = jax.random.normal(rng, shape, jnp.float32) * width
    if len(pieces) > 0:
        values = shard_levels(rng, shape, pieces, -0.22, 0.18) * values
    return jnp.clip(values, min=-limit, max=limit).astype(kind)


def setup_inputs(seed: int = 0, part: int = 0) -> dict:
    key_list = jax.random.split(jax.random.key(seed), 9)
    own_keys = jax.random.split(jax.random.fold_in(key_list[8], part), 9)
    left_blocks = gaussian(own_keys[0], (N_ROW, NB, MA, 2, BS, BS), BS ** -0.5, 0.5, ((0, 4), (1, 4)))
    left_rows = draw_left_rows(jax.random.fold_in(jax.random.fold_in(key_list[8], part), 71), part)
    left_count = draw_left_count(jax.random.fold_in(jax.random.fold_in(key_list[8], part), 71), part)
    left_level = set_ends(jax.random.randint(own_keys[3], (N_ROW, NB, MA), 0, 8), jax.random.fold_in(own_keys[3], 1), 0, 7).astype(jnp.int32)
    right_blocks = gaussian(own_keys[4], (SETS, N_ROW * KB, N_COL, MB, 2, BS, BS), 1.0, 6.0, ((1, 4), (2, 4)))
    right_cols = draw_right_cols(jax.random.fold_in(jax.random.fold_in(key_list[8], part), 71), part)
    right_count = draw_right_count(jax.random.fold_in(jax.random.fold_in(key_list[8], part), 71), part)
    right_level = set_ends(jax.random.randint(own_keys[7], (SETS, N_ROW * KB, N_COL, MB), 0, 8), jax.random.fold_in(own_keys[7], 1), 0, 7).astype(jnp.int32)
    return dict(left_blocks=left_blocks, left_rows=left_rows, left_count=left_count, left_level=left_level, right_blocks=right_blocks, right_cols=right_cols, right_count=right_count, right_level=right_level)


def reference(left_blocks, left_rows, left_count, left_level, right_blocks, right_cols, right_count, right_level):
    right_flat = right_blocks.reshape(NB, N_COL, MB, 2, BS, BS)
    cols_flat = right_cols.reshape(NB, N_COL, MB)
    count_flat = right_count.reshape(NB, N_COL)
    level_flat = right_level.reshape(NB, N_COL, MB)
    slot_left = jnp.arange(MA, dtype=jnp.int32)
    slot_right = jnp.arange(MB, dtype=jnp.int32)
    group_base = (jnp.arange(N_ROW, dtype=jnp.int32) * GR)[:, None, None, None]
    panel_base = (jnp.arange(N_COL, dtype=jnp.int32) * KB)[None, None, :, None]

    def one_column(total, column):
        blocks_a, rows_a, count_a, level_a, blocks_b, cols_b, count_b, level_b = column
        live_a = slot_left[None, :] < count_a.astype(jnp.int32)[:, None]
        live_b = slot_right[None, :] < count_b.astype(jnp.int32)[:, None]
        kept = live_a[:, :, None, None] & live_b[None, None, :, :]
        kept = kept & (level_a.astype(jnp.int32)[:, :, None, None] + level_b.astype(jnp.int32)[None, None, :, :] >= LEVEL_CUT)
        terms = jnp.einsum("pmcij,qndjl->pmqncdil", blocks_a.astype(jnp.float32), blocks_b.astype(jnp.float32),
                           precision=lax.Precision.HIGHEST)
        real_part = terms[:, :, :, :, 0, 0] - terms[:, :, :, :, 1, 1]
        imag_part = terms[:, :, :, :, 0, 1] + terms[:, :, :, :, 1, 0]
        product = jnp.stack([real_part, imag_part], axis=4) * kept[..., None, None, None].astype(jnp.float32)
        row_index = group_base + rows_a.astype(jnp.int32)[:, :, None, None]
        col_index = panel_base + cols_b.astype(jnp.int32)[None, None, :, :]
        row_index = jnp.broadcast_to(row_index, kept.shape).reshape(-1)
        col_index = jnp.broadcast_to(col_index, kept.shape).reshape(-1)
        total = total.at[row_index, col_index].add(product.reshape(-1, 2, BS, BS))
        return total, None

    columns = (jnp.moveaxis(left_blocks, 1, 0), jnp.moveaxis(left_rows, 1, 0), jnp.moveaxis(left_count, 1, 0),
               jnp.moveaxis(left_level, 1, 0), right_flat, cols_flat, count_flat, level_flat)
    total = jnp.zeros((N_ROW * GR, NB, 2, BS, BS), jnp.float32)
    total, unused = lax.scan(one_column, total, columns)
    return total.astype(jnp.bfloat16)
```

```python
import functools

import jax
import jax.numpy as jnp
from jax import lax
from jax.experimental import pallas as pl
from jax.experimental.pallas import tpu as pltpu
from jax.sharding import PartitionSpec as P

GR = 8
LEVEL_CUT = 7
DEAD = -1000
GROUP = 4
MAIN_CUTS = 2
RIGHT_CUTS = 8
VMEM_BYTES = 62 * 1024 * 1024
MESH = pl.DeviceIdType.MESH
ROW_LEFT, ROW_MAX, ROW_TARGET, ROW_COLS, ROW_RIGHT = 0, 1, 3, 4, 5


def variants(slots):
    main = slots * 22 // 32
    found = []
    for size in range(main, slots, max(1, slots // 16)):
        found.append((size, 0, slots))
    found.append((slots, 0, slots))
    return found


def plan_kernel(
    sizes, options, tile, left_meta, right_meta, table, choice, tiles, send, recv,
):
    n_kpt, n_row, n_col, sets, per, ma, mb = sizes
    slots = per * ma
    kpt, row, col = (lax.axis_index(name) for name in ("kpt", "row", "col"))
    total = n_kpt * n_row * n_col
    me = (kpt * n_row + row) * n_col + col

    def place_of(step):
        other = (me + step) % total
        return {
            "kpt": other // (n_row * n_col), "row": (other // n_col) % n_row, "col": other % n_col
        }

    def copy_of(step):
        return pltpu.make_async_remote_copy(
            src_ref=tile, dst_ref=tiles.at[me], send_sem=send.at[step], recv_sem=recv.at[step],
            device_id=place_of(step), device_id_type=MESH,
        )

    barrier = pltpu.get_barrier_semaphore()

    @pl.loop(1, total)
    def _(step):
        pl.semaphore_signal(barrier, inc=1, device_id=place_of(step), device_id_type=MESH)

    tiles[me] = tile[...]
    pl.semaphore_wait(barrier, total - 1)

    @pl.loop(1, total)
    def _(step):
        copy_of(step).start()

    @pl.loop(1, total)
    def _(step):
        copy_of(step).wait_recv()

    def at_device(k, r, c):
        return (k * n_row + r) * n_col + c

    for c in range(n_col):
        left_meta[c] = tiles[at_device(kpt, row, c)]
    for r in range(n_row):
        right_meta[r] = tiles[at_device(kpt, r, col)]

    def right_max(k, panel, q):
        return tiles[at_device(k, panel % n_row, q), pl.ds(ROW_MAX + panel // n_row, 1), :]

    def count_needed(levels, most):
        return jnp.sum(
            jnp.where(levels + most >= LEVEL_CUT, 1.0, 0.0), axis=1, keepdims=True
        )

    main = options[0][0]

    def measure_part(k, carry):
        most_end, most_mid = carry
        for panel in range(n_col):
            levels = jnp.concatenate(
                [tiles[at_device(k, r, panel), pl.ds(ROW_LEFT, 1), :] for r in range(n_row)],
                axis=0,
            )
            rights = [right_max(k, panel, q) for q in range(n_col)]
            if panel > 0:
                most_end = jnp.maximum(most_end, count_needed(levels, rights[0]))
            if panel < n_col - 1:
                most_end = jnp.maximum(most_end, count_needed(levels, rights[-1]))
            if panel > 1:
                most_mid = jnp.maximum(
                    most_mid, count_needed(levels, functools.reduce(jnp.maximum, rights[:panel]))
                )
            if panel < n_col - 2:
                most_mid = jnp.maximum(
                    most_mid,
                    count_needed(levels, functools.reduce(jnp.maximum, rights[panel + 1:])),
                )
        return most_end, most_mid

    zero = jnp.zeros((n_row, 1), jnp.float32)
    most_end, most_mid = lax.fori_loop(0, n_kpt, measure_part, (zero, zero))
    index = jnp.zeros((n_row, 1), jnp.float32)
    for size, _, middle in options[:-1]:
        index = index + jnp.where((most_end > size) | (most_mid > middle), 1.0, 0.0)
    choice[0] = jnp.max(index).astype(jnp.int32)

    lane = lax.broadcasted_iota(jnp.int32, (128, 128), 1)
    line = lax.broadcasted_iota(jnp.int32, (128, 128), 0)
    lane_row = lane[:1].astype(jnp.float32)

    def ranks(panel, up):
        levels = tiles[at_device(kpt, row, panel), pl.ds(ROW_LEFT, 1), :]
        end = right_max(kpt, panel, n_col - 1 if up else 0)
        union = jnp.full((1, 128), DEAD, jnp.int32)
        for q in range(n_col):
            beyond = q > panel if up else q < panel
            union = jnp.maximum(union, jnp.where(beyond, right_max(kpt, panel, q), DEAD))
        kind = jnp.where(
            levels + end >= LEVEL_CUT, 0.0, jnp.where(levels + union >= LEVEL_CUT, 1.0, 2.0)
        )
        key = jnp.where(lane_row < slots, kind, 3.0) * 128.0 + lane_row
        key_row = jnp.broadcast_to(key, (128, 128))
        key_line = jnp.sum(jnp.where(lane == line, key_row, 0.0), axis=1, keepdims=True)
        before = jnp.where(key_line < key_row, 1.0, 0.0)
        rank_row = jnp.sum(before, axis=0, keepdims=True)
        after = jnp.where(key_row < key_line, 1.0, 0.0)
        rank_line = jnp.sum(after, axis=1, keepdims=True)
        return rank_row, rank_line

    def write(at, values):
        table[pl.ds(at, 1), :] = values.astype(jnp.int32)

    for panel in range(n_col):
        rank_down = ranks(panel, False)[0] if panel > 0 else lane_row
        rank_up = ranks(panel, True)[0] if panel < n_col - 1 else lane_row
        place = jnp.where(panel > col, rank_down, jnp.where(panel < col, rank_up, lane_row))
        write(panel, place + panel * slots)
    for at, up in ((n_col, False), (n_col + 1, True)):
        rank_line = ranks(col, up)[1]
        hit = jnp.where(rank_line == lane.astype(jnp.float32), line.astype(jnp.float32), 0.0)
        write(at, jnp.sum(hit, axis=0, keepdims=True))

    @pl.loop(1, total)
    def _(step):
        copy_of(step).wait_send()


def gather_kernel(
    n_row, n_col, option, left, right, table,
    left_all, right_all,
    own_left, packed_down, packed_up,
    up_send, up_recv, down_send, down_recv,
    x_send, x_recv, own_send, own_recv, pass_send, pass_recv,
    stage_sem, left_sem, right_sem,
):
    row = lax.axis_index("row")
    col = lax.axis_index("col")
    n_chip = n_row // 2
    chip, core = row // 2, row % 2
    partner = chip * 2 + 1 - core
    slots = left.shape[0]
    main, _, middle = option

    staged = pltpu.make_async_copy(left, own_left, stage_sem)
    staged.start()
    barrier = pltpu.get_barrier_semaphore()
    for step in range(1, n_row):
        pl.semaphore_signal(
            barrier, inc=1, device_id={"row": (row + step) % n_row}, device_id_type=MESH
        )
    for step in (1, n_col - 1):
        pl.semaphore_signal(
            barrier, inc=1, device_id={"col": (col + step) % n_col}, device_id_type=MESH
        )

    bounds = [main * at // MAIN_CUTS for at in range(MAIN_CUTS + 1)]
    cuts = [(low, high, False) for low, high in zip(bounds, bounds[1:])]
    if middle > main:
        cuts.append((main, middle, True))
    right_size = right.shape[1] // RIGHT_CUTS

    def left_copy(step, cut, up):
        low, high, _ = cuts[cut]
        panel = col - step if up else col + step
        source = (
            (packed_up if up else packed_down).at[pl.ds(low, high - low)]
            if step == 0 else left_all.at[panel, pl.ds(low, high - low)]
        )
        send, recv = (up_send, up_recv) if up else (down_send, down_recv)
        return pltpu.make_async_remote_copy(
            src_ref=source, dst_ref=left_all.at[panel, pl.ds(low, high - low)],
            send_sem=send.at[step, cut], recv_sem=recv.at[step, cut],
            device_id={"col": col + 1 if up else col - 1}, device_id_type=MESH,
        )

    def left_sends(step, cut, up):
        mid = cuts[cut][2]
        if up:
            return (col + 1 < n_col - (1 if mid else 0)) & (col - step >= 0)
        return (col - 1 >= (1 if mid else 0)) & (col + step < n_col)

    def left_receives(step, cut, up):
        mid = cuts[cut][2]
        if up:
            return (col - 1 - step >= 0) & (col < n_col - (1 if mid else 0))
        return (col + 1 + step < n_col) & (col >= (1 if mid else 0))

    def across(step, cut):
        span = pl.ds(cut * right_size, right_size)
        other = ((chip + step) % n_chip) * 2 + core
        return pltpu.make_async_remote_copy(
            src_ref=right.at[:, span], dst_ref=right_all.at[:, row, span],
            send_sem=x_send.at[step - 1, cut], recv_sem=x_recv.at[step - 1, cut],
            device_id={"row": other}, device_id_type=MESH,
        )

    def passed(step, cut):
        span = pl.ds(cut * right_size, right_size)
        panel = ((chip + n_chip - step) % n_chip) * 2 + core
        return pltpu.make_async_remote_copy(
            src_ref=right_all.at[:, panel, span], dst_ref=right_all.at[:, panel, span],
            send_sem=pass_send.at[step - 1, cut], recv_sem=pass_recv.at[step - 1, cut],
            device_id={"row": partner}, device_id_type=MESH,
        )

    own = pltpu.make_async_remote_copy(
        src_ref=right, dst_ref=right_all.at[:, row],
        send_sem=own_send, recv_sem=own_recv,
        device_id={"row": partner}, device_id_type=MESH,
    )
    kept = (
        pltpu.make_async_copy(left, left_all.at[col], left_sem),
        pltpu.make_async_copy(right, right_all.at[:, row], right_sem),
    )

    staged.wait()

    @pl.loop(0, middle)
    def _(at):
        packed_down[at] = own_left[table[n_col, at]]
        packed_up[at] = own_left[table[n_col + 1, at]]

    pl.semaphore_wait(barrier, n_row + 1)
    for cut in range(len(cuts)):
        for up in (True, False):
            pl.when(left_sends(0, cut, up))(left_copy(0, cut, up).start)
    for step in range(1, n_chip):
        for cut in range(RIGHT_CUTS):
            across(step, cut).start()
    own.start()
    for copy in kept:
        copy.start()

    def take_left(step, cut):
        for up in (True, False):
            pl.when(left_receives(step, cut, up))(left_copy(step, cut, up).wait_recv)
            if step + 1 < n_col - 1:
                pl.when(left_sends(step + 1, cut, up))(left_copy(step + 1, cut, up).start)

    def take_right(step, cut):
        across(step, cut).wait_recv()
        passed(step, cut).start()

    left_jobs = [
        (step * middle + cuts[cut][1], functools.partial(take_left, step, cut))
        for step in range(n_col - 1) for cut in range(len(cuts))
    ]
    right_jobs = [
        (((step - 1) * RIGHT_CUTS + cut + 1) * right.shape[0] * right_size + 0.5,
         functools.partial(take_right, step, cut))
        for step in range(1, n_chip) for cut in range(RIGHT_CUTS)
    ]
    for _, job in sorted(left_jobs + right_jobs, key=lambda entry: entry[0]):
        job()

    own.wait()
    for copy in kept:
        copy.wait()
    for step in range(1, n_chip):
        for cut in range(RIGHT_CUTS):
            across(step, cut).wait_send()
            passed(step, cut).wait()
    for step in range(n_col - 1):
        for cut in range(len(cuts)):
            for up in (True, False):
                pl.when(left_sends(step, cut, up))(left_copy(step, cut, up).wait_send)


def product_kernel(
    sizes, left, right, left_meta, right_meta, table, out, total, stage, pairs, touched, out_sem,
):
    n_row, n_col, sets, per, ma, mb, kb_cols = sizes
    blocks = GR * kb_cols

    @pl.loop(0, blocks + 1)
    def _(block):
        touched[block] = 0

    count = jnp.int32(0)
    for panel in range(n_col):
        which, at = panel // n_row, panel % n_row

        def gather(k, count):
            rights = []
            for n in range(mb):
                spot = (which * per + k) * mb + n
                rights.append((right_meta[at, ROW_COLS, spot], right_meta[at, ROW_RIGHT, spot]))
            slot = panel * per + k
            for m in range(ma):
                spot = k * ma + m
                target = left_meta[panel, ROW_TARGET, spot] * kb_cols
                level = left_meta[panel, ROW_LEFT, spot]
                code = table[panel, spot] * 1024 + slot * mb
                for n in range(mb):
                    pairs[count] = (code + n) * 1024 + target + rights[n][0]
                    count = count + jnp.where(level + rights[n][1] >= LEVEL_CUT, 1, 0)
            return count

        count = lax.fori_loop(0, per, gather, count, unroll=4)
    for extra in range(GROUP):
        pairs[count + extra] = blocks

    @pl.loop(0, (count + GROUP - 1) // GROUP)
    def _(group):
        done = []
        for lane in range(GROUP):
            code = pairs[group * GROUP + lane]
            target = code & 1023
            block = left[code >> 20]
            width = block.shape[1]
            wide = jnp.concatenate([block[:width], block[width:]], axis=1)
            other = right[(code >> 10) & 1023]
            real, imag = other[:width], other[width:]
            matrix = jnp.concatenate(
                [jnp.concatenate([real, imag], axis=1), jnp.concatenate([-imag, real], axis=1)],
                axis=0,
            )
            done.append((target, jnp.dot(wide, matrix, preferred_element_type=jnp.float32)))
        for target, product in done:
            old = touched[target] > 0
            total[target] = jnp.where(old, total[target], 0.0) + product
            touched[target] = 1

    def out_copy(line):
        span = pl.ds(line * kb_cols, kb_cols)
        return pltpu.make_async_copy(stage.at[span], out.at[span], out_sem.at[line])

    @pl.loop(0, GR)
    def _(line):
        @pl.loop(0, kb_cols, unroll=4)
        def _(k):
            block = line * kb_cols + k
            value = jnp.where(touched[block] > 0, total[block], 0.0).astype(stage.dtype)
            width = value.shape[0]
            stage[block, :width] = value[:, :width]
            stage[block, width:] = value[:, width:]

        out_copy(line).start()

    @pl.loop(0, GR)
    def _(line):
        out_copy(line).wait()


def body(
    n_kpt, n_row, n_col, left_blocks, left_rows, left_count, left_level,
    right_blocks, right_cols, right_count, right_level,
):
    _, per, ma, _, width, _ = left_blocks.shape
    sets, right_per, _, mb = right_blocks.shape[:4]
    assert right_per == per and sets * n_row == n_col and n_row % 2 == 0 and sets <= 2
    assert per * ma <= 128 and sets * per * mb <= 128
    slots = per * ma
    left = left_blocks.reshape(slots, 2 * width, width)
    right = right_blocks.reshape(sets, per * mb, 2 * width, width)

    def line(array):
        flat = array.reshape(1, -1)
        return jnp.pad(flat, ((0, 0), (0, 128 - flat.shape[1])), constant_values=DEAD)

    left_levels = jnp.where(
        jnp.arange(ma, dtype=jnp.int32) < left_count[..., None], left_level, DEAD
    )
    right_levels = jnp.where(
        jnp.arange(mb, dtype=jnp.int32) < right_count[..., None], right_level, DEAD
    ).reshape(sets, per, mb)
    most = jnp.repeat(jnp.max(right_levels, axis=2), ma, axis=1)
    lines = [line(left_levels)]
    lines += [line(most[at % sets]) for at in range(2)]
    lines += [line(left_rows), line(right_cols), line(right_levels)]
    tile = jnp.concatenate(lines + [lines[0]] * 2, axis=0)

    any_space = pl.BlockSpec(memory_space=pl.ANY)
    vmem = pl.BlockSpec(memory_space=pltpu.VMEM)
    smem = pl.BlockSpec(memory_space=pltpu.SMEM)
    dma = pltpu.SemaphoreType.DMA
    n_chip = n_row // 2
    total = n_kpt * n_row * n_col
    options = variants(slots)
    table_rows = -(-(n_col + 4) // 8) * 8
    left_meta, right_meta, table, choice = pl.pallas_call(
        functools.partial(plan_kernel, (n_kpt, n_row, n_col, sets, per, ma, mb), options),
        out_shape=(
            jax.ShapeDtypeStruct((n_col, 8, 128), jnp.int32),
            jax.ShapeDtypeStruct((n_row, 8, 128), jnp.int32),
            jax.ShapeDtypeStruct((table_rows, 128), jnp.int32),
            jax.ShapeDtypeStruct((1,), jnp.int32),
        ),
        in_specs=[vmem],
        out_specs=(vmem, vmem, vmem, smem),
        scratch_shapes=[pltpu.VMEM((total, 8, 128), jnp.int32), dma((total,)), dma((total,))],
        compiler_params=pltpu.CompilerParams(collective_id=0, has_side_effects=True),
        name="plan",
    )(tile)

    kb_cols = n_row * sets * per // n_col
    blocks = GR * kb_cols
    left_shape = (n_col,) + left.shape
    right_shape = (sets, n_row) + right.shape[1:]
    limit = VMEM_BYTES - (n_col * left.size + n_row * right.size) * left.dtype.itemsize

    def run(at, left, right, left_meta, right_meta, table):
        cuts = MAIN_CUTS + 1
        left_all, right_all = pl.pallas_call(
            functools.partial(gather_kernel, n_row, n_col, options[at]),
            out_shape=(
                pltpu.VMEM(left_shape, left.dtype),
                pltpu.VMEM(right_shape, right.dtype),
            ),
            in_specs=[any_space, any_space, smem],
            out_specs=(vmem, vmem),
            scratch_shapes=[
                *[pltpu.VMEM(left.shape, left.dtype)] * 3,
                *[dma((n_col - 1, cuts))] * 4,
                *[dma((n_chip - 1, RIGHT_CUTS))] * 2,
                *[dma] * 2,
                *[dma((n_chip - 1, RIGHT_CUTS))] * 2,
                *[dma] * 3,
            ],
            compiler_params=pltpu.CompilerParams(
                collective_id=1 + at, has_side_effects=True, vmem_limit_bytes=limit
            ),
            name=f"gather_panels_{at}",
        )(left, right, table)
        return pl.pallas_call(
            functools.partial(product_kernel, (n_row, n_col, sets, per, ma, mb, kb_cols)),
            out_shape=jax.ShapeDtypeStruct((blocks, 2 * width, width), jnp.bfloat16),
            in_specs=[vmem] * 2 + [smem] * 3,
            out_specs=any_space,
            scratch_shapes=[
                pltpu.VMEM((blocks + 1, width, 2 * width), jnp.float32),
                pltpu.VMEM((blocks, 2 * width, width), jnp.bfloat16),
                pltpu.SMEM((n_col * per * ma * mb + GROUP,), jnp.int32),
                pltpu.SMEM((blocks + 1,), jnp.int32),
                dma((GR,)),
            ],
            compiler_params=pltpu.CompilerParams(vmem_limit_bytes=limit),
            name="pair_products",
        )(
            pltpu.with_memory_space_constraint(
                left_all.reshape((-1,) + left.shape[1:]), pltpu.VMEM
            ),
            pltpu.with_memory_space_constraint(
                right_all.reshape((-1,) + right.shape[2:]), pltpu.VMEM
            ),
            left_meta, right_meta, table,
        )

    out = lax.switch(
        choice[0], [functools.partial(run, at) for at in range(len(options))],
        left, right, left_meta, right_meta, table,
    )
    return out.reshape(GR, kb_cols, 2, width, width)


def solution(mesh):
    in_specs = (
        P(("kpt", "row"), "col", None, None, None, None),
        P(("kpt", "row"), "col", None),
        P(("kpt", "row"), "col"),
        P(("kpt", "row"), "col", None),
        P("kpt", "row", "col", None, None, None, None),
        P("kpt", "row", "col", None),
        P("kpt", "row", "col"),
        P("kpt", "row", "col", None),
    )
    out_specs = P(("kpt", "row"), "col", None, None, None)
    return jax.shard_map(
        functools.partial(body, mesh.shape["kpt"], mesh.shape["row"], mesh.shape["col"]),
        mesh=mesh, in_specs=in_specs, out_specs=out_specs, check_vma=False,
    )
```

```python
import functools

import jax
import jax.numpy as jnp
from jax import lax
from jax.experimental import pallas as pl
from jax.experimental.pallas import tpu as pltpu
from jax.sharding import PartitionSpec as P

GR = 8
LEVEL_CUT = 7
DEAD = -1000
GROUP = 4
MAIN_CUTS = 2
RIGHT_CUTS = 8
VMEM_BYTES = 62 * 1024 * 1024
MESH = pl.DeviceIdType.MESH
FAR = 2.0 ** 17


def variants(slots):
    main = slots * 22 // 32
    found = []
    for size in range(main, slots, max(1, slots // 16)):
        found.append((size, 0, slots))
    found.append((slots, 0, slots))
    return found


def ordered(levels, end, union, slots, lane_row):
    ma, per = levels.shape[0], slots // levels.shape[0]
    rows, columns = [], []
    lane = lax.broadcasted_iota(jnp.int32, (per, 128), 1)
    line = lax.broadcasted_iota(jnp.int32, (per, 128), 0)
    for m in range(ma):
        kind = jnp.where(
            levels[m:m + 1] + end >= LEVEL_CUT, 0.0,
            jnp.where(levels[m:m + 1] + union >= LEVEL_CUT, 1.0, 2.0),
        )
        key = jnp.where(lane_row < per, kind * 128.0 + lane_row * ma + m, 1024.0)
        rows.append(key)
        columns.append(jnp.sum(
            jnp.where(lane == line, jnp.broadcast_to(key, (per, 128)), 0.0), axis=1, keepdims=True
        ))
    return rows, columns


def plan_kernel(
    sizes, options, left_level, left_rows, left_count, right_level, right_cols, right_count,
    meta, tiles, perm, choice, tile, send, recv,
):
    n_kpt, n_row, n_col, sets, per, ma, mb = sizes
    slots = per * ma
    kpt, row, col = (lax.axis_index(name) for name in ("kpt", "row", "col"))
    total = n_kpt * n_row * n_col
    me = (kpt * n_row + row) * n_col + col

    def place_of(step):
        other = (me + step) % total
        return {
            "kpt": other // (n_row * n_col), "row": (other // n_col) % n_row, "col": other % n_col
        }

    def copy_of(step):
        return pltpu.make_async_remote_copy(
            src_ref=tile, dst_ref=tiles.at[me], send_sem=send.at[step], recv_sem=recv.at[step],
            device_id=place_of(step), device_id_type=MESH,
        )

    barrier = pltpu.get_barrier_semaphore()

    @pl.loop(1, total)
    def _(step):
        pl.semaphore_signal(barrier, inc=1, device_id=place_of(step), device_id_type=MESH)

    tile[...] = jnp.full(tile.shape, DEAD, jnp.int32)
    live = lax.broadcasted_iota(jnp.int32, (ma, per), 0) < left_count[...]
    levels = jnp.where(live, left_level[...], DEAD)
    tile[:ma, :per] = levels
    rights = []
    for which in range(sets):
        live = lax.broadcasted_iota(jnp.int32, (mb, per), 0) < right_count[which]
        rights.append(jnp.where(live, right_level[which], DEAD))
        tile[ma + which:ma + which + 1, :per] = jnp.max(rights[-1], axis=0, keepdims=True)
    tiles[me] = tile[...]
    pl.semaphore_wait(barrier, total - 1)

    @pl.loop(1, total)
    def _(step):
        copy_of(step).start()

    meta[...] = jnp.full(meta.shape, DEAD, jnp.int32)
    meta[:ma, :per] = levels
    meta[ma:2 * ma, :per] = left_rows[...]
    for which in range(sets):
        base = 2 * ma + which * 2 * mb
        meta[base:base + mb, :per] = right_cols[which]
        meta[base + mb:base + 2 * mb, :per] = rights[which]

    @pl.loop(1, total)
    def _(step):
        copy_of(step).wait_recv()

    def at_device(k, r, c):
        return (k * n_row + r) * n_col + c

    def right_max(k, panel, q):
        return tiles[at_device(k, panel % n_row, q), pl.ds(ma + panel // n_row, 1), :]

    def measure_part(k, carry):
        most_end, most_mid = carry
        for panel in range(n_col):
            levels = [
                jnp.concatenate(
                    [tiles[at_device(k, r, panel), pl.ds(m, 1), :] for r in range(n_row)], axis=0
                )
                for m in range(ma)
            ]

            def needed(most):
                hits = [jnp.where(level + most >= LEVEL_CUT, 1.0, 0.0) for level in levels]
                return jnp.sum(functools.reduce(jnp.add, hits), axis=1, keepdims=True)

            rights = [right_max(k, panel, q) for q in range(n_col)]
            if panel > 0:
                most_end = jnp.maximum(most_end, needed(rights[0]))
            if panel < n_col - 1:
                most_end = jnp.maximum(most_end, needed(rights[-1]))
            if panel > 1:
                union = functools.reduce(jnp.maximum, rights[:panel])
                most_mid = jnp.maximum(most_mid, needed(union))
            if panel < n_col - 2:
                union = functools.reduce(jnp.maximum, rights[panel + 1:])
                most_mid = jnp.maximum(most_mid, needed(union))
        return most_end, most_mid

    zero = jnp.zeros((n_row, 1), jnp.float32)
    most_end, most_mid = lax.fori_loop(0, n_kpt, measure_part, (zero, zero))
    index = jnp.zeros((n_row, 1), jnp.float32)
    for size, _, middle in options[:-1]:
        index = index + jnp.where((most_end > size) | (most_mid > middle), 1.0, 0.0)
    choice[0] = jnp.max(index).astype(jnp.int32)

    lane_row = lax.broadcasted_iota(jnp.int32, (1, 128), 1).astype(jnp.float32)
    line = lax.broadcasted_iota(jnp.int32, (per, 128), 0).astype(jnp.float32)
    mine = tiles[me, :ma, :]
    for at, up in enumerate((False, True)):
        which = ma + col // n_row
        near = [
            tiles[at_device(kpt, col % n_row, q), pl.ds(which, 1), :] for q in range(n_col)
        ]
        union = jnp.full((1, 128), DEAD, jnp.int32)
        for q in range(n_col):
            beyond = q > col if up else q < col
            union = jnp.maximum(union, jnp.where(beyond, near[q], DEAD))
        rows, columns = ordered(mine, near[-1] if up else near[0], union, slots, lane_row)
        found = jnp.zeros((1, 128), jnp.float32)
        for m in range(ma):
            before = [jnp.where(key < columns[m], 1.0, 0.0) for key in rows]
            rank = jnp.sum(functools.reduce(jnp.add, before), axis=1, keepdims=True)
            hit = jnp.where(rank == lane_row, line * ma + m, 0.0)
            found = found + jnp.sum(hit, axis=0, keepdims=True)
        perm[pl.ds(at, 1), :] = found.astype(jnp.int32)

    @pl.loop(1, total)
    def _(step):
        copy_of(step).wait_send()


def order_pairs(sizes, kpt, col, tiles, left_meta, right_meta, order):
    n_row, n_col, sets, per, ma, mb, kb_cols = sizes
    slots, high = per * ma, n_col * per
    blocks = GR * kb_cols
    lane_row = lax.broadcasted_iota(jnp.int32, (1, 128), 1).astype(jnp.float32)

    def right_max(panel, q):
        at = (kpt * n_row + panel % n_row) * n_col + q
        return tiles[at, pl.ds(ma + panel // n_row, 1), :]

    lefts = jnp.zeros((2 * ma, 128), jnp.float32)
    rights = jnp.zeros((2 * mb, 128), jnp.float32)
    places = jnp.zeros((8, 128), jnp.float32)
    for panel in range(n_col):
        levels = left_meta[panel, :ma, :]
        down, up = panel > col, panel < col
        end = jnp.where(down, right_max(panel, 0), right_max(panel, n_col - 1))
        union = jnp.full((1, 128), DEAD, jnp.int32)
        for q in range(n_col):
            beyond = down if q < panel else up
            if q != panel:
                union = jnp.maximum(union, jnp.where(beyond, right_max(panel, q), DEAD))
        rows, columns = ordered(levels, end, union, slots, lane_row)
        found = []
        for m in range(ma):
            before = [jnp.where(key < rows[m], 1.0, 0.0) for key in columns]
            rank = jnp.sum(functools.reduce(jnp.add, before), axis=0, keepdims=True)
            found.append(jnp.where(down | up, rank, lane_row * ma + m) + panel * slots)
        found = jnp.concatenate(found + [jnp.zeros((8 - ma, 128), jnp.float32)], axis=0)
        base = 2 * ma + panel // n_row * 2 * mb
        here = (lane_row >= panel * per) & (lane_row < (panel + 1) * per)

        def moved(values):
            values = pltpu.roll(values, panel * per, 1) if panel else values
            return jnp.where(here, values, 0.0)

        lefts = lefts + moved(left_meta[panel, :2 * ma, :].astype(jnp.float32))
        right = right_meta[panel % n_row, base:base + 2 * mb, :].astype(jnp.float32)
        rights = rights + moved(right)
        places = places + moved(found)

    lane = lax.broadcasted_iota(jnp.int32, (high, 128), 1)
    line = lax.broadcasted_iota(jnp.int32, (high, 128), 0)

    def column(values):
        wide = jnp.broadcast_to(values, (high, 128))
        return jnp.sum(jnp.where(lane == line, wide, 0.0), axis=1, keepdims=True)

    keys, key_columns, code_columns, target_columns = [], [], [], []
    for m in range(ma):
        for n in range(mb):
            kept = lefts[m:m + 1] + rights[mb + n:mb + n + 1] >= LEVEL_CUT
            target = lefts[ma + m:ma + m + 1] * kb_cols + rights[n:n + 1]
            spot = lane_row + (m * mb + n) * 128.0
            key = jnp.where(kept, target * 1024.0 + spot, FAR + spot)
            keys.append(jnp.where(lane_row < high, key, 2 * FAR))
            key_columns.append(column(keys[-1]))
            code_columns.append(column(places[m:m + 1] * 1024.0 + lane_row * mb + n))
            target_columns.append(column(jnp.where(kept, target, 1.0 * blocks)))
    ranks = []
    for mine in key_columns:
        before = [jnp.where(key < mine, 1.0, 0.0) for key in keys]
        ranks.append(jnp.sum(functools.reduce(jnp.add, before), axis=1, keepdims=True))

    def gathered(hits):
        return jnp.sum(functools.reduce(jnp.add, hits), axis=0, keepdims=True)

    def write(at, values):
        order[pl.ds(at, 1), :] = values.astype(jnp.int32)

    lines = -(-high * ma * mb // 128)
    for at in range(lines):
        spot = lane_row + at * 128.0
        for base, columns in ((0, code_columns), (lines, target_columns)):
            write(base + at, gathered([
                jnp.where(rank == spot, values, 0.0) for rank, values in zip(ranks, columns)
            ]))
    bound = (lane_row + 1.0) * (kb_cols * 1024.0)
    write(2 * lines, gathered([jnp.where(mine < bound, 1.0, 0.0) for mine in key_columns]))
    filled = gathered([jnp.where(mine == lane_row, 1.0, 0.0) for mine in target_columns])
    empty = jnp.where((filled < 0.5) & (lane_row < blocks), 1.0, 0.0)
    lane = lax.broadcasted_iota(jnp.int32, (128, 128), 1).astype(jnp.float32)
    line = lax.broadcasted_iota(jnp.int32, (128, 128), 0).astype(jnp.float32)
    wide = jnp.broadcast_to(empty, (128, 128))
    rank = jnp.sum(jnp.where(lane < line, wide, 0.0), axis=1, keepdims=True)
    flag = jnp.sum(jnp.where(lane == line, wide, 0.0), axis=1, keepdims=True)
    write(2 * lines + 1, gathered([jnp.where(rank == lane, line * flag, 0.0)]))
    write(2 * lines + 2, jnp.broadcast_to(jnp.sum(empty, axis=1, keepdims=True), (1, 128)))


def gather_kernel(
    sizes, option, left, right, perm, meta, tiles,
    left_all, right_all, order,
    own_left, packed_down, packed_up, left_meta, right_meta,
    up_send, up_recv, down_send, down_recv,
    x_send, x_recv, own_send, own_recv, pass_send, pass_recv,
    lm_send, lm_recv, rm_send, rm_recv, stage_sem, left_sem, right_sem,
):
    n_row, n_col = sizes[:2]
    row = lax.axis_index("row")
    col = lax.axis_index("col")
    n_chip = n_row // 2
    chip, core = row // 2, row % 2
    partner = chip * 2 + 1 - core
    slots = left.shape[0]
    main, _, middle = option

    staged = pltpu.make_async_copy(left, own_left, stage_sem)
    staged.start()
    barrier = pltpu.get_barrier_semaphore()
    for step in range(1, n_row):
        pl.semaphore_signal(
            barrier, inc=1, device_id={"row": (row + step) % n_row}, device_id_type=MESH
        )
    for step in range(1, n_col):
        pl.semaphore_signal(
            barrier, inc=1, device_id={"col": (col + step) % n_col}, device_id_type=MESH
        )

    bounds = [main * at // MAIN_CUTS for at in range(MAIN_CUTS + 1)]
    cuts = [(low, high, False) for low, high in zip(bounds, bounds[1:])]
    if middle > main:
        cuts.append((main, middle, True))
    right_size = right.shape[1] // RIGHT_CUTS

    def left_copy(step, cut, up):
        low, high, _ = cuts[cut]
        panel = col - step if up else col + step
        source = (
            (packed_up if up else packed_down).at[pl.ds(low, high - low)]
            if step == 0 else left_all.at[panel, pl.ds(low, high - low)]
        )
        send, recv = (up_send, up_recv) if up else (down_send, down_recv)
        return pltpu.make_async_remote_copy(
            src_ref=source, dst_ref=left_all.at[panel, pl.ds(low, high - low)],
            send_sem=send.at[step, cut], recv_sem=recv.at[step, cut],
            device_id={"col": col + 1 if up else col - 1}, device_id_type=MESH,
        )

    def left_sends(step, cut, up):
        mid = cuts[cut][2]
        if up:
            return (col + 1 < n_col - (1 if mid else 0)) & (col - step >= 0)
        return (col - 1 >= (1 if mid else 0)) & (col + step < n_col)

    def left_receives(step, cut, up):
        mid = cuts[cut][2]
        if up:
            return (col - 1 - step >= 0) & (col < n_col - (1 if mid else 0))
        return (col + 1 + step < n_col) & (col >= (1 if mid else 0))

    def across(step, cut):
        span = pl.ds(cut * right_size, right_size)
        other = ((chip + step) % n_chip) * 2 + core
        return pltpu.make_async_remote_copy(
            src_ref=right.at[:, span], dst_ref=right_all.at[:, row, span],
            send_sem=x_send.at[step - 1, cut], recv_sem=x_recv.at[step - 1, cut],
            device_id={"row": other}, device_id_type=MESH,
        )

    def passed(step, cut):
        span = pl.ds(cut * right_size, right_size)
        panel = ((chip + n_chip - step) % n_chip) * 2 + core
        return pltpu.make_async_remote_copy(
            src_ref=right_all.at[:, panel, span], dst_ref=right_all.at[:, panel, span],
            send_sem=pass_send.at[step - 1, cut], recv_sem=pass_recv.at[step - 1, cut],
            device_id={"row": partner}, device_id_type=MESH,
        )

    own = pltpu.make_async_remote_copy(
        src_ref=right, dst_ref=right_all.at[:, row],
        send_sem=own_send, recv_sem=own_recv,
        device_id={"row": partner}, device_id_type=MESH,
    )
    kept = (
        pltpu.make_async_copy(left, left_all.at[col], left_sem),
        pltpu.make_async_copy(right, right_all.at[:, row], right_sem),
    )

    staged.wait()

    @pl.loop(0, middle)
    def _(at):
        packed_down[at] = own_left[perm[0, at]]
        packed_up[at] = own_left[perm[1, at]]

    left_meta[col] = meta[...]
    right_meta[row] = meta[...]

    def meta_copies():
        for step in range(1, n_col):
            yield pltpu.make_async_remote_copy(
                src_ref=meta, dst_ref=left_meta.at[col],
                send_sem=lm_send.at[step - 1], recv_sem=lm_recv.at[step - 1],
                device_id={"col": (col + step) % n_col}, device_id_type=MESH,
            )
        for step in range(1, n_row):
            yield pltpu.make_async_remote_copy(
                src_ref=meta, dst_ref=right_meta.at[row],
                send_sem=rm_send.at[step - 1], recv_sem=rm_recv.at[step - 1],
                device_id={"row": (row + step) % n_row}, device_id_type=MESH,
            )

    pl.semaphore_wait(barrier, n_row + n_col - 2)
    for copy in meta_copies():
        copy.start()
    for cut in range(len(cuts)):
        for up in (True, False):
            pl.when(left_sends(0, cut, up))(left_copy(0, cut, up).start)
    for step in range(1, n_chip):
        for cut in range(RIGHT_CUTS):
            across(step, cut).start()
    own.start()
    for copy in kept:
        copy.start()

    def take_left(step, cut):
        for up in (True, False):
            pl.when(left_receives(step, cut, up))(left_copy(step, cut, up).wait_recv)
            if step + 1 < n_col - 1:
                pl.when(left_sends(step + 1, cut, up))(left_copy(step + 1, cut, up).start)

    def take_right(step, cut):
        across(step, cut).wait_recv()
        passed(step, cut).start()

    def take_order():
        for copy in meta_copies():
            copy.wait()
        order_pairs(sizes, lax.axis_index("kpt"), col, tiles, left_meta, right_meta, order)

    left_jobs = [
        (step * middle + cuts[cut][1], functools.partial(take_left, step, cut))
        for step in range(n_col - 1) for cut in range(len(cuts))
    ]
    right_jobs = [
        (((step - 1) * RIGHT_CUTS + cut + 1) * right.shape[0] * right_size + 0.5,
         functools.partial(take_right, step, cut))
        for step in range(1, n_chip) for cut in range(RIGHT_CUTS)
    ]
    for _, job in sorted([(7, take_order)] + left_jobs + right_jobs, key=lambda entry: entry[0]):
        job()

    own.wait()
    for copy in kept:
        copy.wait()
    for step in range(1, n_chip):
        for cut in range(RIGHT_CUTS):
            across(step, cut).wait_send()
            passed(step, cut).wait()
    for step in range(n_col - 1):
        for cut in range(len(cuts)):
            for up in (True, False):
                pl.when(left_sends(step, cut, up))(left_copy(step, cut, up).wait_send)


def product_kernel(sizes, left, right, order, out, stage, partial, out_sem):
    n_row, n_col, sets, per, ma, mb, kb_cols = sizes
    blocks = GR * kb_cols
    lines = -(-n_col * per * ma * mb // 128)
    width = stage.shape[2]
    empty = jnp.zeros(stage.shape[1:], stage.dtype)

    @pl.loop(0, order[2 * lines + 2, 0])
    def _(at):
        stage[order[2 * lines + 1, at]] = empty

    def out_copy(line):
        span = pl.ds(line * kb_cols, kb_cols)
        return pltpu.make_async_copy(stage.at[span], out.at[span], out_sem.at[line])

    count = order[2 * lines, GR - 1]

    def group(at, carry):
        line, last = carry
        codes, targets, done = [], [], []
        for lane in range(GROUP):
            spot = at * GROUP + lane
            codes.append(order[spot // 128, spot % 128])
            targets.append(order[lines + spot // 128, spot % 128])
        for code in codes:
            block = left[code // 1024]
            wide = jnp.concatenate([block[:width], block[width:]], axis=1)
            other = right[code % 1024]
            real, imag = other[:width], other[width:]
            matrix = jnp.concatenate(
                [jnp.concatenate([real, imag], axis=1), jnp.concatenate([-imag, real], axis=1)],
                axis=0,
            )
            done.append(jnp.dot(wide, matrix, preferred_element_type=jnp.float32))
        held = partial[...]
        for target, product in zip(targets, done):
            held = jnp.where(target == last, held, 0.0) + product
            value = held.astype(stage.dtype)
            stage[target, :width] = value[:, :width]
            stage[target, width:] = value[:, width:]
            last = target
        partial[...] = held
        ready = (line < GR) & (at * GROUP >= order[2 * lines, jnp.minimum(line, GR - 1)])
        pl.when(ready)(lambda: out_copy(line).start())
        return line + jnp.where(ready, 1, 0), last

    partial[...] = jnp.zeros(partial.shape, partial.dtype)
    line, _ = lax.fori_loop(
        0, (count + GROUP - 1) // GROUP, group, (jnp.int32(0), jnp.int32(-1))
    )

    @pl.loop(line, GR)
    def _(line):
        out_copy(line).start()

    @pl.loop(0, GR)
    def _(line):
        out_copy(line).wait()


def body(
    n_kpt, n_row, n_col, left_blocks, left_rows, left_count, left_level,
    right_blocks, right_cols, right_count, right_level,
):
    _, per, ma, _, width, _ = left_blocks.shape
    sets, right_per, _, mb = right_blocks.shape[:4]
    assert right_per == per and sets * n_row == n_col and n_row % 2 == 0 and sets <= 2
    blocks = GR * (n_row * sets * per // n_col)
    assert n_col * per <= 128 and per * ma <= 128 and blocks <= 128 and ma * mb <= 8
    slots = per * ma
    left = left_blocks.reshape(slots, 2 * width, width)
    right = right_blocks.reshape(sets, per * mb, 2 * width, width)
    any_space = pl.BlockSpec(memory_space=pl.ANY)
    vmem = pl.BlockSpec(memory_space=pltpu.VMEM)
    smem = pl.BlockSpec(memory_space=pltpu.SMEM)
    dma = pltpu.SemaphoreType.DMA
    n_chip = n_row // 2
    total = n_kpt * n_row * n_col
    options = variants(slots)
    sizes = (n_row, n_col, sets, per, ma, mb, n_row * sets * per // n_col)
    tile_rows = -(-(ma + sets) // 4) * 4
    meta_rows = -(-(2 * ma + 2 * mb * sets) // 8) * 8
    lines = -(-n_col * per * ma * mb // 128)
    order_rows = -(-(2 * lines + 3) // 8) * 8
    meta, tiles, perm, choice = pl.pallas_call(
        functools.partial(plan_kernel, (n_kpt,) + sizes[:-1], options),
        out_shape=(
            jax.ShapeDtypeStruct((meta_rows, 128), jnp.int32),
            jax.ShapeDtypeStruct((total, tile_rows, 128), jnp.int32),
            jax.ShapeDtypeStruct((2, 128), jnp.int32),
            jax.ShapeDtypeStruct((1,), jnp.int32),
        ),
        in_specs=[vmem] * 6,
        out_specs=(vmem, vmem, vmem, smem),
        scratch_shapes=[pltpu.VMEM((tile_rows, 128), jnp.int32), dma((total,)), dma((total,))],
        compiler_params=pltpu.CompilerParams(collective_id=0, has_side_effects=True),
        name="plan",
    )(
        left_level[0].T, left_rows[0].T, left_count,
        right_level[:, :, 0].transpose(0, 2, 1), right_cols[:, :, 0].transpose(0, 2, 1),
        right_count.transpose(0, 2, 1),
    )

    kb_cols = sizes[-1]
    left_shape = (n_col,) + left.shape
    right_shape = (sets, n_row) + right.shape[1:]
    limit = VMEM_BYTES - (n_col * left.size + n_row * right.size) * left.dtype.itemsize

    def run(at, left, right, perm, meta, tiles):
        cuts = MAIN_CUTS + 1
        left_all, right_all, order = pl.pallas_call(
            functools.partial(gather_kernel, sizes, options[at]),
            out_shape=(
                pltpu.VMEM(left_shape, left.dtype),
                pltpu.VMEM(right_shape, right.dtype),
                jax.ShapeDtypeStruct((order_rows, 128), jnp.int32),
            ),
            in_specs=[any_space, any_space, smem, vmem, vmem],
            out_specs=(vmem, vmem, vmem),
            scratch_shapes=[
                *[pltpu.VMEM(left.shape, left.dtype)] * 3,
                pltpu.VMEM((n_col, meta_rows, 128), jnp.int32),
                pltpu.VMEM((n_row, meta_rows, 128), jnp.int32),
                *[dma((n_col - 1, cuts))] * 4,
                *[dma((n_chip - 1, RIGHT_CUTS))] * 2,
                *[dma] * 2,
                *[dma((n_chip - 1, RIGHT_CUTS))] * 2,
                *[dma((n_col - 1,))] * 2,
                *[dma((n_row - 1,))] * 2,
                *[dma] * 3,
            ],
            compiler_params=pltpu.CompilerParams(
                collective_id=1 + at, has_side_effects=True, vmem_limit_bytes=limit
            ),
            name=f"gather_panels_{at}",
        )(left, right, perm, meta, tiles)
        return pl.pallas_call(
            functools.partial(product_kernel, sizes),
            out_shape=jax.ShapeDtypeStruct((blocks, 2 * width, width), jnp.bfloat16),
            in_specs=[vmem, vmem, smem],
            out_specs=any_space,
            scratch_shapes=[
                pltpu.VMEM((blocks + 1, 2 * width, width), jnp.bfloat16),
                pltpu.VMEM((width, 2 * width), jnp.float32),
                dma((GR,)),
            ],
            compiler_params=pltpu.CompilerParams(vmem_limit_bytes=limit),
            name="pair_products",
        )(
            pltpu.with_memory_space_constraint(
                left_all.reshape((-1,) + left.shape[1:]), pltpu.VMEM
            ),
            pltpu.with_memory_space_constraint(
                right_all.reshape((-1,) + right.shape[2:]), pltpu.VMEM
            ),
            order,
        )

    out = lax.switch(
        choice[0], [functools.partial(run, at) for at in range(len(options))],
        left, right, perm, meta, tiles,
    )
    return out.reshape(GR, kb_cols, 2, width, width)


def solution(mesh):
    in_specs = (
        P(("kpt", "row"), "col", None, None, None, None),
        P(("kpt", "row"), "col", None),
        P(("kpt", "row"), "col"),
        P(("kpt", "row"), "col", None),
        P("kpt", "row", "col", None, None, None, None),
        P("kpt", "row", "col", None),
        P("kpt", "row", "col"),
        P("kpt", "row", "col", None),
    )
    out_specs = P(("kpt", "row"), "col", None, None, None)
    return jax.shard_map(
        functools.partial(body, mesh.shape["kpt"], mesh.shape["row"], mesh.shape["col"]),
        mesh=mesh, in_specs=in_specs, out_specs=out_specs, check_vma=False,
    )
```

```python
import functools

import jax
import jax.numpy as jnp
from jax import lax
from jax.experimental import pallas as pl
from jax.experimental.pallas import tpu as pltpu
from jax.sharding import PartitionSpec as P

GR = 8
LEVEL_CUT = 7
DEAD = -1000
GROUP = 4
MAIN_CUTS = 2
RIGHT_CUTS = 8
VMEM_BYTES = 62 * 1024 * 1024
MESH = pl.DeviceIdType.MESH
FAR = 2.0 ** 17


def variants(slots, n_col, right_slots):
    main, head = slots * 18 // 32, slots * 27 // 32
    middle, rights = slots * 30 // 32, right_slots * 56 // 64
    scale = slots * (n_col - 1) / 96
    found = [
        (main, max(1, int(spill * scale)), head, middle, rights) for spill in (5, 7, 9, 11, 13, 16)
    ]
    found.append((main, max(1, int(24 * scale)), slots, slots, right_slots))
    return found + [(slots, 0, slots, slots, right_slots)]


def ordered(levels, end, union, slots, lane_row):
    ma, per = levels.shape[0], slots // levels.shape[0]
    rows, columns = [], []
    lane = lax.broadcasted_iota(jnp.int32, (per, 128), 1)
    line = lax.broadcasted_iota(jnp.int32, (per, 128), 0)
    for m in range(ma):
        kind = jnp.where(
            levels[m:m + 1] + end >= LEVEL_CUT, 0.0,
            jnp.where(levels[m:m + 1] + union >= LEVEL_CUT, 1.0, 2.0),
        )
        key = jnp.where(lane_row < per, kind * 128.0 + lane_row * ma + m, 1024.0)
        rows.append(key)
        columns.append(jnp.sum(
            jnp.where(lane == line, jnp.broadcast_to(key, (per, 128)), 0.0), axis=1, keepdims=True
        ))
    return rows, columns


def spilled(levels, end, main):
    hits = [
        jnp.where(levels[m:m + 1] + end >= LEVEL_CUT, 1.0, 0.0) for m in range(levels.shape[0])
    ]
    size = jnp.sum(functools.reduce(jnp.add, hits), axis=1, keepdims=True)
    return jnp.maximum(size - main, 0.0)


def placed(live, per, lane, line):
    padded = live if live.shape[1] == 128 else jnp.concatenate(
        [live, jnp.zeros((1, 128 - per), jnp.float32)], axis=1
    )
    wide = jnp.broadcast_to(padded, (per, 128))
    own = jnp.sum(jnp.where(lane == line, wide, 0.0), axis=1, keepdims=True)
    first = jnp.sum(jnp.where(lane < line, wide, 0.0), axis=1, keepdims=True)
    return own, first


def plan_kernel(
    sizes, options, left_level, left_rows, left_count, right_level, right_cols, right_count,
    meta, tiles, perm, choice, tile, send, recv,
):
    n_kpt, n_row, n_col, sets, per, ma, mb = sizes
    slots = per * ma
    kpt, row, col = (lax.axis_index(name) for name in ("kpt", "row", "col"))
    total = n_kpt * n_row * n_col
    me = (kpt * n_row + row) * n_col + col

    def place_of(step):
        other = (me + step) % total
        return {
            "kpt": other // (n_row * n_col), "row": (other // n_col) % n_row, "col": other % n_col
        }

    def copy_of(step):
        return pltpu.make_async_remote_copy(
            src_ref=tile, dst_ref=tiles.at[me], send_sem=send.at[step], recv_sem=recv.at[step],
            device_id=place_of(step), device_id_type=MESH,
        )

    barrier = pltpu.get_barrier_semaphore()

    @pl.loop(1, total)
    def _(step):
        pl.semaphore_signal(barrier, inc=1, device_id=place_of(step), device_id_type=MESH)

    tile[...] = jnp.full(tile.shape, DEAD, jnp.int32)
    live = lax.broadcasted_iota(jnp.int32, (ma, per), 0) < left_count[...]
    levels = jnp.where(live, left_level[...], DEAD)
    tile[:ma, :per] = levels
    rights = []
    for which in range(sets):
        live = lax.broadcasted_iota(jnp.int32, (mb, per), 0) < right_count[which]
        rights.append(jnp.where(live, right_level[which], DEAD))
        tile[ma + which:ma + which + 1, :per] = jnp.max(rights[-1], axis=0, keepdims=True)
        size = jnp.sum(right_count[which].astype(jnp.float32), axis=1, keepdims=True)
        tile[ma + which:ma + which + 1, 127:] = size.astype(jnp.int32)
    tiles[me] = tile[...]
    pl.semaphore_wait(barrier, total - 1)

    @pl.loop(1, total)
    def _(step):
        copy_of(step).start()

    meta[...] = jnp.full(meta.shape, DEAD, jnp.int32)
    meta[:ma, :per] = levels
    meta[ma:2 * ma, :per] = left_rows[...]
    for which in range(sets):
        base = 2 * ma + which * 2 * mb
        meta[base:base + mb, :per] = right_cols[which]
        meta[base + mb:base + 2 * mb, :per] = rights[which]

    @pl.loop(1, total)
    def _(step):
        copy_of(step).wait_recv()

    def at_device(k, r, c):
        return (k * n_row + r) * n_col + c

    def right_max(k, panel, q):
        return tiles[at_device(k, panel % n_row, q), pl.ds(ma + panel // n_row, 1), :]

    def measure_part(k, carry):
        most_end, most_mid, most_spill, most_right = carry
        spills = [zero, zero]
        for panel in range(n_col):
            levels = [
                jnp.concatenate(
                    [tiles[at_device(k, r, panel), pl.ds(m, 1), :] for r in range(n_row)], axis=0
                )
                for m in range(ma)
            ]

            def needed(most):
                hits = [jnp.where(level + most >= LEVEL_CUT, 1.0, 0.0) for level in levels]
                return jnp.sum(functools.reduce(jnp.add, hits), axis=1, keepdims=True)

            rights = [right_max(k, panel, q) for q in range(n_col)]
            for right in rights:
                most_right = jnp.maximum(most_right, right)
            for way, (taken, right) in enumerate(
                ((panel > 0, rights[0]), (panel < n_col - 1, rights[-1]))
            ):
                if taken:
                    wanted = needed(right)
                    most_end = jnp.maximum(most_end, wanted)
                    spills[way] = spills[way] + jnp.maximum(wanted - main, 0.0)
            if panel > 1:
                union = functools.reduce(jnp.maximum, rights[:panel])
                most_mid = jnp.maximum(most_mid, needed(union))
            if panel < n_col - 2:
                union = functools.reduce(jnp.maximum, rights[panel + 1:])
                most_mid = jnp.maximum(most_mid, needed(union))
        most_spill = jnp.maximum(most_spill, jnp.maximum(*spills))
        return most_end, most_mid, most_spill, most_right

    main = options[0][0]
    zero = jnp.zeros((n_row, 1), jnp.float32)
    most_end, most_mid, most_spill, most_right = lax.fori_loop(
        0, n_kpt, measure_part, (zero, zero, zero, jnp.zeros((1, 128), jnp.int32))
    )
    lanes = lax.broadcasted_iota(jnp.int32, (1, 128), 1)
    most_right = jnp.max(
        jnp.where(lanes == 127, most_right, 0).astype(jnp.float32), axis=1, keepdims=True
    )
    index = zero
    for _, spill, head, middle, limit in options[:-1]:
        over = (most_spill > spill) | (most_end > head) | (most_mid > middle)
        index = index + jnp.where(over | (most_right > limit), 1.0, 0.0)
    choice[0] = jnp.max(index).astype(jnp.int32)

    lane_row = lax.broadcasted_iota(jnp.int32, (1, 128), 1).astype(jnp.float32)
    line = lax.broadcasted_iota(jnp.int32, (per, 128), 0).astype(jnp.float32)
    mine = tiles[me, :ma, :]
    for at, up in enumerate((False, True)):
        which = ma + col // n_row
        near = [
            tiles[at_device(kpt, col % n_row, q), pl.ds(which, 1), :] for q in range(n_col)
        ]
        union = jnp.full((1, 128), DEAD, jnp.int32)
        for q in range(n_col):
            beyond = q > col if up else q < col
            union = jnp.maximum(union, jnp.where(beyond, near[q], DEAD))
        rows, columns = ordered(mine, near[-1] if up else near[0], union, slots, lane_row)
        found = jnp.zeros((1, 128), jnp.float32)
        for m in range(ma):
            before = [jnp.where(key < columns[m], 1.0, 0.0) for key in rows]
            rank = jnp.sum(functools.reduce(jnp.add, before), axis=1, keepdims=True)
            hit = jnp.where(rank == lane_row, line * ma + m, 0.0)
            found = found + jnp.sum(hit, axis=0, keepdims=True)
        perm[pl.ds(at, 1), :] = found.astype(jnp.int32)

    for at, up in ((2, False), (3, True)):
        panels = range(n_col - 2, -1, -1) if up else range(1, n_col)
        code, low = jnp.zeros((1, 128), jnp.float32), jnp.zeros((1, 1), jnp.float32)
        for panel in panels:
            levels = tiles[at_device(kpt, row, panel), :ma, :]
            end = right_max(kpt, panel, n_col - 1 if up else 0)
            high = low + spilled(levels, end, main)
            own = up and panel == n_col - 2
            base = (n_col if own else panel) * slots
            inside = (lane_row >= low) & (lane_row < high)
            code = code + jnp.where(inside, base + lane_row - low, 0.0)
            low = high
        perm[pl.ds(at, 1), :] = code.astype(jnp.int32)
    lane = lax.broadcasted_iota(jnp.int32, (per, 128), 1).astype(jnp.float32)
    for which in range(sets):
        live, first = placed(right_count[which].astype(jnp.float32), per, lane, line)
        found = jnp.zeros((1, 128), jnp.float32)
        for n in range(mb):
            hit = jnp.where((first + n == lane) & (live > n), line * mb + n, 0.0)
            found = found + jnp.sum(hit, axis=0, keepdims=True)
        perm[pl.ds(4 + which, 1), :] = found.astype(jnp.int32)

    @pl.loop(1, total)
    def _(step):
        copy_of(step).wait_send()


def order_pairs(sizes, main, kpt, col, tiles, left_meta, right_meta, order):
    n_row, n_col, sets, per, ma, mb, kb_cols = sizes
    slots, high = per * ma, n_col * per
    blocks = GR * kb_cols
    lane_row = lax.broadcasted_iota(jnp.int32, (1, 128), 1).astype(jnp.float32)

    def right_max(panel, q):
        at = (kpt * n_row + panel % n_row) * n_col + q
        return tiles[at, pl.ds(ma + panel // n_row, 1), :]

    lefts = jnp.zeros((2 * ma, 128), jnp.float32)
    rights = jnp.zeros((2 * mb, 128), jnp.float32)
    places = jnp.zeros((8, 128), jnp.float32)
    spots = jnp.zeros((8, 128), jnp.float32)
    thin = lax.broadcasted_iota(jnp.int32, (per, 128), 1).astype(jnp.float32)
    thick = lax.broadcasted_iota(jnp.int32, (per, 128), 0).astype(jnp.float32)
    lows, low = [None] * n_col, jnp.zeros((1, 1), jnp.float32)
    for panel in range(1, n_col):
        lows[panel] = low
        low = low + spilled(left_meta[panel, :ma, :], right_max(panel, 0), main)
    low = jnp.zeros((1, 1), jnp.float32)
    for panel in range(n_col - 2, -1, -1):
        lows[panel] = low if lows[panel] is None else jnp.where(col == 0, lows[panel], low)
        low = low + spilled(left_meta[panel, :ma, :], right_max(panel, n_col - 1), main)
    for panel in range(n_col):
        levels = left_meta[panel, :ma, :]
        down, up = panel > col, panel < col
        end = jnp.where(down, right_max(panel, 0), right_max(panel, n_col - 1))
        union = jnp.full((1, 128), DEAD, jnp.int32)
        for q in range(n_col):
            beyond = down if q < panel else up
            if q != panel:
                union = jnp.maximum(union, jnp.where(beyond, right_max(panel, q), DEAD))
        rows, columns = ordered(levels, end, union, slots, lane_row)
        found = []
        for m in range(ma):
            before = [jnp.where(key < rows[m], 1.0, 0.0) for key in columns]
            rank = jnp.sum(functools.reduce(jnp.add, before), axis=0, keepdims=True)
            own = jnp.where(down | up, rank, lane_row * ma + m) + panel * slots
            far = (down | up) & ((col == 0) | (col == n_col - 1)) & (rank >= main)
            found.append(jnp.where(far, n_col * slots + lows[panel] + rank - main, own))
        found = jnp.concatenate(found + [jnp.zeros((8 - ma, 128), jnp.float32)], axis=0)
        base = 2 * ma + panel // n_row * 2 * mb
        here = (lane_row >= panel * per) & (lane_row < (panel + 1) * per)

        def moved(values):
            values = pltpu.roll(values, panel * per, 1) if panel else values
            return jnp.where(here, values, 0.0)

        lefts = lefts + moved(left_meta[panel, :2 * ma, :].astype(jnp.float32))
        right = right_meta[panel % n_row, base:base + 2 * mb, :].astype(jnp.float32)
        rights = rights + moved(right)
        places = places + moved(found)
        size = jnp.zeros((1, 128), jnp.float32)
        for n in range(mb):
            size = size + jnp.where((right[mb + n:mb + n + 1] > DEAD / 2) & (lane_row < per), 1.0, 0.0)
        live, _ = placed(size, per, thin, thick)
        first = jnp.sum(jnp.where(thick < thin, live, 0.0), axis=0, keepdims=True)
        spots = spots + moved(
            jnp.broadcast_to(jnp.where(lane_row < per, first, 0.0) + panel * per * mb, (8, 128))
        )

    lane = lax.broadcasted_iota(jnp.int32, (high, 128), 1)
    line = lax.broadcasted_iota(jnp.int32, (high, 128), 0)

    def column(values):
        wide = jnp.broadcast_to(values, (high, 128))
        return jnp.sum(jnp.where(lane == line, wide, 0.0), axis=1, keepdims=True)

    keys, key_columns, code_columns, target_columns = [], [], [], []
    for m in range(ma):
        for n in range(mb):
            kept = lefts[m:m + 1] + rights[mb + n:mb + n + 1] >= LEVEL_CUT
            target = lefts[ma + m:ma + m + 1] * kb_cols + rights[n:n + 1]
            spot = lane_row + (m * mb + n) * 128.0
            key = jnp.where(kept, target * 1024.0 + spot, FAR + spot)
            keys.append(jnp.where(lane_row < high, key, 2 * FAR))
            key_columns.append(column(keys[-1]))
            code = places[m:m + 1] * 1024.0 + spots[:1] + n
            code_columns.append(column(jnp.where(kept, code, 0.0)))
            target_columns.append(column(jnp.where(kept, target, 1.0 * blocks)))
    ranks = []
    for mine in key_columns:
        before = [jnp.where(key < mine, 1.0, 0.0) for key in keys]
        ranks.append(jnp.sum(functools.reduce(jnp.add, before), axis=1, keepdims=True))

    def gathered(hits):
        return jnp.sum(functools.reduce(jnp.add, hits), axis=0, keepdims=True)

    def write(at, values):
        order[pl.ds(at, 1), :] = values.astype(jnp.int32)

    lines = -(-high * ma * mb // 128)
    for at in range(lines):
        spot = lane_row + at * 128.0
        for base, columns in ((0, code_columns), (lines, target_columns)):
            write(base + at, gathered([
                jnp.where(rank == spot, values, 0.0) for rank, values in zip(ranks, columns)
            ]))
    bound = (lane_row + 1.0) * (kb_cols * 1024.0)
    write(2 * lines, gathered([jnp.where(mine < bound, 1.0, 0.0) for mine in key_columns]))
    filled = gathered([jnp.where(mine == lane_row, 1.0, 0.0) for mine in target_columns])
    empty = jnp.where((filled < 0.5) & (lane_row < blocks), 1.0, 0.0)
    lane = lax.broadcasted_iota(jnp.int32, (128, 128), 1).astype(jnp.float32)
    line = lax.broadcasted_iota(jnp.int32, (128, 128), 0).astype(jnp.float32)
    wide = jnp.broadcast_to(empty, (128, 128))
    rank = jnp.sum(jnp.where(lane < line, wide, 0.0), axis=1, keepdims=True)
    flag = jnp.sum(jnp.where(lane == line, wide, 0.0), axis=1, keepdims=True)
    write(2 * lines + 1, gathered([jnp.where(rank == lane, line * flag, 0.0)]))
    write(2 * lines + 2, jnp.broadcast_to(jnp.sum(empty, axis=1, keepdims=True), (1, 128)))


def gather_kernel(
    sizes, option, left, right, perm, meta, tiles,
    left_all, right_all, order,
    own_left, own_right, packed_down, packed_up, side, spill_down, spill_up,
    left_meta, right_meta,
    up_send, up_recv, down_send, down_recv, spill_send, spill_recv,
    x_send, x_recv, own_send, own_recv, pass_send, pass_recv,
    lm_send, lm_recv, rm_send, rm_recv, stage_sem, right_sem, left_sem,
):
    n_row, n_col, sets = sizes[:3]
    row = lax.axis_index("row")
    col = lax.axis_index("col")
    n_chip = n_row // 2
    chip, core = row // 2, row % 2
    partner = chip * 2 + 1 - core
    slots = left.shape[0]
    main, spill, head, middle, limit = option

    stages = (
        pltpu.make_async_copy(left, own_left, stage_sem),
        pltpu.make_async_copy(right, own_right, right_sem),
        pltpu.make_async_copy(left, left_all.at[pl.ds(col * slots, slots)], left_sem),
    )
    for copy in stages:
        copy.start()
    barrier = pltpu.get_barrier_semaphore()
    for step in range(1, n_row):
        pl.semaphore_signal(
            barrier, inc=1, device_id={"row": (row + step) % n_row}, device_id_type=MESH
        )
    for step in range(1, n_col):
        pl.semaphore_signal(
            barrier, inc=1, device_id={"col": (col + step) % n_col}, device_id_type=MESH
        )

    bounds = [main * at // MAIN_CUTS for at in range(MAIN_CUTS + 1)]
    cuts = [(low, high, "main") for low, high in zip(bounds, bounds[1:])]
    if head > main:
        cuts.append((main, head, "side"))
    if middle > head:
        cuts.append((head, middle, "rest"))
    bounds = [limit * at // RIGHT_CUTS for at in range(RIGHT_CUTS + 1)]
    right_cuts = [pl.ds(low, high - low) for low, high in zip(bounds, bounds[1:])]

    def left_copy(step, cut, up):
        low, high, kind = cuts[cut]
        panel = col - step if up else col + step
        span = pl.ds(panel * slots + low, high - low)
        target = side.at[span] if kind == "side" else left_all.at[span]
        source = (packed_up if up else packed_down).at[pl.ds(low, high - low)]
        send, recv = (up_send, up_recv) if up else (down_send, down_recv)
        return pltpu.make_async_remote_copy(
            src_ref=source if step == 0 else target, dst_ref=target,
            send_sem=send.at[step, cut], recv_sem=recv.at[step, cut],
            device_id={"col": col + 1 if up else col - 1}, device_id_type=MESH,
        )

    def left_sends(step, cut, up):
        mid = 0 if cuts[cut][2] == "main" else 1
        if up:
            return (col + 1 < n_col - mid) & (col - step >= 0)
        return (col - 1 >= mid) & (col + step < n_col)

    def left_receives(step, cut, up):
        mid = 0 if cuts[cut][2] == "main" else 1
        if up:
            return (col - 1 - step >= 0) & (col < n_col - mid)
        return (col + 1 + step < n_col) & (col >= mid)

    def start_left(step, cut):
        for up in (True, False):
            pl.when(left_sends(step, cut, up))(left_copy(step, cut, up).start)

    def spill_copy(up):
        return pltpu.make_async_remote_copy(
            src_ref=spill_up if up else spill_down,
            dst_ref=left_all.at[pl.ds(n_col * slots, spill)],
            send_sem=spill_send.at[int(up)], recv_sem=spill_recv.at[int(up)],
            device_id={"col": n_col - 1 if up else 0}, device_id_type=MESH,
        )

    def across(step, cut):
        span = right_cuts[cut]
        other = ((chip + step) % n_chip) * 2 + core
        return pltpu.make_async_remote_copy(
            src_ref=right_all.at[:, row, span], dst_ref=right_all.at[:, row, span],
            send_sem=x_send.at[step - 1, cut], recv_sem=x_recv.at[step - 1, cut],
            device_id={"row": other}, device_id_type=MESH,
        )

    def passed(step, cut):
        span = right_cuts[cut]
        panel = ((chip + n_chip - step) % n_chip) * 2 + core
        return pltpu.make_async_remote_copy(
            src_ref=right_all.at[:, panel, span], dst_ref=right_all.at[:, panel, span],
            send_sem=pass_send.at[step - 1, cut], recv_sem=pass_recv.at[step - 1, cut],
            device_id={"row": partner}, device_id_type=MESH,
        )

    own = pltpu.make_async_remote_copy(
        src_ref=right_all.at[:, row, pl.ds(0, limit)],
        dst_ref=right_all.at[:, row, pl.ds(0, limit)],
        send_sem=own_send, recv_sem=own_recv,
        device_id={"row": partner}, device_id_type=MESH,
    )

    stages[0].wait()

    @pl.loop(0, middle)
    def _(at):
        packed_down[at] = own_left[perm[0, at]]
        packed_up[at] = own_left[perm[1, at]]

    left_meta[col] = meta[...]
    right_meta[row] = meta[...]

    def meta_copies():
        for step in range(1, n_col):
            yield pltpu.make_async_remote_copy(
                src_ref=meta, dst_ref=left_meta.at[col],
                send_sem=lm_send.at[step - 1], recv_sem=lm_recv.at[step - 1],
                device_id={"col": (col + step) % n_col}, device_id_type=MESH,
            )
        for step in range(1, n_row):
            yield pltpu.make_async_remote_copy(
                src_ref=meta, dst_ref=right_meta.at[row],
                send_sem=rm_send.at[step - 1], recv_sem=rm_recv.at[step - 1],
                device_id={"row": (row + step) % n_row}, device_id_type=MESH,
            )

    pl.semaphore_wait(barrier, n_row + n_col - 2)
    for copy in meta_copies():
        copy.start()
    for cut in range(len(cuts)):
        if cuts[cut][2] != "rest":
            start_left(0, cut)

    stages[1].wait()
    for which in range(sets):
        @pl.loop(0, limit)
        def _(at):
            right_all[which, row, at] = own_right[which, perm[4 + which, at]]

    for step in range(1, n_chip):
        for cut in range(RIGHT_CUTS):
            across(step, cut).start()
    own.start()
    if spill:
        @pl.loop(main, head)
        def _(at):
            side[col * slots + at] = packed_down[at]
            side[n_col * slots + at] = packed_up[at]

    def take_left(step, cut):
        for up in (True, False):
            pl.when(left_receives(step, cut, up))(left_copy(step, cut, up).wait_recv)
            if step + 1 < n_col - 1:
                pl.when(left_sends(step + 1, cut, up))(left_copy(step + 1, cut, up).start)

    def take_right(step, cut):
        across(step, cut).wait_recv()
        passed(step, cut).start()

    def take_order():
        for copy in meta_copies():
            copy.wait()
        order_pairs(
            sizes, main, lax.axis_index("kpt"), col, tiles, left_meta, right_meta, order
        )

    def send_spill():
        for up in (False, True):
            target, line = (spill_up, 3) if up else (spill_down, 2)

            @pl.when(col == (n_col - 2 if up else 1))
            def _():
                @pl.loop(0, spill)
                def _(at):
                    target[at] = side[perm[line, at] + main]

                spill_copy(up).start()

    heads = (n_col - 2) * head
    jobs = [(7, take_order)]
    if spill:
        jobs.append((heads + 0.02, send_spill))
    for cut, (low, high, kind) in enumerate(cuts):
        if kind == "rest":
            jobs.append(((n_col - 3) * head + 0.03, functools.partial(start_left, 0, cut)))
        for step in range(n_col - 1 if kind == "main" else n_col - 2):
            when = step * head + high
            if kind == "rest":
                when = heads + (step + 1) * (high - low) + 0.04
            jobs.append((when, functools.partial(take_left, step, cut)))
    for step in range(1, n_chip):
        for cut in range(RIGHT_CUTS):
            when = ((step - 1) * RIGHT_CUTS + cut + 1) * limit * sets / RIGHT_CUTS + 0.5
            jobs.append((when, functools.partial(take_right, step, cut)))
    for _, job in sorted(jobs, key=lambda entry: entry[0]):
        job()

    stages[2].wait()
    if head > main:
        for step in range(1, n_col):
            for panel, there in (
                (col - step, (col - step >= 0) & (col < n_col - 1)),
                (col + step, (col + step < n_col) & (col > 0)),
            ):
                @pl.when(there)
                def _():
                    @pl.loop(main, head)
                    def _(at):
                        left_all[panel * slots + at] = side[panel * slots + at]

    if spill:
        for up in (False, True):
            pl.when(col == (n_col - 1 if up else 0))(spill_copy(up).wait_recv)
            pl.when(col == (n_col - 2 if up else 1))(spill_copy(up).wait_send)
    own.wait()
    for step in range(1, n_chip):
        for cut in range(RIGHT_CUTS):
            across(step, cut).wait_send()
            passed(step, cut).wait()
    for cut, entry in enumerate(cuts):
        for step in range(n_col - 1 if entry[2] == "main" else n_col - 2):
            for up in (True, False):
                pl.when(left_sends(step, cut, up))(left_copy(step, cut, up).wait_send)


def product_kernel(sizes, left, right, order, out, stage, partial, out_sem):
    n_row, n_col, sets, per, ma, mb, kb_cols = sizes
    blocks = GR * kb_cols
    lines = -(-n_col * per * ma * mb // 128)
    width = stage.shape[2]
    empty = jnp.zeros(stage.shape[1:], stage.dtype)

    @pl.loop(0, order[2 * lines + 2, 0])
    def _(at):
        stage[order[2 * lines + 1, at]] = empty

    def out_copy(line):
        span = pl.ds(line * kb_cols, kb_cols)
        return pltpu.make_async_copy(stage.at[span], out.at[span], out_sem.at[line])

    count = order[2 * lines, GR - 1]

    def group(at, carry):
        line, last = carry
        codes, targets, done = [], [], []
        for lane in range(GROUP):
            spot = at * GROUP + lane
            codes.append(order[spot // 128, spot % 128])
            targets.append(order[lines + spot // 128, spot % 128])
        for code in codes:
            block = left[code // 1024]
            wide = jnp.concatenate([block[:width], block[width:]], axis=1)
            other = right[code % 1024]
            real, imag = other[:width], other[width:]
            matrix = jnp.concatenate(
                [jnp.concatenate([real, imag], axis=1), jnp.concatenate([-imag, real], axis=1)],
                axis=0,
            )
            done.append(jnp.dot(wide, matrix, preferred_element_type=jnp.float32))
        held = partial[...]
        for target, product in zip(targets, done):
            held = jnp.where(target == last, held, 0.0) + product
            value = held.astype(stage.dtype)
            stage[target, :width] = value[:, :width]
            stage[target, width:] = value[:, width:]
            last = target
        partial[...] = held
        ready = (line < GR) & (at * GROUP >= order[2 * lines, jnp.minimum(line, GR - 1)])
        pl.when(ready)(lambda: out_copy(line).start())
        return line + jnp.where(ready, 1, 0), last

    partial[...] = jnp.zeros(partial.shape, partial.dtype)
    line, _ = lax.fori_loop(
        0, (count + GROUP - 1) // GROUP, group, (jnp.int32(0), jnp.int32(-1))
    )

    @pl.loop(line, GR)
    def _(line):
        out_copy(line).start()

    @pl.loop(0, GR)
    def _(line):
        out_copy(line).wait()


def body(
    n_kpt, n_row, n_col, left_blocks, left_rows, left_count, left_level,
    right_blocks, right_cols, right_count, right_level,
):
    _, per, ma, _, width, _ = left_blocks.shape
    sets, right_per, _, mb = right_blocks.shape[:4]
    assert right_per == per and sets * n_row == n_col and n_row % 2 == 0 and sets <= 2
    blocks = GR * (n_row * sets * per // n_col)
    assert n_col * per <= 128 and per * ma <= 128 and blocks <= 128 and ma * mb <= 8
    slots = per * ma
    left = left_blocks.reshape(slots, 2 * width, width)
    right = right_blocks.reshape(sets, per * mb, 2 * width, width)
    any_space = pl.BlockSpec(memory_space=pl.ANY)
    vmem = pl.BlockSpec(memory_space=pltpu.VMEM)
    smem = pl.BlockSpec(memory_space=pltpu.SMEM)
    dma = pltpu.SemaphoreType.DMA
    n_chip = n_row // 2
    total = n_kpt * n_row * n_col
    options = variants(slots, n_col, per * mb)
    sizes = (n_row, n_col, sets, per, ma, mb, n_row * sets * per // n_col)
    tile_rows = -(-(ma + sets) // 4) * 4
    meta_rows = -(-(2 * ma + 2 * mb * sets) // 8) * 8
    lines = -(-n_col * per * ma * mb // 128)
    order_rows = -(-(2 * lines + 3) // 8) * 8
    meta, tiles, perm, choice = pl.pallas_call(
        functools.partial(plan_kernel, (n_kpt,) + sizes[:-1], options),
        out_shape=(
            jax.ShapeDtypeStruct((meta_rows, 128), jnp.int32),
            jax.ShapeDtypeStruct((total, tile_rows, 128), jnp.int32),
            jax.ShapeDtypeStruct((8, 128), jnp.int32),
            jax.ShapeDtypeStruct((1,), jnp.int32),
        ),
        in_specs=[vmem] * 6,
        out_specs=(vmem, vmem, vmem, smem),
        scratch_shapes=[pltpu.VMEM((tile_rows, 128), jnp.int32), dma((total,)), dma((total,))],
        compiler_params=pltpu.CompilerParams(collective_id=0, has_side_effects=True),
        name="plan",
    )(
        left_level[0].T, left_rows[0].T, left_count,
        right_level[:, :, 0].transpose(0, 2, 1), right_cols[:, :, 0].transpose(0, 2, 1),
        right_count.transpose(0, 2, 1),
    )

    kb_cols = sizes[-1]
    right_shape = (sets, n_row) + right.shape[1:]
    most = n_col * left.size + n_row * right.size + 24 * left.size // slots
    limit = VMEM_BYTES - most * left.dtype.itemsize

    def run(at, left, right, perm, meta, tiles):
        cuts, spill = MAIN_CUTS + 2, max(options[at][1], 1)
        left_all, right_all, order = pl.pallas_call(
            functools.partial(gather_kernel, sizes, options[at]),
            out_shape=(
                pltpu.VMEM((n_col * slots + options[at][1],) + left.shape[1:], left.dtype),
                pltpu.VMEM(right_shape, right.dtype),
                jax.ShapeDtypeStruct((order_rows, 128), jnp.int32),
            ),
            in_specs=[any_space, any_space, smem, vmem, vmem],
            out_specs=(vmem, vmem, vmem),
            scratch_shapes=[
                pltpu.VMEM(left.shape, left.dtype),
                pltpu.VMEM(right.shape, right.dtype),
                *[pltpu.VMEM(left.shape, left.dtype)] * 2,
                pltpu.VMEM(((n_col + 1) * slots,) + left.shape[1:], left.dtype),
                *[pltpu.VMEM((spill,) + left.shape[1:], left.dtype)] * 2,
                pltpu.VMEM((n_col, meta_rows, 128), jnp.int32),
                pltpu.VMEM((n_row, meta_rows, 128), jnp.int32),
                *[dma((n_col - 1, cuts))] * 4,
                *[dma((2,))] * 2,
                *[dma((n_chip - 1, RIGHT_CUTS))] * 2,
                *[dma] * 2,
                *[dma((n_chip - 1, RIGHT_CUTS))] * 2,
                *[dma((n_col - 1,))] * 2,
                *[dma((n_row - 1,))] * 2,
                *[dma] * 3,
            ],
            compiler_params=pltpu.CompilerParams(
                collective_id=1 + at, has_side_effects=True, vmem_limit_bytes=limit
            ),
            name=f"gather_panels_{at}",
        )(left, right, perm, meta, tiles)
        return pl.pallas_call(
            functools.partial(product_kernel, sizes),
            out_shape=jax.ShapeDtypeStruct((blocks, 2 * width, width), jnp.bfloat16),
            in_specs=[vmem, vmem, smem],
            out_specs=any_space,
            scratch_shapes=[
                pltpu.VMEM((blocks + 1, 2 * width, width), jnp.bfloat16),
                pltpu.VMEM((width, 2 * width), jnp.float32),
                dma((GR,)),
            ],
            compiler_params=pltpu.CompilerParams(vmem_limit_bytes=limit),
            name="pair_products",
        )(
            pltpu.with_memory_space_constraint(
                left_all, pltpu.VMEM
            ),
            pltpu.with_memory_space_constraint(
                right_all.reshape((-1,) + right.shape[2:]), pltpu.VMEM
            ),
            order,
        )

    out = lax.switch(
        choice[0], [functools.partial(run, at) for at in range(len(options))],
        left, right, perm, meta, tiles,
    )
    return out.reshape(GR, kb_cols, 2, width, width)


def solution(mesh):
    in_specs = (
        P(("kpt", "row"), "col", None, None, None, None),
        P(("kpt", "row"), "col", None),
        P(("kpt", "row"), "col"),
        P(("kpt", "row"), "col", None),
        P("kpt", "row", "col", None, None, None, None),
        P("kpt", "row", "col", None),
        P("kpt", "row", "col"),
        P("kpt", "row", "col", None),
    )
    out_specs = P(("kpt", "row"), "col", None, None, None)
    return jax.shard_map(
        functools.partial(body, mesh.shape["kpt"], mesh.shape["row"], mesh.shape["col"]),
        mesh=mesh, in_specs=in_specs, out_specs=out_specs, check_vma=False,
    )
```

```python
import functools

import jax
import jax.numpy as jnp
from jax import lax
from jax.experimental import pallas as pl
from jax.experimental.pallas import tpu as pltpu
from jax.sharding import PartitionSpec as P

GR = 8
LEVEL_CUT = 7
DEAD = -1000
GROUP = 24
MAIN_CUTS = 2
RIGHT_CUTS = 8
VMEM_BYTES = 62 * 1024 * 1024
MESH = pl.DeviceIdType.MESH
FAR = 2.0 ** 17


def variants(slots, n_col, right_slots):
    main, head = slots * 18 // 32, slots * 27 // 32
    middle, rights = slots * 30 // 32, right_slots * 56 // 64
    scale = slots * (n_col - 1) / 96
    found = [
        (main, max(1, int(spill * scale)), head, middle, rights) for spill in (5, 7, 9, 11, 13, 16)
    ]
    found.append((main, max(1, int(24 * scale)), slots, slots, right_slots))
    return found + [(slots, 0, slots, slots, right_slots)]


def ordered(levels, end, union, slots, lane_row):
    ma, per = levels.shape[0], slots // levels.shape[0]
    rows, columns = [], []
    lane = lax.broadcasted_iota(jnp.int32, (per, 128), 1)
    line = lax.broadcasted_iota(jnp.int32, (per, 128), 0)
    for m in range(ma):
        kind = jnp.where(
            levels[m:m + 1] + end >= LEVEL_CUT, 0.0,
            jnp.where(levels[m:m + 1] + union >= LEVEL_CUT, 1.0, 2.0),
        )
        key = jnp.where(lane_row < per, kind * 128.0 + lane_row * ma + m, 1024.0)
        rows.append(key)
        columns.append(jnp.sum(
            jnp.where(lane == line, jnp.broadcast_to(key, (per, 128)), 0.0), axis=1, keepdims=True
        ))
    return rows, columns


def spilled(levels, end, main):
    hits = [
        jnp.where(levels[m:m + 1] + end >= LEVEL_CUT, 1.0, 0.0) for m in range(levels.shape[0])
    ]
    size = jnp.sum(functools.reduce(jnp.add, hits), axis=1, keepdims=True)
    return jnp.maximum(size - main, 0.0)


def placed(live, per, lane, line):
    padded = live if live.shape[1] == 128 else jnp.concatenate(
        [live, jnp.zeros((1, 128 - per), jnp.float32)], axis=1
    )
    wide = jnp.broadcast_to(padded, (per, 128))
    own = jnp.sum(jnp.where(lane == line, wide, 0.0), axis=1, keepdims=True)
    first = jnp.sum(jnp.where(lane < line, wide, 0.0), axis=1, keepdims=True)
    return own, first


def plan_kernel(
    sizes, options, left,
    left_level, left_rows, left_count, right_level, right_cols, right_count,
    own_left, left_meta, right_meta, tiles, perm, choice,
    tile, meta, send, recv, lm_send, lm_recv, rm_send, rm_recv, left_sem,
):
    n_kpt, n_row, n_col, sets, per, ma, mb = sizes
    slots = per * ma
    kpt, row, col = (lax.axis_index(name) for name in ("kpt", "row", "col"))
    total = n_kpt * n_row * n_col
    me = (kpt * n_row + row) * n_col + col

    def place_of(step):
        other = (me + step) % total
        return {
            "kpt": other // (n_row * n_col), "row": (other // n_col) % n_row, "col": other % n_col
        }

    def copy_of(step):
        return pltpu.make_async_remote_copy(
            src_ref=tile, dst_ref=tiles.at[me], send_sem=send.at[step], recv_sem=recv.at[step],
            device_id=place_of(step), device_id_type=MESH,
        )

    barrier = pltpu.get_barrier_semaphore()

    @pl.loop(1, total)
    def _(step):
        pl.semaphore_signal(barrier, inc=1, device_id=place_of(step), device_id_type=MESH)

    stages = (
        pltpu.make_async_copy(left, own_left, left_sem),
    )
    for copy in stages:
        copy.start()
    tile[...] = jnp.full(tile.shape, DEAD, jnp.int32)
    live = lax.broadcasted_iota(jnp.int32, (ma, per), 0) < left_count[...]
    levels = jnp.where(live, left_level[...], DEAD)
    tile[:ma, :per] = levels
    rights = []
    for which in range(sets):
        live = lax.broadcasted_iota(jnp.int32, (mb, per), 0) < right_count[which]
        rights.append(jnp.where(live, right_level[which], DEAD))
        tile[ma + which:ma + which + 1, :per] = jnp.max(rights[-1], axis=0, keepdims=True)
        size = jnp.sum(right_count[which].astype(jnp.float32), axis=1, keepdims=True)
        tile[ma + which:ma + which + 1, 127:] = size.astype(jnp.int32)
    tiles[me] = tile[...]
    meta[...] = jnp.full(meta.shape, DEAD, jnp.int32)
    meta[:ma, :per] = levels
    meta[ma:2 * ma, :per] = left_rows[...]
    for which in range(sets):
        base = 2 * ma + which * 2 * mb
        meta[base:base + mb, :per] = right_cols[which]
        meta[base + mb:base + 2 * mb, :per] = rights[which]
    left_meta[col] = meta[...]
    right_meta[row] = meta[...]
    pl.semaphore_wait(barrier, total - 1)

    @pl.loop(1, total)
    def _(step):
        copy_of(step).start()

    def meta_copies():
        for step in range(1, n_col):
            yield pltpu.make_async_remote_copy(
                src_ref=meta, dst_ref=left_meta.at[col],
                send_sem=lm_send.at[step - 1], recv_sem=lm_recv.at[step - 1],
                device_id={"col": (col + step) % n_col}, device_id_type=MESH,
            )
        for step in range(1, n_row):
            yield pltpu.make_async_remote_copy(
                src_ref=meta, dst_ref=right_meta.at[row],
                send_sem=rm_send.at[step - 1], recv_sem=rm_recv.at[step - 1],
                device_id={"row": (row + step) % n_row}, device_id_type=MESH,
            )

    for copy in meta_copies():
        copy.start()

    @pl.loop(1, total)
    def _(step):
        copy_of(step).wait_recv()

    def at_device(k, r, c):
        return (k * n_row + r) * n_col + c

    def right_max(k, panel, q):
        return tiles[at_device(k, panel % n_row, q), pl.ds(ma + panel // n_row, 1), :]

    def measure_part(k, carry):
        most_end, most_mid, most_spill, most_right = carry
        spills = [zero, zero]
        for panel in range(n_col):
            levels = [
                jnp.concatenate(
                    [tiles[at_device(k, r, panel), pl.ds(m, 1), :] for r in range(n_row)], axis=0
                )
                for m in range(ma)
            ]

            def needed(most):
                hits = [jnp.where(level + most >= LEVEL_CUT, 1.0, 0.0) for level in levels]
                return jnp.sum(functools.reduce(jnp.add, hits), axis=1, keepdims=True)

            rights = [right_max(k, panel, q) for q in range(n_col)]
            for right in rights:
                most_right = jnp.maximum(most_right, right)
            for way, (taken, right) in enumerate(
                ((panel > 0, rights[0]), (panel < n_col - 1, rights[-1]))
            ):
                if taken:
                    wanted = needed(right)
                    most_end = jnp.maximum(most_end, wanted)
                    spills[way] = spills[way] + jnp.maximum(wanted - main, 0.0)
            if panel > 1:
                union = functools.reduce(jnp.maximum, rights[:panel])
                most_mid = jnp.maximum(most_mid, needed(union))
            if panel < n_col - 2:
                union = functools.reduce(jnp.maximum, rights[panel + 1:])
                most_mid = jnp.maximum(most_mid, needed(union))
        most_spill = jnp.maximum(most_spill, jnp.maximum(*spills))
        return most_end, most_mid, most_spill, most_right

    main = options[0][0]
    zero = jnp.zeros((n_row, 1), jnp.float32)
    most_end, most_mid, most_spill, most_right = lax.fori_loop(
        0, n_kpt, measure_part, (zero, zero, zero, jnp.zeros((1, 128), jnp.int32))
    )
    lanes = lax.broadcasted_iota(jnp.int32, (1, 128), 1)
    most_right = jnp.max(
        jnp.where(lanes == 127, most_right, 0).astype(jnp.float32), axis=1, keepdims=True
    )
    index = zero
    for _, spill, head, middle, limit in options[:-1]:
        over = (most_spill > spill) | (most_end > head) | (most_mid > middle)
        index = index + jnp.where(over | (most_right > limit), 1.0, 0.0)
    choice[0] = jnp.max(index).astype(jnp.int32)

    lane_row = lax.broadcasted_iota(jnp.int32, (1, 128), 1).astype(jnp.float32)
    line = lax.broadcasted_iota(jnp.int32, (per, 128), 0).astype(jnp.float32)
    mine = tiles[me, :ma, :]
    for at, up in enumerate((False, True)):
        which = ma + col // n_row
        near = [
            tiles[at_device(kpt, col % n_row, q), pl.ds(which, 1), :] for q in range(n_col)
        ]
        union = jnp.full((1, 128), DEAD, jnp.int32)
        for q in range(n_col):
            beyond = q > col if up else q < col
            union = jnp.maximum(union, jnp.where(beyond, near[q], DEAD))
        rows, columns = ordered(mine, near[-1] if up else near[0], union, slots, lane_row)
        found = jnp.zeros((1, 128), jnp.float32)
        for m in range(ma):
            before = [jnp.where(key < columns[m], 1.0, 0.0) for key in rows]
            rank = jnp.sum(functools.reduce(jnp.add, before), axis=1, keepdims=True)
            hit = jnp.where(rank == lane_row, line * ma + m, 0.0)
            found = found + jnp.sum(hit, axis=0, keepdims=True)
        perm[pl.ds(at, 1), :] = found.astype(jnp.int32)

    for at, up in ((2, False), (3, True)):
        panels = range(n_col - 2, -1, -1) if up else range(1, n_col)
        code, low = jnp.zeros((1, 128), jnp.float32), jnp.zeros((1, 1), jnp.float32)
        for panel in panels:
            levels = tiles[at_device(kpt, row, panel), :ma, :]
            end = right_max(kpt, panel, n_col - 1 if up else 0)
            high = low + spilled(levels, end, main)
            own = up and panel == n_col - 2
            base = (n_col if own else panel) * slots
            inside = (lane_row >= low) & (lane_row < high)
            code = code + jnp.where(inside, base + lane_row - low, 0.0)
            low = high
        perm[pl.ds(at, 1), :] = code.astype(jnp.int32)
    lane = lax.broadcasted_iota(jnp.int32, (per, 128), 1).astype(jnp.float32)
    for which in range(sets):
        live, first = placed(right_count[which].astype(jnp.float32), per, lane, line)
        found = jnp.zeros((1, 128), jnp.float32)
        for n in range(mb):
            hit = jnp.where((first + n == lane) & (live > n), line * mb + n, 0.0)
            found = found + jnp.sum(hit, axis=0, keepdims=True)
        perm[pl.ds(4 + which, 1), :] = found.astype(jnp.int32)

    for copy in meta_copies():
        copy.wait()
    for copy in stages:
        copy.wait()

    @pl.loop(1, total)
    def _(step):
        copy_of(step).wait_send()


def order_pairs(sizes, main, kpt, col, tiles, left_meta, right_meta, order):
    n_row, n_col, sets, per, ma, mb, kb_cols = sizes
    slots, high = per * ma, n_col * per
    blocks = GR * kb_cols
    lane_row = lax.broadcasted_iota(jnp.int32, (1, 128), 1).astype(jnp.float32)

    def right_max(panel, q):
        at = (kpt * n_row + panel % n_row) * n_col + q
        return tiles[at, pl.ds(ma + panel // n_row, 1), :]

    lefts = jnp.zeros((2 * ma, 128), jnp.float32)
    rights = jnp.zeros((2 * mb, 128), jnp.float32)
    places = jnp.zeros((8, 128), jnp.float32)
    spots = jnp.zeros((8, 128), jnp.float32)
    thin = lax.broadcasted_iota(jnp.int32, (per, 128), 1).astype(jnp.float32)
    thick = lax.broadcasted_iota(jnp.int32, (per, 128), 0).astype(jnp.float32)
    lows, low = [None] * n_col, jnp.zeros((1, 1), jnp.float32)
    for panel in range(1, n_col):
        lows[panel] = low
        low = low + spilled(left_meta[panel, :ma, :], right_max(panel, 0), main)
    low = jnp.zeros((1, 1), jnp.float32)
    for panel in range(n_col - 2, -1, -1):
        lows[panel] = low if lows[panel] is None else jnp.where(col == 0, lows[panel], low)
        low = low + spilled(left_meta[panel, :ma, :], right_max(panel, n_col - 1), main)
    for panel in range(n_col):
        levels = left_meta[panel, :ma, :]
        down, up = panel > col, panel < col
        end = jnp.where(down, right_max(panel, 0), right_max(panel, n_col - 1))
        union = jnp.full((1, 128), DEAD, jnp.int32)
        for q in range(n_col):
            beyond = down if q < panel else up
            if q != panel:
                union = jnp.maximum(union, jnp.where(beyond, right_max(panel, q), DEAD))
        rows, columns = ordered(levels, end, union, slots, lane_row)
        found = []
        for m in range(ma):
            before = [jnp.where(key < rows[m], 1.0, 0.0) for key in columns]
            rank = jnp.sum(functools.reduce(jnp.add, before), axis=0, keepdims=True)
            own = jnp.where(down | up, rank, lane_row * ma + m) + panel * slots
            far = (down | up) & ((col == 0) | (col == n_col - 1)) & (rank >= main)
            found.append(jnp.where(far, n_col * slots + lows[panel] + rank - main, own))
        found = jnp.concatenate(found + [jnp.zeros((8 - ma, 128), jnp.float32)], axis=0)
        base = 2 * ma + panel // n_row * 2 * mb
        here = (lane_row >= panel * per) & (lane_row < (panel + 1) * per)

        def moved(values):
            values = pltpu.roll(values, panel * per, 1) if panel else values
            return jnp.where(here, values, 0.0)

        lefts = lefts + moved(left_meta[panel, :2 * ma, :].astype(jnp.float32))
        right = right_meta[panel % n_row, base:base + 2 * mb, :].astype(jnp.float32)
        rights = rights + moved(right)
        places = places + moved(found)
        size = jnp.zeros((1, 128), jnp.float32)
        for n in range(mb):
            size = size + jnp.where((right[mb + n:mb + n + 1] > DEAD / 2) & (lane_row < per), 1.0, 0.0)
        live, _ = placed(size, per, thin, thick)
        first = jnp.sum(jnp.where(thick < thin, live, 0.0), axis=0, keepdims=True)
        spots = spots + moved(
            jnp.broadcast_to(jnp.where(lane_row < per, first, 0.0) + panel * per * mb, (8, 128))
        )

    lane = lax.broadcasted_iota(jnp.int32, (high, 128), 1)
    line = lax.broadcasted_iota(jnp.int32, (high, 128), 0)

    def column(values):
        wide = jnp.broadcast_to(values, (high, 128))
        return jnp.sum(jnp.where(lane == line, wide, 0.0), axis=1, keepdims=True)

    keys, key_columns, code_columns, target_columns = [], [], [], []
    for m in range(ma):
        for n in range(mb):
            kept = lefts[m:m + 1] + rights[mb + n:mb + n + 1] >= LEVEL_CUT
            target = lefts[ma + m:ma + m + 1] * kb_cols + rights[n:n + 1]
            spot = lane_row + (m * mb + n) * 128.0
            key = jnp.where(kept, target * 1024.0 + spot, FAR + spot)
            keys.append(jnp.where(lane_row < high, key, 2 * FAR))
            key_columns.append(column(keys[-1]))
            code = places[m:m + 1] * 1024.0 + spots[:1] + n
            code_columns.append(column(jnp.where(kept, code, 0.0)))
            target_columns.append(column(jnp.where(kept, target, 1.0 * blocks)))
    ranks = []
    for mine in key_columns:
        before = [jnp.where(key < mine, 1.0, 0.0) for key in keys]
        ranks.append(jnp.sum(functools.reduce(jnp.add, before), axis=1, keepdims=True))

    def gathered(hits):
        return jnp.sum(functools.reduce(jnp.add, hits), axis=0, keepdims=True)

    def write(at, values):
        order[pl.ds(at, 1), :] = values.astype(jnp.int32)

    lines = -(-high * ma * mb // 128)
    for at in range(lines):
        spot = lane_row + at * 128.0
        for base, columns in ((0, code_columns), (lines, target_columns)):
            write(base + at, gathered([
                jnp.where(rank == spot, values, 0.0) for rank, values in zip(ranks, columns)
            ]))
    bound = (lane_row + 1.0) * (kb_cols * 1024.0)
    write(2 * lines, gathered([jnp.where(mine < bound, 1.0, 0.0) for mine in key_columns]))
    filled = gathered([jnp.where(mine == lane_row, 1.0, 0.0) for mine in target_columns])
    empty = jnp.where((filled < 0.5) & (lane_row < blocks), 1.0, 0.0)
    lane = lax.broadcasted_iota(jnp.int32, (128, 128), 1).astype(jnp.float32)
    line = lax.broadcasted_iota(jnp.int32, (128, 128), 0).astype(jnp.float32)
    wide = jnp.broadcast_to(empty, (128, 128))
    rank = jnp.sum(jnp.where(lane < line, wide, 0.0), axis=1, keepdims=True)
    flag = jnp.sum(jnp.where(lane == line, wide, 0.0), axis=1, keepdims=True)
    size = jnp.broadcast_to(jnp.sum(empty, axis=1, keepdims=True), (1, 128))
    listed = gathered([jnp.where(rank == lane, line * flag, 0.0)])
    write(2 * lines + 1, jnp.where(lane_row < size, listed, 1.0 * blocks))
    write(2 * lines + 2, size)


def gather_kernel(
    sizes, option, left, own_left, right, perm, left_meta, right_meta, tiles,
    left_all, right_all, order,
    own_right, packed_down, packed_up, side, spill_down, spill_up,
    up_send, up_recv, down_send, down_recv, spill_send, spill_recv,
    x_send, x_recv, own_send, own_recv, pass_send, pass_recv,
    left_sem, right_sem,
):
    n_row, n_col, sets = sizes[:3]
    row = lax.axis_index("row")
    col = lax.axis_index("col")
    n_chip = n_row // 2
    chip, core = row // 2, row % 2
    partner = chip * 2 + 1 - core
    slots = left.shape[0]
    main, spill, head, middle, limit = option

    barrier = pltpu.get_barrier_semaphore()
    for there, step in ((col > 0, -1), (col + 1 < n_col, 1)):
        @pl.when(there)
        def _():
            pl.semaphore_signal(
                barrier, inc=1, device_id={"col": col + step}, device_id_type=MESH
            )
    others = [partner] + [((chip + step) % n_chip) * 2 + core for step in range(1, n_chip)]
    for other in others:
        pl.semaphore_signal(barrier, inc=1, device_id={"row": other}, device_id_type=MESH)
    kept = pltpu.make_async_copy(left, left_all.at[pl.ds(col * slots, slots)], left_sem)
    kept.start()

    bounds = [main * at // MAIN_CUTS for at in range(MAIN_CUTS + 1)]
    cuts = [(low, high, "main") for low, high in zip(bounds, bounds[1:])]
    if head > main:
        cuts.append((main, head, "side"))
    if middle > head:
        cuts.append((head, middle, "rest"))
    bounds = [limit * at // RIGHT_CUTS for at in range(RIGHT_CUTS + 1)]
    right_cuts = [pl.ds(low, high - low) for low, high in zip(bounds, bounds[1:])]

    def left_copy(step, cut, up):
        low, high, kind = cuts[cut]
        panel = col - step if up else col + step
        span = pl.ds(panel * slots + low, high - low)
        target = side.at[span] if kind == "side" else left_all.at[span]
        source = (packed_up if up else packed_down).at[pl.ds(low, high - low)]
        send, recv = (up_send, up_recv) if up else (down_send, down_recv)
        return pltpu.make_async_remote_copy(
            src_ref=source if step == 0 else target, dst_ref=target,
            send_sem=send.at[step, cut], recv_sem=recv.at[step, cut],
            device_id={"col": col + 1 if up else col - 1}, device_id_type=MESH,
        )

    def left_sends(step, cut, up):
        mid = 0 if cuts[cut][2] == "main" else 1
        if up:
            return (col + 1 < n_col - mid) & (col - step >= 0)
        return (col - 1 >= mid) & (col + step < n_col)

    def left_receives(step, cut, up):
        mid = 0 if cuts[cut][2] == "main" else 1
        if up:
            return (col - 1 - step >= 0) & (col < n_col - mid)
        return (col + 1 + step < n_col) & (col >= mid)

    def start_left(step, cut):
        for up in (True, False):
            pl.when(left_sends(step, cut, up))(left_copy(step, cut, up).start)

    def spill_copy(up):
        return pltpu.make_async_remote_copy(
            src_ref=spill_up if up else spill_down,
            dst_ref=left_all.at[pl.ds(n_col * slots, spill)],
            send_sem=spill_send.at[int(up)], recv_sem=spill_recv.at[int(up)],
            device_id={"col": n_col - 1 if up else 0}, device_id_type=MESH,
        )

    def across(step, cut):
        span = right_cuts[cut]
        other = ((chip + step) % n_chip) * 2 + core
        return pltpu.make_async_remote_copy(
            src_ref=right_all.at[:, row, span], dst_ref=right_all.at[:, row, span],
            send_sem=x_send.at[step - 1, cut], recv_sem=x_recv.at[step - 1, cut],
            device_id={"row": other}, device_id_type=MESH,
        )

    def passed(step, cut):
        span = right_cuts[cut]
        panel = ((chip + n_chip - step) % n_chip) * 2 + core
        return pltpu.make_async_remote_copy(
            src_ref=right_all.at[:, panel, span], dst_ref=right_all.at[:, panel, span],
            send_sem=pass_send.at[step - 1, cut], recv_sem=pass_recv.at[step - 1, cut],
            device_id={"row": partner}, device_id_type=MESH,
        )

    own = pltpu.make_async_remote_copy(
        src_ref=right_all.at[:, row, pl.ds(0, limit)],
        dst_ref=right_all.at[:, row, pl.ds(0, limit)],
        send_sem=own_send, recv_sem=own_recv,
        device_id={"row": partner}, device_id_type=MESH,
    )

    def pack_left(low, high):
        @pl.loop(low, high)
        def _(at):
            packed_down[at] = own_left[perm[0, at]]
            packed_up[at] = own_left[perm[1, at]]

    pack_left(*cuts[0][:2])
    pl.semaphore_wait(
        barrier, len(others) + jnp.where(col > 0, 1, 0) + jnp.where(col + 1 < n_col, 1, 0)
    )
    start_left(0, 0)
    staged = pltpu.make_async_copy(right, own_right, right_sem)
    staged.start()
    pack_left(cuts[0][1], middle)
    for cut in range(1, len(cuts)):
        if cuts[cut][2] != "rest":
            start_left(0, cut)

    staged.wait()
    for which in range(sets):
        @pl.loop(0, limit)
        def _(at):
            right_all[which, row, at] = own_right[which, perm[4 + which, at]]

    for step in range(1, n_chip):
        for cut in range(RIGHT_CUTS):
            across(step, cut).start()
    own.start()
    if spill:
        @pl.loop(main, head)
        def _(at):
            side[col * slots + at] = packed_down[at]
            side[n_col * slots + at] = packed_up[at]

    def take_left(step, cut):
        for up in (True, False):
            pl.when(left_receives(step, cut, up))(left_copy(step, cut, up).wait_recv)
            if step + 1 < n_col - 1:
                pl.when(left_sends(step + 1, cut, up))(left_copy(step + 1, cut, up).start)

    def take_right(step, cut):
        across(step, cut).wait_recv()
        passed(step, cut).start()

    def take_order():
        order_pairs(
            sizes, main, lax.axis_index("kpt"), col, tiles, left_meta, right_meta, order
        )

    def send_spill():
        for up in (False, True):
            target, line = (spill_up, 3) if up else (spill_down, 2)

            @pl.when(col == (n_col - 2 if up else 1))
            def _():
                @pl.loop(0, spill)
                def _(at):
                    target[at] = side[perm[line, at] + main]

                spill_copy(up).start()

    heads = (n_col - 2) * head
    jobs = [(7, take_order)]
    if spill:
        jobs.append((heads + 0.02, send_spill))
    for cut, (low, high, kind) in enumerate(cuts):
        if kind == "rest":
            jobs.append(((n_col - 3) * head + 0.03, functools.partial(start_left, 0, cut)))
        for step in range(n_col - 1 if kind == "main" else n_col - 2):
            when = step * head + high
            if kind == "rest":
                when = heads + (step + 1) * (high - low) + 0.04
            jobs.append((when, functools.partial(take_left, step, cut)))
    for step in range(1, n_chip):
        for cut in range(RIGHT_CUTS):
            when = ((step - 1) * RIGHT_CUTS + cut + 1) * limit * sets / RIGHT_CUTS + 0.5
            jobs.append((when, functools.partial(take_right, step, cut)))
    for _, job in sorted(jobs, key=lambda entry: entry[0]):
        job()

    kept.wait()
    if head > main:
        for step in range(1, n_col):
            for panel, there in (
                (col - step, (col - step >= 0) & (col < n_col - 1)),
                (col + step, (col + step < n_col) & (col > 0)),
            ):
                @pl.when(there)
                def _():
                    @pl.loop(main, head)
                    def _(at):
                        left_all[panel * slots + at] = side[panel * slots + at]

    if spill:
        for up in (False, True):
            pl.when(col == (n_col - 1 if up else 0))(spill_copy(up).wait_recv)
            pl.when(col == (n_col - 2 if up else 1))(spill_copy(up).wait_send)
    own.wait()
    for step in range(1, n_chip):
        for cut in range(RIGHT_CUTS):
            across(step, cut).wait_send()
            passed(step, cut).wait()
    for cut, entry in enumerate(cuts):
        for step in range(n_col - 1 if entry[2] == "main" else n_col - 2):
            for up in (True, False):
                pl.when(left_sends(step, cut, up))(left_copy(step, cut, up).wait_send)


def product_kernel(sizes, left, right, order, out, stage, partial, out_sem):
    n_row, n_col, sets, per, ma, mb, kb_cols = sizes
    blocks = GR * kb_cols
    lines = -(-n_col * per * ma * mb // 128)
    width = stage.shape[2]
    empty = jnp.zeros(stage.shape[1:], stage.dtype)

    @pl.loop(0, (order[2 * lines + 2, 0] + 3) // 4)
    def _(at):
        for lane in range(4):
            stage[order[2 * lines + 1, at * 4 + lane]] = empty

    def out_copy(line):
        span = pl.ds(line * kb_cols, kb_cols)
        return pltpu.make_async_copy(stage.at[span], out.at[span], out_sem.at[line])

    count = order[2 * lines, GR - 1]

    def group(at, carry):
        line, last = carry
        codes, targets, done = [], [], []
        for lane in range(GROUP):
            spot = at * GROUP + lane
            codes.append(order[spot // 128, spot % 128])
            targets.append(order[lines + spot // 128, spot % 128])
        for code in codes:
            block = left[code // 1024]
            wide = jnp.concatenate([block[:width], block[width:]], axis=1)
            other = right[code % 1024]
            real, imag = other[:width], other[width:]
            matrix = jnp.concatenate(
                [jnp.concatenate([real, imag], axis=1), jnp.concatenate([-imag, real], axis=1)],
                axis=0,
            )
            done.append(jnp.dot(wide, matrix, preferred_element_type=jnp.float32))
        held = partial[...]
        for target, product in zip(targets, done):
            held = jnp.where(target == last, held, 0.0) + product
            value = held.astype(stage.dtype)
            stage[target, :width] = value[:, :width]
            stage[target, width:] = value[:, width:]
            last = target
        partial[...] = held
        for _ in range(1 + GROUP // 12):
            ready = (line < GR) & (at * GROUP >= order[2 * lines, jnp.minimum(line, GR - 1)])
            pl.when(ready)(out_copy(jnp.minimum(line, GR - 1)).start)
            line = line + jnp.where(ready, 1, 0)
        return line, last

    partial[...] = jnp.zeros(partial.shape, partial.dtype)
    line, _ = lax.fori_loop(
        0, (count + GROUP - 1) // GROUP, group, (jnp.int32(0), jnp.int32(-1))
    )

    @pl.loop(line, GR)
    def _(line):
        out_copy(line).start()

    @pl.loop(0, GR)
    def _(line):
        out_copy(line).wait()


def body(
    n_kpt, n_row, n_col, left_blocks, left_rows, left_count, left_level,
    right_blocks, right_cols, right_count, right_level,
):
    _, per, ma, _, width, _ = left_blocks.shape
    sets, right_per, _, mb = right_blocks.shape[:4]
    assert right_per == per and sets * n_row == n_col and n_row % 2 == 0 and sets <= 2
    blocks = GR * (n_row * sets * per // n_col)
    assert n_col * per <= 128 and per * ma <= 128 and blocks <= 128 and ma * mb <= 8
    slots = per * ma
    left = left_blocks.reshape(slots, 2 * width, width)
    right = right_blocks.reshape(sets, per * mb, 2 * width, width)
    any_space = pl.BlockSpec(memory_space=pl.ANY)
    vmem = pl.BlockSpec(memory_space=pltpu.VMEM)
    smem = pl.BlockSpec(memory_space=pltpu.SMEM)
    dma = pltpu.SemaphoreType.DMA
    n_chip = n_row // 2
    total = n_kpt * n_row * n_col
    options = variants(slots, n_col, per * mb)
    sizes = (n_row, n_col, sets, per, ma, mb, n_row * sets * per // n_col)
    tile_rows = -(-(ma + sets) // 4) * 4
    meta_rows = -(-(2 * ma + 2 * mb * sets) // 8) * 8
    lines = -(-n_col * per * ma * mb // 128)
    order_rows = -(-(2 * lines + 3) // 8) * 8
    own_left, left_meta, right_meta, tiles, perm, choice = pl.pallas_call(
        functools.partial(plan_kernel, (n_kpt,) + sizes[:-1], options),
        out_shape=(
            pltpu.VMEM(left.shape, left.dtype),
            jax.ShapeDtypeStruct((n_col, meta_rows, 128), jnp.int32),
            jax.ShapeDtypeStruct((n_row, meta_rows, 128), jnp.int32),
            jax.ShapeDtypeStruct((total, tile_rows, 128), jnp.int32),
            jax.ShapeDtypeStruct((8, 128), jnp.int32),
            jax.ShapeDtypeStruct((1,), jnp.int32),
        ),
        in_specs=[any_space] + [vmem] * 6,
        out_specs=(vmem,) * 5 + (smem,),
        scratch_shapes=[
            pltpu.VMEM((tile_rows, 128), jnp.int32),
            pltpu.VMEM((meta_rows, 128), jnp.int32),
            *[dma((total,))] * 2,
            *[dma((n_col - 1,))] * 2,
            *[dma((n_row - 1,))] * 2,
            dma,
        ],
        compiler_params=pltpu.CompilerParams(collective_id=0, has_side_effects=True),
        name="plan",
    )(
        left, left_level[0].T, left_rows[0].T, left_count,
        right_level[:, :, 0].transpose(0, 2, 1), right_cols[:, :, 0].transpose(0, 2, 1),
        right_count.transpose(0, 2, 1),
    )

    kb_cols = sizes[-1]
    right_shape = (sets, n_row) + right.shape[1:]
    most = (n_col + 1) * left.size + n_row * right.size + 24 * left.size // slots
    limit = VMEM_BYTES - most * left.dtype.itemsize

    def run(at, left, own_left, right, perm, left_meta, right_meta, tiles):
        cuts, spill = MAIN_CUTS + 2, max(options[at][1], 1)
        left_all, right_all, order = pl.pallas_call(
            functools.partial(gather_kernel, sizes, options[at]),
            out_shape=(
                pltpu.VMEM((n_col * slots + options[at][1],) + left.shape[1:], left.dtype),
                pltpu.VMEM(right_shape, right.dtype),
                jax.ShapeDtypeStruct((order_rows, 128), jnp.int32),
            ),
            in_specs=[any_space, vmem, any_space, smem, vmem, vmem, vmem],
            out_specs=(vmem, vmem, vmem),
            scratch_shapes=[
                pltpu.VMEM(right.shape, right.dtype),
                *[pltpu.VMEM(left.shape, left.dtype)] * 2,
                pltpu.VMEM(((n_col + 1) * slots,) + left.shape[1:], left.dtype),
                *[pltpu.VMEM((spill,) + left.shape[1:], left.dtype)] * 2,
                *[dma((n_col - 1, cuts))] * 4,
                *[dma((2,))] * 2,
                *[dma((n_chip - 1, RIGHT_CUTS))] * 2,
                *[dma] * 2,
                *[dma((n_chip - 1, RIGHT_CUTS))] * 2,
                *[dma] * 2,
            ],
            compiler_params=pltpu.CompilerParams(
                collective_id=1 + at, has_side_effects=True, vmem_limit_bytes=limit
            ),
            name=f"gather_panels_{at}",
        )(
            left, pltpu.with_memory_space_constraint(own_left, pltpu.VMEM),
            right, perm, left_meta, right_meta, tiles,
        )
        return pl.pallas_call(
            functools.partial(product_kernel, sizes),
            out_shape=jax.ShapeDtypeStruct((blocks, 2 * width, width), jnp.bfloat16),
            in_specs=[vmem, vmem, smem],
            out_specs=any_space,
            scratch_shapes=[
                pltpu.VMEM((blocks + 1, 2 * width, width), jnp.bfloat16),
                pltpu.VMEM((width, 2 * width), jnp.float32),
                dma((GR,)),
            ],
            compiler_params=pltpu.CompilerParams(vmem_limit_bytes=limit),
            name="pair_products",
        )(
            pltpu.with_memory_space_constraint(
                left_all, pltpu.VMEM
            ),
            pltpu.with_memory_space_constraint(
                right_all.reshape((-1,) + right.shape[2:]), pltpu.VMEM
            ),
            order,
        )

    out = lax.switch(
        choice[0], [functools.partial(run, at) for at in range(len(options))],
        left, own_left, right, perm, left_meta, right_meta, tiles,
    )
    return out.reshape(GR, kb_cols, 2, width, width)


def solution(mesh):
    in_specs = (
        P(("kpt", "row"), "col", None, None, None, None),
        P(("kpt", "row"), "col", None),
        P(("kpt", "row"), "col"),
        P(("kpt", "row"), "col", None),
        P("kpt", "row", "col", None, None, None, None),
        P("kpt", "row", "col", None),
        P("kpt", "row", "col"),
        P("kpt", "row", "col", None),
    )
    out_specs = P(("kpt", "row"), "col", None, None, None)
    return jax.shard_map(
        functools.partial(body, mesh.shape["kpt"], mesh.shape["row"], mesh.shape["col"]),
        mesh=mesh, in_specs=in_specs, out_specs=out_specs, check_vma=False,
    )
```

```python
import functools

import jax
import jax.numpy as jnp
from jax import lax
from jax.experimental import pallas as pl
from jax.experimental.pallas import tpu as pltpu
from jax.sharding import PartitionSpec as P

GR = 8
LEVEL_CUT = 7
DEAD = -1000
GROUP = 24
MAIN_CUTS = 2
RIGHT_CUTS = 8
VMEM_BYTES = 62 * 1024 * 1024
MESH = pl.DeviceIdType.MESH
FAR = 2.0 ** 17


def variants(slots, n_col, right_slots):
    scale = slots * (n_col - 1) / 96
    found = []
    for spill, head, middle, rights in (
        (5, 25, 28, 52), (7, 26, 28, 54), (9, 26, 29, 54), (11, 26, 30, 56), (13, 27, 30, 56),
        (16, 28, 30, 58), (24, 32, 32, 64),
    ):
        found.append((
            slots * 18 // 32, max(1, int(spill * scale)), slots * head // 32,
            slots * middle // 32, right_slots * rights // 64,
        ))
    return found + [(slots, 0, slots, slots, right_slots)]


def ordered(levels, end, union, slots, lane_row):
    ma, per = levels.shape[0], slots // levels.shape[0]
    rows, columns = [], []
    lane = lax.broadcasted_iota(jnp.int32, (per, 128), 1)
    line = lax.broadcasted_iota(jnp.int32, (per, 128), 0)
    for m in range(ma):
        kind = jnp.where(
            levels[m:m + 1] + end >= LEVEL_CUT, 0.0,
            jnp.where(levels[m:m + 1] + union >= LEVEL_CUT, 1.0, 2.0),
        )
        key = jnp.where(lane_row < per, kind * 128.0 + lane_row * ma + m, 1024.0)
        rows.append(key)
        columns.append(jnp.sum(
            jnp.where(lane == line, jnp.broadcast_to(key, (per, 128)), 0.0), axis=1, keepdims=True
        ))
    return rows, columns


def spilled(levels, end, main):
    hits = [
        jnp.where(levels[m:m + 1] + end >= LEVEL_CUT, 1.0, 0.0) for m in range(levels.shape[0])
    ]
    size = jnp.sum(functools.reduce(jnp.add, hits), axis=1, keepdims=True)
    return jnp.maximum(size - main, 0.0)


def placed(live, per, lane, line):
    padded = live if live.shape[1] == 128 else jnp.concatenate(
        [live, jnp.zeros((1, 128 - per), jnp.float32)], axis=1
    )
    wide = jnp.broadcast_to(padded, (per, 128))
    own = jnp.sum(jnp.where(lane == line, wide, 0.0), axis=1, keepdims=True)
    first = jnp.sum(jnp.where(lane < line, wide, 0.0), axis=1, keepdims=True)
    return own, first


def plan_kernel(
    sizes, options, left,
    left_level, left_rows, left_count, right_level, right_cols, right_count,
    own_left, left_meta, right_meta, tiles, perm, choice,
    tile, meta, send, recv, lm_send, lm_recv, rm_send, rm_recv, left_sem,
):
    n_kpt, n_row, n_col, sets, per, ma, mb = sizes
    slots = per * ma
    kpt, row, col = (lax.axis_index(name) for name in ("kpt", "row", "col"))
    total = n_kpt * n_row * n_col
    me = (kpt * n_row + row) * n_col + col

    def place_of(step):
        other = (me + step) % total
        return {
            "kpt": other // (n_row * n_col), "row": (other // n_col) % n_row, "col": other % n_col
        }

    def copy_of(step):
        return pltpu.make_async_remote_copy(
            src_ref=tile, dst_ref=tiles.at[me], send_sem=send.at[step], recv_sem=recv.at[step],
            device_id=place_of(step), device_id_type=MESH,
        )

    barrier = pltpu.get_barrier_semaphore()

    @pl.loop(1, total)
    def _(step):
        pl.semaphore_signal(barrier, inc=1, device_id=place_of(step), device_id_type=MESH)

    stages = (
        pltpu.make_async_copy(left, own_left, left_sem),
    )
    for copy in stages:
        copy.start()
    tile[...] = jnp.full(tile.shape, DEAD, jnp.int32)
    live = lax.broadcasted_iota(jnp.int32, (ma, per), 0) < left_count[...]
    levels = jnp.where(live, left_level[...], DEAD)
    tile[:ma, :per] = levels
    rights = []
    for which in range(sets):
        live = lax.broadcasted_iota(jnp.int32, (mb, per), 0) < right_count[which]
        rights.append(jnp.where(live, right_level[which], DEAD))
        tile[ma + which:ma + which + 1, :per] = jnp.max(rights[-1], axis=0, keepdims=True)
        size = jnp.sum(right_count[which].astype(jnp.float32), axis=1, keepdims=True)
        tile[ma + which:ma + which + 1, 127:] = size.astype(jnp.int32)
    tiles[me] = tile[...]
    meta[...] = jnp.full(meta.shape, DEAD, jnp.int32)
    meta[:ma, :per] = levels
    meta[ma:2 * ma, :per] = left_rows[...]
    for which in range(sets):
        base = 2 * ma + which * 2 * mb
        meta[base:base + mb, :per] = right_cols[which]
        meta[base + mb:base + 2 * mb, :per] = rights[which]
    left_meta[col] = meta[...]
    right_meta[row] = meta[...]
    pl.semaphore_wait(barrier, total - 1)

    @pl.loop(1, total)
    def _(step):
        copy_of(step).start()

    def meta_copies():
        for step in range(1, n_col):
            yield pltpu.make_async_remote_copy(
                src_ref=meta, dst_ref=left_meta.at[col],
                send_sem=lm_send.at[step - 1], recv_sem=lm_recv.at[step - 1],
                device_id={"col": (col + step) % n_col}, device_id_type=MESH,
            )
        for step in range(1, n_row):
            yield pltpu.make_async_remote_copy(
                src_ref=meta, dst_ref=right_meta.at[row],
                send_sem=rm_send.at[step - 1], recv_sem=rm_recv.at[step - 1],
                device_id={"row": (row + step) % n_row}, device_id_type=MESH,
            )

    for copy in meta_copies():
        copy.start()

    @pl.loop(1, total)
    def _(step):
        copy_of(step).wait_recv()

    def at_device(k, r, c):
        return (k * n_row + r) * n_col + c

    def right_max(k, panel, q):
        return tiles[at_device(k, panel % n_row, q), pl.ds(ma + panel // n_row, 1), :]

    def measure_part(k, carry):
        most_end, most_mid, most_spill, most_right = carry
        spills = [zero, zero]
        for panel in range(n_col):
            levels = [
                jnp.concatenate(
                    [tiles[at_device(k, r, panel), pl.ds(m, 1), :] for r in range(n_row)], axis=0
                )
                for m in range(ma)
            ]

            def needed(most):
                hits = [jnp.where(level + most >= LEVEL_CUT, 1.0, 0.0) for level in levels]
                return jnp.sum(functools.reduce(jnp.add, hits), axis=1, keepdims=True)

            rights = [right_max(k, panel, q) for q in range(n_col)]
            for right in rights:
                most_right = jnp.maximum(most_right, right)
            for way, (taken, right) in enumerate(
                ((panel > 0, rights[0]), (panel < n_col - 1, rights[-1]))
            ):
                if taken:
                    wanted = needed(right)
                    most_end = jnp.maximum(most_end, wanted)
                    spills[way] = spills[way] + jnp.maximum(wanted - main, 0.0)
            if panel > 1:
                union = functools.reduce(jnp.maximum, rights[:panel])
                most_mid = jnp.maximum(most_mid, needed(union))
            if panel < n_col - 2:
                union = functools.reduce(jnp.maximum, rights[panel + 1:])
                most_mid = jnp.maximum(most_mid, needed(union))
        most_spill = jnp.maximum(most_spill, jnp.maximum(*spills))
        return most_end, most_mid, most_spill, most_right

    main = options[0][0]
    zero = jnp.zeros((n_row, 1), jnp.float32)
    most_end, most_mid, most_spill, most_right = lax.fori_loop(
        0, n_kpt, measure_part, (zero, zero, zero, jnp.zeros((1, 128), jnp.int32))
    )
    lanes = lax.broadcasted_iota(jnp.int32, (1, 128), 1)
    most_right = jnp.max(
        jnp.where(lanes == 127, most_right, 0).astype(jnp.float32), axis=1, keepdims=True
    )
    index = zero
    for _, spill, head, middle, limit in options[:-1]:
        over = (most_spill > spill) | (most_end > head) | (most_mid > middle)
        index = index + jnp.where(over | (most_right > limit), 1.0, 0.0)
    choice[0] = jnp.max(index).astype(jnp.int32)

    lane_row = lax.broadcasted_iota(jnp.int32, (1, 128), 1).astype(jnp.float32)
    line = lax.broadcasted_iota(jnp.int32, (per, 128), 0).astype(jnp.float32)
    mine = tiles[me, :ma, :]
    for at, up in enumerate((False, True)):
        which = ma + col // n_row
        near = [
            tiles[at_device(kpt, col % n_row, q), pl.ds(which, 1), :] for q in range(n_col)
        ]
        union = jnp.full((1, 128), DEAD, jnp.int32)
        for q in range(n_col):
            beyond = q > col if up else q < col
            union = jnp.maximum(union, jnp.where(beyond, near[q], DEAD))
        rows, columns = ordered(mine, near[-1] if up else near[0], union, slots, lane_row)
        found = jnp.zeros((1, 128), jnp.float32)
        for m in range(ma):
            before = [jnp.where(key < columns[m], 1.0, 0.0) for key in rows]
            rank = jnp.sum(functools.reduce(jnp.add, before), axis=1, keepdims=True)
            hit = jnp.where(rank == lane_row, line * ma + m, 0.0)
            found = found + jnp.sum(hit, axis=0, keepdims=True)
        perm[pl.ds(at, 1), :] = found.astype(jnp.int32)

    for at, up in ((2, False), (3, True)):
        panels = range(n_col - 2, -1, -1) if up else range(1, n_col)
        code, low = jnp.zeros((1, 128), jnp.float32), jnp.zeros((1, 1), jnp.float32)
        for panel in panels:
            levels = tiles[at_device(kpt, row, panel), :ma, :]
            end = right_max(kpt, panel, n_col - 1 if up else 0)
            high = low + spilled(levels, end, main)
            own = up and panel == n_col - 2
            base = (n_col if own else panel) * slots
            inside = (lane_row >= low) & (lane_row < high)
            code = code + jnp.where(inside, base + lane_row - low, 0.0)
            low = high
        perm[pl.ds(at, 1), :] = code.astype(jnp.int32)
    lane = lax.broadcasted_iota(jnp.int32, (per, 128), 1).astype(jnp.float32)
    for which in range(sets):
        live, first = placed(right_count[which].astype(jnp.float32), per, lane, line)
        found = jnp.zeros((1, 128), jnp.float32)
        for n in range(mb):
            hit = jnp.where((first + n == lane) & (live > n), line * mb + n, 0.0)
            found = found + jnp.sum(hit, axis=0, keepdims=True)
        perm[pl.ds(4 + which, 1), :] = found.astype(jnp.int32)

    for copy in meta_copies():
        copy.wait()
    for copy in stages:
        copy.wait()

    @pl.loop(1, total)
    def _(step):
        copy_of(step).wait_send()


def order_pairs(sizes, main, kpt, col, tiles, left_meta, right_meta, order):
    n_row, n_col, sets, per, ma, mb, kb_cols = sizes
    slots, high = per * ma, n_col * per
    blocks = GR * kb_cols
    lane_row = lax.broadcasted_iota(jnp.int32, (1, 128), 1).astype(jnp.float32)

    def right_max(panel, q):
        at = (kpt * n_row + panel % n_row) * n_col + q
        return tiles[at, pl.ds(ma + panel // n_row, 1), :]

    lefts = jnp.zeros((2 * ma, 128), jnp.float32)
    rights = jnp.zeros((2 * mb, 128), jnp.float32)
    places = jnp.zeros((8, 128), jnp.float32)
    spots = jnp.zeros((8, 128), jnp.float32)
    thin = lax.broadcasted_iota(jnp.int32, (per, 128), 1).astype(jnp.float32)
    thick = lax.broadcasted_iota(jnp.int32, (per, 128), 0).astype(jnp.float32)
    lows, low = [None] * n_col, jnp.zeros((1, 1), jnp.float32)
    for panel in range(1, n_col):
        lows[panel] = low
        low = low + spilled(left_meta[panel, :ma, :], right_max(panel, 0), main)
    low = jnp.zeros((1, 1), jnp.float32)
    for panel in range(n_col - 2, -1, -1):
        lows[panel] = low if lows[panel] is None else jnp.where(col == 0, lows[panel], low)
        low = low + spilled(left_meta[panel, :ma, :], right_max(panel, n_col - 1), main)
    for panel in range(n_col):
        levels = left_meta[panel, :ma, :]
        down, up = panel > col, panel < col
        end = jnp.where(down, right_max(panel, 0), right_max(panel, n_col - 1))
        union = jnp.full((1, 128), DEAD, jnp.int32)
        for q in range(n_col):
            beyond = down if q < panel else up
            if q != panel:
                union = jnp.maximum(union, jnp.where(beyond, right_max(panel, q), DEAD))
        rows, columns = ordered(levels, end, union, slots, lane_row)
        found = []
        for m in range(ma):
            before = [jnp.where(key < rows[m], 1.0, 0.0) for key in columns]
            rank = jnp.sum(functools.reduce(jnp.add, before), axis=0, keepdims=True)
            own = jnp.where(down | up, rank, lane_row * ma + m) + panel * slots
            far = (down | up) & ((col == 0) | (col == n_col - 1)) & (rank >= main)
            found.append(jnp.where(far, n_col * slots + lows[panel] + rank - main, own))
        found = jnp.concatenate(found + [jnp.zeros((8 - ma, 128), jnp.float32)], axis=0)
        base = 2 * ma + panel // n_row * 2 * mb
        here = (lane_row >= panel * per) & (lane_row < (panel + 1) * per)

        def moved(values):
            values = pltpu.roll(values, panel * per, 1) if panel else values
            return jnp.where(here, values, 0.0)

        lefts = lefts + moved(left_meta[panel, :2 * ma, :].astype(jnp.float32))
        right = right_meta[panel % n_row, base:base + 2 * mb, :].astype(jnp.float32)
        rights = rights + moved(right)
        places = places + moved(found)
        size = jnp.zeros((1, 128), jnp.float32)
        for n in range(mb):
            size = size + jnp.where((right[mb + n:mb + n + 1] > DEAD / 2) & (lane_row < per), 1.0, 0.0)
        live, _ = placed(size, per, thin, thick)
        first = jnp.sum(jnp.where(thick < thin, live, 0.0), axis=0, keepdims=True)
        spots = spots + moved(
            jnp.broadcast_to(jnp.where(lane_row < per, first, 0.0) + panel * per * mb, (8, 128))
        )

    lane = lax.broadcasted_iota(jnp.int32, (high, 128), 1)
    line = lax.broadcasted_iota(jnp.int32, (high, 128), 0)

    def column(values):
        wide = jnp.broadcast_to(values, (high, 128))
        return jnp.sum(jnp.where(lane == line, wide, 0.0), axis=1, keepdims=True)

    keys, key_columns, code_columns, target_columns = [], [], [], []
    for m in range(ma):
        for n in range(mb):
            kept = lefts[m:m + 1] + rights[mb + n:mb + n + 1] >= LEVEL_CUT
            target = lefts[ma + m:ma + m + 1] * kb_cols + rights[n:n + 1]
            spot = lane_row + (m * mb + n) * 128.0
            key = jnp.where(kept, target * 1024.0 + spot, FAR + spot)
            keys.append(jnp.where(lane_row < high, key, 2 * FAR))
            key_columns.append(column(keys[-1]))
            code = places[m:m + 1] * 1024.0 + spots[:1] + n
            code_columns.append(column(jnp.where(kept, code, 0.0)))
            target_columns.append(column(jnp.where(kept, target, 1.0 * blocks)))
    ranks = []
    for mine in key_columns:
        before = [jnp.where(key < mine, 1.0, 0.0) for key in keys]
        ranks.append(jnp.sum(functools.reduce(jnp.add, before), axis=1, keepdims=True))

    def gathered(hits):
        return jnp.sum(functools.reduce(jnp.add, hits), axis=0, keepdims=True)

    def write(at, values):
        order[pl.ds(at, 1), :] = values.astype(jnp.int32)

    lines = -(-high * ma * mb // 128)
    for at in range(lines):
        spot = lane_row + at * 128.0
        for base, columns in ((0, code_columns), (lines, target_columns)):
            write(base + at, gathered([
                jnp.where(rank == spot, values, 0.0) for rank, values in zip(ranks, columns)
            ]))
    bound = (lane_row + 1.0) * (kb_cols * 1024.0)
    write(2 * lines, gathered([jnp.where(mine < bound, 1.0, 0.0) for mine in key_columns]))
    filled = gathered([jnp.where(mine == lane_row, 1.0, 0.0) for mine in target_columns])
    empty = jnp.where((filled < 0.5) & (lane_row < blocks), 1.0, 0.0)
    lane = lax.broadcasted_iota(jnp.int32, (128, 128), 1).astype(jnp.float32)
    line = lax.broadcasted_iota(jnp.int32, (128, 128), 0).astype(jnp.float32)
    wide = jnp.broadcast_to(empty, (128, 128))
    rank = jnp.sum(jnp.where(lane < line, wide, 0.0), axis=1, keepdims=True)
    flag = jnp.sum(jnp.where(lane == line, wide, 0.0), axis=1, keepdims=True)
    size = jnp.broadcast_to(jnp.sum(empty, axis=1, keepdims=True), (1, 128))
    listed = gathered([jnp.where(rank == lane, line * flag, 0.0)])
    write(2 * lines + 1, jnp.where(lane_row < size, listed, 1.0 * blocks))
    write(2 * lines + 2, size)


def gather_kernel(
    sizes, option, left, own_left, right, perm, left_meta, right_meta, tiles,
    left_all, right_all, order,
    own_right, packed_down, packed_up, side, spill_down, spill_up,
    up_send, up_recv, down_send, down_recv, spill_send, spill_recv,
    x_send, x_recv, own_send, own_recv, pass_send, pass_recv,
    left_sem, right_sem,
):
    n_row, n_col, sets = sizes[:3]
    row = lax.axis_index("row")
    col = lax.axis_index("col")
    n_chip = n_row // 2
    chip, core = row // 2, row % 2
    partner = chip * 2 + 1 - core
    slots = left.shape[0]
    main, spill, head, middle, limit = option

    barrier = pltpu.get_barrier_semaphore()
    for there, step in ((col > 0, -1), (col + 1 < n_col, 1)):
        @pl.when(there)
        def _():
            pl.semaphore_signal(
                barrier, inc=1, device_id={"col": col + step}, device_id_type=MESH
            )
    others = [partner] + [((chip + step) % n_chip) * 2 + core for step in range(1, n_chip)]
    for other in others:
        pl.semaphore_signal(barrier, inc=1, device_id={"row": other}, device_id_type=MESH)
    kept = pltpu.make_async_copy(left, left_all.at[pl.ds(col * slots, slots)], left_sem)
    kept.start()

    bounds = [main * at // MAIN_CUTS for at in range(MAIN_CUTS + 1)]
    cuts = [(low, high, "main") for low, high in zip(bounds, bounds[1:])]
    if head > main:
        cuts.append((main, head, "side"))
    if middle > head:
        cuts.append((head, middle, "rest"))
    bounds = [limit * at // RIGHT_CUTS for at in range(RIGHT_CUTS + 1)]
    right_cuts = [pl.ds(low, high - low) for low, high in zip(bounds, bounds[1:])]

    def left_copy(step, cut, up):
        low, high, kind = cuts[cut]
        panel = col - step if up else col + step
        span = pl.ds(panel * slots + low, high - low)
        target = side.at[span] if kind == "side" else left_all.at[span]
        source = (packed_up if up else packed_down).at[pl.ds(low, high - low)]
        send, recv = (up_send, up_recv) if up else (down_send, down_recv)
        return pltpu.make_async_remote_copy(
            src_ref=source if step == 0 else target, dst_ref=target,
            send_sem=send.at[step, cut], recv_sem=recv.at[step, cut],
            device_id={"col": col + 1 if up else col - 1}, device_id_type=MESH,
        )

    def left_sends(step, cut, up):
        mid = 0 if cuts[cut][2] == "main" else 1
        if up:
            return (col + 1 < n_col - mid) & (col - step >= 0)
        return (col - 1 >= mid) & (col + step < n_col)

    def left_receives(step, cut, up):
        mid = 0 if cuts[cut][2] == "main" else 1
        if up:
            return (col - 1 - step >= 0) & (col < n_col - mid)
        return (col + 1 + step < n_col) & (col >= mid)

    def start_left(step, cut):
        for up in (True, False):
            pl.when(left_sends(step, cut, up))(left_copy(step, cut, up).start)

    def spill_copy(up):
        return pltpu.make_async_remote_copy(
            src_ref=spill_up if up else spill_down,
            dst_ref=left_all.at[pl.ds(n_col * slots, spill)],
            send_sem=spill_send.at[int(up)], recv_sem=spill_recv.at[int(up)],
            device_id={"col": n_col - 1 if up else 0}, device_id_type=MESH,
        )

    def across(step, cut):
        span = right_cuts[cut]
        other = ((chip + step) % n_chip) * 2 + core
        return pltpu.make_async_remote_copy(
            src_ref=right_all.at[:, row, span], dst_ref=right_all.at[:, row, span],
            send_sem=x_send.at[step - 1, cut], recv_sem=x_recv.at[step - 1, cut],
            device_id={"row": other}, device_id_type=MESH,
        )

    def passed(step, cut):
        span = right_cuts[cut]
        panel = ((chip + n_chip - step) % n_chip) * 2 + core
        return pltpu.make_async_remote_copy(
            src_ref=right_all.at[:, panel, span], dst_ref=right_all.at[:, panel, span],
            send_sem=pass_send.at[step - 1, cut], recv_sem=pass_recv.at[step - 1, cut],
            device_id={"row": partner}, device_id_type=MESH,
        )

    own = pltpu.make_async_remote_copy(
        src_ref=right_all.at[:, row, pl.ds(0, limit)],
        dst_ref=right_all.at[:, row, pl.ds(0, limit)],
        send_sem=own_send, recv_sem=own_recv,
        device_id={"row": partner}, device_id_type=MESH,
    )

    def pack_left(low, high):
        @pl.loop(low, high)
        def _(at):
            packed_down[at] = own_left[perm[0, at]]
            packed_up[at] = own_left[perm[1, at]]

    pack_left(*cuts[0][:2])
    pl.semaphore_wait(
        barrier, len(others) + jnp.where(col > 0, 1, 0) + jnp.where(col + 1 < n_col, 1, 0)
    )
    start_left(0, 0)
    staged = pltpu.make_async_copy(right, own_right, right_sem)
    staged.start()
    pack_left(cuts[0][1], middle)
    for cut in range(1, len(cuts)):
        if cuts[cut][2] == "main":
            start_left(0, cut)

    staged.wait()
    for which in range(sets):
        @pl.loop(0, limit)
        def _(at):
            right_all[which, row, at] = own_right[which, perm[4 + which, at]]

    for step in range(1, n_chip):
        for cut in range(RIGHT_CUTS):
            across(step, cut).start()
    own.start()
    if spill:
        @pl.loop(main, head)
        def _(at):
            side[col * slots + at] = packed_down[at]
            side[n_col * slots + at] = packed_up[at]

    def take_left(step, cut):
        for up in (True, False):
            pl.when(left_receives(step, cut, up))(left_copy(step, cut, up).wait_recv)
            if step + 1 < n_col - 1:
                pl.when(left_sends(step + 1, cut, up))(left_copy(step + 1, cut, up).start)

    def take_right(step, cut):
        across(step, cut).wait_recv()
        passed(step, cut).start()

    def take_order():
        order_pairs(
            sizes, main, lax.axis_index("kpt"), col, tiles, left_meta, right_meta, order
        )

    def send_spill():
        for up in (False, True):
            target, line = (spill_up, 3) if up else (spill_down, 2)

            @pl.when(col == (n_col - 2 if up else 1))
            def _():
                @pl.loop(0, spill)
                def _(at):
                    target[at] = side[perm[line, at] + main]

                spill_copy(up).start()

    def take_sides():
        for step in range(1, n_col):
            for panel, there in (
                (col - step, (col - step >= 0) & (col < n_col - 1)),
                (col + step, (col + step < n_col) & (col > 0)),
            ):
                @pl.when(there)
                def _():
                    @pl.loop(main, head)
                    def _(at):
                        left_all[panel * slots + at] = side[panel * slots + at]

    mains, heads = (n_col - 2) * main, (n_col - 2) * head
    jobs = [(7, take_order)]
    if spill:
        jobs.append((heads + 0.02, send_spill))
    if head > main:
        jobs.append((heads + 0.03, take_sides))
    for cut, (low, high, kind) in enumerate(cuts):
        start = functools.partial(start_left, 0, cut)
        if kind == "side":
            jobs.append(((n_col - 3) * main + 0.01, start))
        elif kind == "rest":
            jobs.append((mains + (n_col - 3) * (head - main) + 0.01, start))
        for step in range(n_col - 1 if kind == "main" else n_col - 2):
            when = step * main + high
            if kind == "side":
                when = mains + (step + 1) * (high - low)
            elif kind == "rest":
                when = heads + (step + 1) * (high - low) + 0.04
            jobs.append((when, functools.partial(take_left, step, cut)))
    for step in range(1, n_chip):
        for cut in range(RIGHT_CUTS):
            when = ((step - 1) * RIGHT_CUTS + cut + 1) * limit * sets / RIGHT_CUTS + 2
            jobs.append((when, functools.partial(take_right, step, cut)))
    for _, job in sorted(jobs, key=lambda entry: entry[0]):
        job()

    kept.wait()
    if spill:
        for up in (False, True):
            pl.when(col == (n_col - 1 if up else 0))(spill_copy(up).wait_recv)
            pl.when(col == (n_col - 2 if up else 1))(spill_copy(up).wait_send)
    own.wait()
    for step in range(1, n_chip):
        for cut in range(RIGHT_CUTS):
            across(step, cut).wait_send()
            passed(step, cut).wait()
    for cut, entry in enumerate(cuts):
        for step in range(n_col - 1 if entry[2] == "main" else n_col - 2):
            for up in (True, False):
                pl.when(left_sends(step, cut, up))(left_copy(step, cut, up).wait_send)


def product_kernel(sizes, left, right, order, out, stage, partial, out_sem):
    n_row, n_col, sets, per, ma, mb, kb_cols = sizes
    blocks = GR * kb_cols
    lines = -(-n_col * per * ma * mb // 128)
    width = stage.shape[2]
    empty = jnp.zeros(stage.shape[1:], stage.dtype)

    @pl.loop(0, (order[2 * lines + 2, 0] + 3) // 4)
    def _(at):
        for lane in range(4):
            stage[order[2 * lines + 1, at * 4 + lane]] = empty

    def out_copy(line):
        span = pl.ds(line * kb_cols, kb_cols)
        return pltpu.make_async_copy(stage.at[span], out.at[span], out_sem.at[line])

    count = order[2 * lines, GR - 1]

    def group(at, carry):
        line, last = carry
        codes, targets, done = [], [], []
        for lane in range(GROUP):
            spot = at * GROUP + lane
            codes.append(order[spot // 128, spot % 128])
            targets.append(order[lines + spot // 128, spot % 128])
        for code in codes:
            block = left[code // 1024]
            wide = jnp.concatenate([block[:width], block[width:]], axis=1)
            other = right[code % 1024]
            real, imag = other[:width], other[width:]
            matrix = jnp.concatenate(
                [jnp.concatenate([real, imag], axis=1), jnp.concatenate([-imag, real], axis=1)],
                axis=0,
            )
            done.append(jnp.dot(wide, matrix, preferred_element_type=jnp.float32))
        held = partial[...]
        for target, product in zip(targets, done):
            held = jnp.where(target == last, held, 0.0) + product
            value = held.astype(stage.dtype)
            stage[target, :width] = value[:, :width]
            stage[target, width:] = value[:, width:]
            last = target
        partial[...] = held
        for _ in range(1 + GROUP // 12):
            ready = (line < GR) & (at * GROUP >= order[2 * lines, jnp.minimum(line, GR - 1)])
            pl.when(ready)(out_copy(jnp.minimum(line, GR - 1)).start)
            line = line + jnp.where(ready, 1, 0)
        return line, last

    partial[...] = jnp.zeros(partial.shape, partial.dtype)
    line, _ = lax.fori_loop(
        0, (count + GROUP - 1) // GROUP, group, (jnp.int32(0), jnp.int32(-1))
    )

    @pl.loop(line, GR)
    def _(line):
        out_copy(line).start()

    @pl.loop(0, GR)
    def _(line):
        out_copy(line).wait()


def body(
    n_kpt, n_row, n_col, left_blocks, left_rows, left_count, left_level,
    right_blocks, right_cols, right_count, right_level,
):
    _, per, ma, _, width, _ = left_blocks.shape
    sets, right_per, _, mb = right_blocks.shape[:4]
    assert right_per == per and sets * n_row == n_col and n_row % 2 == 0 and sets <= 2
    blocks = GR * (n_row * sets * per // n_col)
    assert n_col * per <= 128 and per * ma <= 128 and blocks <= 128 and ma * mb <= 8
    slots = per * ma
    left = left_blocks.reshape(slots, 2 * width, width)
    right = right_blocks.reshape(sets, per * mb, 2 * width, width)
    any_space = pl.BlockSpec(memory_space=pl.ANY)
    vmem = pl.BlockSpec(memory_space=pltpu.VMEM)
    smem = pl.BlockSpec(memory_space=pltpu.SMEM)
    dma = pltpu.SemaphoreType.DMA
    n_chip = n_row // 2
    total = n_kpt * n_row * n_col
    options = variants(slots, n_col, per * mb)
    sizes = (n_row, n_col, sets, per, ma, mb, n_row * sets * per // n_col)
    tile_rows = -(-(ma + sets) // 4) * 4
    meta_rows = -(-(2 * ma + 2 * mb * sets) // 8) * 8
    lines = -(-n_col * per * ma * mb // 128)
    order_rows = -(-(2 * lines + 3) // 8) * 8
    own_left, left_meta, right_meta, tiles, perm, choice = pl.pallas_call(
        functools.partial(plan_kernel, (n_kpt,) + sizes[:-1], options),
        out_shape=(
            pltpu.VMEM(left.shape, left.dtype),
            jax.ShapeDtypeStruct((n_col, meta_rows, 128), jnp.int32),
            jax.ShapeDtypeStruct((n_row, meta_rows, 128), jnp.int32),
            jax.ShapeDtypeStruct((total, tile_rows, 128), jnp.int32),
            jax.ShapeDtypeStruct((8, 128), jnp.int32),
            jax.ShapeDtypeStruct((1,), jnp.int32),
        ),
        in_specs=[any_space] + [vmem] * 6,
        out_specs=(vmem,) * 5 + (smem,),
        scratch_shapes=[
            pltpu.VMEM((tile_rows, 128), jnp.int32),
            pltpu.VMEM((meta_rows, 128), jnp.int32),
            *[dma((total,))] * 2,
            *[dma((n_col - 1,))] * 2,
            *[dma((n_row - 1,))] * 2,
            dma,
        ],
        compiler_params=pltpu.CompilerParams(collective_id=0, has_side_effects=True),
        name="plan",
    )(
        left, left_level[0].T, left_rows[0].T, left_count,
        right_level[:, :, 0].transpose(0, 2, 1), right_cols[:, :, 0].transpose(0, 2, 1),
        right_count.transpose(0, 2, 1),
    )

    kb_cols = sizes[-1]
    right_shape = (sets, n_row) + right.shape[1:]
    most = (n_col + 1) * left.size + n_row * right.size + 24 * left.size // slots
    limit = VMEM_BYTES - most * left.dtype.itemsize

    def run(at, left, own_left, right, perm, left_meta, right_meta, tiles):
        cuts, spill = MAIN_CUTS + 2, max(options[at][1], 1)
        left_all, right_all, order = pl.pallas_call(
            functools.partial(gather_kernel, sizes, options[at]),
            out_shape=(
                pltpu.VMEM((n_col * slots + options[at][1],) + left.shape[1:], left.dtype),
                pltpu.VMEM(right_shape, right.dtype),
                jax.ShapeDtypeStruct((order_rows, 128), jnp.int32),
            ),
            in_specs=[any_space, vmem, any_space, smem, vmem, vmem, vmem],
            out_specs=(vmem, vmem, vmem),
            scratch_shapes=[
                pltpu.VMEM(right.shape, right.dtype),
                *[pltpu.VMEM(left.shape, left.dtype)] * 2,
                pltpu.VMEM(((n_col + 1) * slots,) + left.shape[1:], left.dtype),
                *[pltpu.VMEM((spill,) + left.shape[1:], left.dtype)] * 2,
                *[dma((n_col - 1, cuts))] * 4,
                *[dma((2,))] * 2,
                *[dma((n_chip - 1, RIGHT_CUTS))] * 2,
                *[dma] * 2,
                *[dma((n_chip - 1, RIGHT_CUTS))] * 2,
                *[dma] * 2,
            ],
            compiler_params=pltpu.CompilerParams(
                collective_id=1 + at, has_side_effects=True, vmem_limit_bytes=limit
            ),
            name=f"gather_panels_{at}",
        )(
            left, pltpu.with_memory_space_constraint(own_left, pltpu.VMEM),
            right, perm, left_meta, right_meta, tiles,
        )
        return pl.pallas_call(
            functools.partial(product_kernel, sizes),
            out_shape=jax.ShapeDtypeStruct((blocks, 2 * width, width), jnp.bfloat16),
            in_specs=[vmem, vmem, smem],
            out_specs=any_space,
            scratch_shapes=[
                pltpu.VMEM((blocks + 1, 2 * width, width), jnp.bfloat16),
                pltpu.VMEM((width, 2 * width), jnp.float32),
                dma((GR,)),
            ],
            compiler_params=pltpu.CompilerParams(vmem_limit_bytes=limit),
            name="pair_products",
        )(
            pltpu.with_memory_space_constraint(
                left_all, pltpu.VMEM
            ),
            pltpu.with_memory_space_constraint(
                right_all.reshape((-1,) + right.shape[2:]), pltpu.VMEM
            ),
            order,
        )

    out = lax.switch(
        choice[0], [functools.partial(run, at) for at in range(len(options))],
        left, own_left, right, perm, left_meta, right_meta, tiles,
    )
    return out.reshape(GR, kb_cols, 2, width, width)


def solution(mesh):
    in_specs = (
        P(("kpt", "row"), "col", None, None, None, None),
        P(("kpt", "row"), "col", None),
        P(("kpt", "row"), "col"),
        P(("kpt", "row"), "col", None),
        P("kpt", "row", "col", None, None, None, None),
        P("kpt", "row", "col", None),
        P("kpt", "row", "col"),
        P("kpt", "row", "col", None),
    )
    out_specs = P(("kpt", "row"), "col", None, None, None)
    return jax.shard_map(
        functools.partial(body, mesh.shape["kpt"], mesh.shape["row"], mesh.shape["col"]),
        mesh=mesh, in_specs=in_specs, out_specs=out_specs, check_vma=False,
    )
```

```python
import functools

import jax
import jax.numpy as jnp
from jax import lax
from jax.experimental import pallas as pl
from jax.experimental.pallas import tpu as pltpu
from jax.sharding import PartitionSpec as P

GR = 8
LEVEL_CUT = 7
DEAD = -1000
GROUP = 24
LEAD = 3
MAIN_CUTS = 2
RIGHT_CUTS = 8
VMEM_BYTES = 59 * 1024 * 1024
MESH = pl.DeviceIdType.MESH
FAR = 2.0 ** 17
FIRST = 1000


def variants(slots, n_col, right_slots):
    scale = slots * (n_col - 1) / 96
    found = []
    for spill, head, middle, rights in (
        (5, 25, 28, 52), (6, 25, 28, 52), (7, 26, 28, 54), (8, 26, 29, 54), (9, 26, 29, 54),
        (10, 26, 29, 55), (12, 27, 30, 56), (14, 27, 30, 56), (18, 28, 30, 58), (24, 32, 32, 64),
    ):
        found.append((
            slots * 18 // 32, max(1, int(spill * scale)), slots * head // 32,
            slots * middle // 32, right_slots * rights // 64,
        ))
    return found + [(slots, 0, slots, slots, right_slots)]


def ordered(levels, end, union, slots, lane_row):
    ma, per = levels.shape[0], slots // levels.shape[0]
    rows, columns = [], []
    lane = lax.broadcasted_iota(jnp.int32, (per, 128), 1)
    line = lax.broadcasted_iota(jnp.int32, (per, 128), 0)
    for m in range(ma):
        kind = jnp.where(
            levels[m:m + 1] + end >= LEVEL_CUT, 0.0,
            jnp.where(levels[m:m + 1] + union >= LEVEL_CUT, 1.0, 2.0),
        )
        level = levels[m:m + 1].astype(jnp.float32)
        key = jnp.where(level >= FIRST / 2, -level, kind * 128.0 + lane_row * ma + m)
        rows.append(jnp.where(lane_row < per, key, 1024.0))
        columns.append(jnp.sum(
            jnp.where(lane == line, jnp.broadcast_to(rows[-1], (per, 128)), 0.0),
            axis=1, keepdims=True,
        ))
    return rows, columns


def spilled(levels, end, main):
    hits = [
        jnp.where(levels[m:m + 1] + end >= LEVEL_CUT, 1.0, 0.0) for m in range(levels.shape[0])
    ]
    size = jnp.sum(functools.reduce(jnp.add, hits), axis=1, keepdims=True)
    return jnp.maximum(size - main, 0.0)


def placed(live, per, lane, line):
    padded = live if live.shape[1] == 128 else jnp.concatenate(
        [live, jnp.zeros((1, 128 - per), jnp.float32)], axis=1
    )
    wide = jnp.broadcast_to(padded, (per, 128))
    own = jnp.sum(jnp.where(lane == line, wide, 0.0), axis=1, keepdims=True)
    first = jnp.sum(jnp.where(lane < line, wide, 0.0), axis=1, keepdims=True)
    return own, first


def plan_kernel(
    sizes, options, left,
    left_level, left_rows, left_count, right_level, right_cols, right_count,
    own_left, lead_down, lead_up, left_meta, right_meta, tiles, perm, choice,
    lead, tile, meta, send, recv, lead_send, lead_recv, lm_send, lm_recv, rm_send, rm_recv, left_sem,
):
    n_kpt, n_row, n_col, sets, per, ma, mb = sizes
    slots = per * ma
    kpt, row, col = (lax.axis_index(name) for name in ("kpt", "row", "col"))
    total = n_kpt * n_row * n_col
    me = (kpt * n_row + row) * n_col + col

    def place_of(step):
        other = (me + step) % total
        return {
            "kpt": other // (n_row * n_col), "row": (other // n_col) % n_row, "col": other % n_col
        }

    def copy_of(step):
        return pltpu.make_async_remote_copy(
            src_ref=tile, dst_ref=tiles.at[me], send_sem=send.at[step], recv_sem=recv.at[step],
            device_id=place_of(step), device_id_type=MESH,
        )

    barrier = pltpu.get_barrier_semaphore()

    @pl.loop(1, total)
    def _(step):
        pl.semaphore_signal(barrier, inc=1, device_id=place_of(step), device_id_type=MESH)

    stages = (
        pltpu.make_async_copy(left, own_left, left_sem),
    )
    for copy in stages:
        copy.start()
    tile[...] = jnp.full(tile.shape, DEAD, jnp.int32)
    live = lax.broadcasted_iota(jnp.int32, (ma, per), 0) < left_count[...]
    levels = jnp.where(live, left_level[...], DEAD)
    tile[:ma, :per] = levels
    lane = lax.broadcasted_iota(jnp.int32, (per, 128), 1)
    line = lax.broadcasted_iota(jnp.int32, (per, 128), 0)
    keys, columns, ranks = [], [], []
    for m in range(ma):
        key = 256 * (8 - tile[m:m + 1, :]) + lane[:1] * ma + m
        keys.append(jnp.where(lane[:1] < per, key, 1024 ** 2))
        wide = jnp.broadcast_to(keys[-1], (per, 128))
        columns.append(jnp.sum(jnp.where(lane == line, wide, 0), axis=1, keepdims=True))
    for m in range(ma):
        before = [jnp.where(key < keys[m], 1, 0) for key in columns]
        rank = jnp.sum(functools.reduce(jnp.add, before), axis=0, keepdims=True)
        ranks.append(jnp.where(lane[:1] < per, rank, slots))
        tile[m:m + 1, :] = jnp.where(ranks[-1] < LEAD, FIRST - ranks[-1], tile[m:m + 1, :])
    marked = tile[:ma, :]
    rights = []
    for which in range(sets):
        live = lax.broadcasted_iota(jnp.int32, (mb, per), 0) < right_count[which]
        rights.append(jnp.where(live, right_level[which], DEAD))
        tile[ma + which:ma + which + 1, :per] = jnp.max(rights[-1], axis=0, keepdims=True)
        size = jnp.sum(right_count[which].astype(jnp.float32), axis=1, keepdims=True)
        tile[ma + which:ma + which + 1, 127:] = size.astype(jnp.int32)
    tiles[me] = tile[...]
    meta[...] = jnp.full(meta.shape, DEAD, jnp.int32)
    meta[:ma, :] = marked
    tail = 2 * ma + 2 * mb * sets
    meta[tail:tail + ma, :per] = levels
    meta[ma:2 * ma, :per] = left_rows[...]
    for which in range(sets):
        base = 2 * ma + which * 2 * mb
        meta[base:base + mb, :per] = right_cols[which]
        meta[base + mb:base + 2 * mb, :per] = rights[which]
    left_meta[col] = meta[...]
    right_meta[row] = meta[...]
    stages[0].wait()
    for at in range(LEAD):
        spots = [jnp.where(rank == at, lane[:1] * ma + m, 0) for m, rank in enumerate(ranks)]
        spot = jnp.max(functools.reduce(jnp.maximum, spots))
        lead[at] = own_left[jnp.minimum(jnp.maximum(spot, 0), slots - 1)]

    def lead_copy(up):
        return pltpu.make_async_remote_copy(
            src_ref=lead, dst_ref=lead_up if up else lead_down,
            send_sem=lead_send.at[int(up)], recv_sem=lead_recv.at[int(up)],
            device_id={"col": col + 1 if up else col - 1}, device_id_type=MESH,
        )

    pl.semaphore_wait(barrier, total - 1)

    @pl.loop(1, total)
    def _(step):
        copy_of(step).start()

    def meta_copies():
        for step in range(1, n_col):
            yield pltpu.make_async_remote_copy(
                src_ref=meta, dst_ref=left_meta.at[col],
                send_sem=lm_send.at[step - 1], recv_sem=lm_recv.at[step - 1],
                device_id={"col": (col + step) % n_col}, device_id_type=MESH,
            )
        for step in range(1, n_row):
            yield pltpu.make_async_remote_copy(
                src_ref=meta, dst_ref=right_meta.at[row],
                send_sem=rm_send.at[step - 1], recv_sem=rm_recv.at[step - 1],
                device_id={"row": (row + step) % n_row}, device_id_type=MESH,
            )

    for copy in meta_copies():
        copy.start()
    for up in (False, True):
        pl.when(col + 1 < n_col if up else col > 0)(lead_copy(up).start)

    @pl.loop(1, total)
    def _(step):
        copy_of(step).wait_recv()

    def at_device(k, r, c):
        return (k * n_row + r) * n_col + c

    def right_max(k, panel, q):
        return tiles[at_device(k, panel % n_row, q), pl.ds(ma + panel // n_row, 1), :]

    def measure_part(k, carry):
        most_end, most_mid, most_spill, most_right = carry
        spills = [zero, zero]
        for panel in range(n_col):
            levels = [
                jnp.concatenate(
                    [tiles[at_device(k, r, panel), pl.ds(m, 1), :] for r in range(n_row)], axis=0
                )
                for m in range(ma)
            ]

            def needed(most):
                hits = [jnp.where(level + most >= LEVEL_CUT, 1.0, 0.0) for level in levels]
                return jnp.sum(functools.reduce(jnp.add, hits), axis=1, keepdims=True)

            rights = [right_max(k, panel, q) for q in range(n_col)]
            for right in rights:
                most_right = jnp.maximum(most_right, right)
            for way, (taken, right) in enumerate(
                ((panel > 0, rights[0]), (panel < n_col - 1, rights[-1]))
            ):
                if taken:
                    wanted = needed(right)
                    most_end = jnp.maximum(most_end, wanted)
                    spills[way] = spills[way] + jnp.maximum(wanted - main, 0.0)
            if panel > 1:
                union = functools.reduce(jnp.maximum, rights[:panel])
                most_mid = jnp.maximum(most_mid, needed(union))
            if panel < n_col - 2:
                union = functools.reduce(jnp.maximum, rights[panel + 1:])
                most_mid = jnp.maximum(most_mid, needed(union))
        most_spill = jnp.maximum(most_spill, jnp.maximum(*spills))
        return most_end, most_mid, most_spill, most_right

    main = options[0][0]
    zero = jnp.zeros((n_row, 1), jnp.float32)
    most_end, most_mid, most_spill, most_right = lax.fori_loop(
        0, n_kpt, measure_part, (zero, zero, zero, jnp.zeros((1, 128), jnp.int32))
    )
    lanes = lax.broadcasted_iota(jnp.int32, (1, 128), 1)
    most_right = jnp.max(
        jnp.where(lanes == 127, most_right, 0).astype(jnp.float32), axis=1, keepdims=True
    )
    index = zero
    for _, spill, head, middle, limit in options[:-1]:
        over = (most_spill > spill) | (most_end > head) | (most_mid > middle)
        index = index + jnp.where(over | (most_right > limit), 1.0, 0.0)
    choice[0] = jnp.max(index).astype(jnp.int32)

    lane_row = lax.broadcasted_iota(jnp.int32, (1, 128), 1).astype(jnp.float32)
    line = lax.broadcasted_iota(jnp.int32, (per, 128), 0).astype(jnp.float32)
    mine = tiles[me, :ma, :]
    for at, up in enumerate((False, True)):
        which = ma + col // n_row
        near = [
            tiles[at_device(kpt, col % n_row, q), pl.ds(which, 1), :] for q in range(n_col)
        ]
        union = jnp.full((1, 128), DEAD, jnp.int32)
        for q in range(n_col):
            beyond = q > col if up else q < col
            union = jnp.maximum(union, jnp.where(beyond, near[q], DEAD))
        rows, columns = ordered(mine, near[-1] if up else near[0], union, slots, lane_row)
        found = jnp.zeros((1, 128), jnp.float32)
        for m in range(ma):
            before = [jnp.where(key < columns[m], 1.0, 0.0) for key in rows]
            rank = jnp.sum(functools.reduce(jnp.add, before), axis=1, keepdims=True)
            hit = jnp.where(rank == lane_row, line * ma + m, 0.0)
            found = found + jnp.sum(hit, axis=0, keepdims=True)
        perm[pl.ds(at, 1), :] = found.astype(jnp.int32)

    for at, up in ((2, False), (3, True)):
        panels = range(n_col - 2, -1, -1) if up else range(1, n_col)
        code, low = jnp.zeros((1, 128), jnp.float32), jnp.zeros((1, 1), jnp.float32)
        for panel in panels:
            levels = tiles[at_device(kpt, row, panel), :ma, :]
            end = right_max(kpt, panel, n_col - 1 if up else 0)
            high = low + spilled(levels, end, main)
            own = up and panel == n_col - 2
            base = (n_col if own else panel) * slots
            inside = (lane_row >= low) & (lane_row < high)
            code = code + jnp.where(inside, base + lane_row - low, 0.0)
            low = high
        perm[pl.ds(at, 1), :] = code.astype(jnp.int32)
    lane = lax.broadcasted_iota(jnp.int32, (per, 128), 1).astype(jnp.float32)
    for which in range(sets):
        live, first = placed(right_count[which].astype(jnp.float32), per, lane, line)
        found = jnp.zeros((1, 128), jnp.float32)
        for n in range(mb):
            hit = jnp.where((first + n == lane) & (live > n), line * mb + n, 0.0)
            found = found + jnp.sum(hit, axis=0, keepdims=True)
        perm[pl.ds(4 + which, 1), :] = found.astype(jnp.int32)

    for copy in meta_copies():
        copy.wait()
    for up in (False, True):
        pl.when(col + 1 < n_col if up else col > 0)(lead_copy(up).wait_send)
        pl.when(col > 0 if up else col + 1 < n_col)(lead_copy(up).wait_recv)

    @pl.loop(1, total)
    def _(step):
        copy_of(step).wait_send()


def order_pairs(sizes, main, kpt, col, tiles, left_meta, right_meta, order):
    n_row, n_col, sets, per, ma, mb, kb_cols = sizes
    slots, high = per * ma, n_col * per
    blocks = GR * kb_cols
    lane_row = lax.broadcasted_iota(jnp.int32, (1, 128), 1).astype(jnp.float32)

    def right_max(panel, q):
        at = (kpt * n_row + panel % n_row) * n_col + q
        return tiles[at, pl.ds(ma + panel // n_row, 1), :]

    lefts = jnp.zeros((2 * ma, 128), jnp.float32)
    rights = jnp.zeros((2 * mb, 128), jnp.float32)
    places = jnp.zeros((8, 128), jnp.float32)
    spots = jnp.zeros((8, 128), jnp.float32)
    thin = lax.broadcasted_iota(jnp.int32, (per, 128), 1).astype(jnp.float32)
    thick = lax.broadcasted_iota(jnp.int32, (per, 128), 0).astype(jnp.float32)
    lows, low = [None] * n_col, jnp.zeros((1, 1), jnp.float32)
    for panel in range(1, n_col):
        lows[panel] = low
        low = low + spilled(left_meta[panel, :ma, :], right_max(panel, 0), main)
    low = jnp.zeros((1, 1), jnp.float32)
    for panel in range(n_col - 2, -1, -1):
        lows[panel] = low if lows[panel] is None else jnp.where(col == 0, lows[panel], low)
        low = low + spilled(left_meta[panel, :ma, :], right_max(panel, n_col - 1), main)
    for panel in range(n_col):
        levels = left_meta[panel, :ma, :]
        down, up = panel > col, panel < col
        end = jnp.where(down, right_max(panel, 0), right_max(panel, n_col - 1))
        union = jnp.full((1, 128), DEAD, jnp.int32)
        for q in range(n_col):
            beyond = down if q < panel else up
            if q != panel:
                union = jnp.maximum(union, jnp.where(beyond, right_max(panel, q), DEAD))
        rows, columns = ordered(levels, end, union, slots, lane_row)
        found = []
        for m in range(ma):
            before = [jnp.where(key < rows[m], 1.0, 0.0) for key in columns]
            rank = jnp.sum(functools.reduce(jnp.add, before), axis=0, keepdims=True)
            own = jnp.where(down | up, rank, lane_row * ma + m) + panel * slots
            far = (down | up) & ((col == 0) | (col == n_col - 1)) & (rank >= main)
            found.append(jnp.where(far, n_col * slots + lows[panel] + rank - main, own))
        found = jnp.concatenate(found + [jnp.zeros((8 - ma, 128), jnp.float32)], axis=0)
        base = 2 * ma + panel // n_row * 2 * mb
        here = (lane_row >= panel * per) & (lane_row < (panel + 1) * per)

        def moved(values):
            values = pltpu.roll(values, panel * per, 1) if panel else values
            return jnp.where(here, values, 0.0)

        tail = 2 * ma + 2 * mb * sets
        left = [left_meta[panel, tail:tail + ma, :], left_meta[panel, ma:2 * ma, :]]
        lefts = lefts + moved(jnp.concatenate(left, axis=0).astype(jnp.float32))
        right = right_meta[panel % n_row, base:base + 2 * mb, :].astype(jnp.float32)
        rights = rights + moved(right)
        places = places + moved(found)
        size = jnp.zeros((1, 128), jnp.float32)
        for n in range(mb):
            size = size + jnp.where((right[mb + n:mb + n + 1] > DEAD / 2) & (lane_row < per), 1.0, 0.0)
        live, _ = placed(size, per, thin, thick)
        first = jnp.sum(jnp.where(thick < thin, live, 0.0), axis=0, keepdims=True)
        spots = spots + moved(
            jnp.broadcast_to(jnp.where(lane_row < per, first, 0.0) + panel * per * mb, (8, 128))
        )

    lane = lax.broadcasted_iota(jnp.int32, (high, 128), 1)
    line = lax.broadcasted_iota(jnp.int32, (high, 128), 0)

    def column(values):
        wide = jnp.broadcast_to(values, (high, 128))
        return jnp.sum(jnp.where(lane == line, wide, 0.0), axis=1, keepdims=True)

    keys, key_columns, code_columns, target_columns = [], [], [], []
    for m in range(ma):
        for n in range(mb):
            kept = lefts[m:m + 1] + rights[mb + n:mb + n + 1] >= LEVEL_CUT
            target = lefts[ma + m:ma + m + 1] * kb_cols + rights[n:n + 1]
            spot = lane_row + (m * mb + n) * 128.0
            key = jnp.where(kept, target * 1024.0 + spot, FAR + spot)
            keys.append(jnp.where(lane_row < high, key, 2 * FAR))
            key_columns.append(column(keys[-1]))
            code = places[m:m + 1] * 1024.0 + spots[:1] + n
            code_columns.append(column(jnp.where(kept, code, 0.0)))
            target_columns.append(column(jnp.where(kept, target, 1.0 * blocks)))
    ranks = []
    for mine in key_columns:
        before = [jnp.where(key < mine, 1.0, 0.0) for key in keys]
        ranks.append(jnp.sum(functools.reduce(jnp.add, before), axis=1, keepdims=True))

    def gathered(hits):
        return jnp.sum(functools.reduce(jnp.add, hits), axis=0, keepdims=True)

    def write(at, values):
        order[pl.ds(at, 1), :] = values.astype(jnp.int32)

    lines = -(-high * ma * mb // 128)
    for at in range(lines):
        spot = lane_row + at * 128.0
        for base, columns in ((0, code_columns), (lines, target_columns)):
            write(base + at, gathered([
                jnp.where(rank == spot, values, 0.0) for rank, values in zip(ranks, columns)
            ]))
    bound = (lane_row + 1.0) * (kb_cols * 1024.0)
    write(2 * lines, gathered([jnp.where(mine < bound, 1.0, 0.0) for mine in key_columns]))
    filled = gathered([jnp.where(mine == lane_row, 1.0, 0.0) for mine in target_columns])
    empty = jnp.where((filled < 0.5) & (lane_row < blocks), 1.0, 0.0)
    lane = lax.broadcasted_iota(jnp.int32, (128, 128), 1).astype(jnp.float32)
    line = lax.broadcasted_iota(jnp.int32, (128, 128), 0).astype(jnp.float32)
    wide = jnp.broadcast_to(empty, (128, 128))
    rank = jnp.sum(jnp.where(lane < line, wide, 0.0), axis=1, keepdims=True)
    flag = jnp.sum(jnp.where(lane == line, wide, 0.0), axis=1, keepdims=True)
    size = jnp.broadcast_to(jnp.sum(empty, axis=1, keepdims=True), (1, 128))
    listed = gathered([jnp.where(rank == lane, line * flag, 0.0)])
    write(2 * lines + 1, jnp.where(lane_row < size, listed, 1.0 * blocks))
    write(2 * lines + 2, size)


def gather_kernel(
    sizes, option, left, own_left, lead_down, lead_up, right, perm, left_meta, right_meta, tiles,
    left_all, right_all, order,
    own_right, packed_down, packed_up, side, spill_down, spill_up,
    up_send, up_recv, down_send, down_recv, spill_send, spill_recv,
    x_send, x_recv, own_send, own_recv, pass_send, pass_recv,
    left_sem, right_sem,
):
    n_row, n_col, sets = sizes[:3]
    row = lax.axis_index("row")
    col = lax.axis_index("col")
    n_chip = n_row // 2
    chip, core = row // 2, row % 2
    partner = chip * 2 + 1 - core
    slots = left.shape[0]
    main, spill, head, middle, limit = option

    barrier = pltpu.get_barrier_semaphore()
    for there, step in ((col > 0, -1), (col + 1 < n_col, 1)):
        @pl.when(there)
        def _():
            pl.semaphore_signal(
                barrier, inc=1, device_id={"col": col + step}, device_id_type=MESH
            )
    others = [partner] + [((chip + step) % n_chip) * 2 + core for step in range(1, n_chip)]
    for other in others:
        pl.semaphore_signal(barrier, inc=1, device_id={"row": other}, device_id_type=MESH)
    kept = pltpu.make_async_copy(left, left_all.at[pl.ds(col * slots, slots)], left_sem)
    kept.start()

    bounds = [LEAD + (main - LEAD) * at // MAIN_CUTS for at in range(MAIN_CUTS + 1)]
    cuts = [(low, high, "main") for low, high in zip(bounds, bounds[1:])]
    cuts.append((0, LEAD, "lead"))
    if head > main:
        cuts.append((main, head, "side"))
    if middle > head:
        cuts.append((head, middle, "rest"))
    bounds = [limit * at // RIGHT_CUTS for at in range(RIGHT_CUTS + 1)]
    right_cuts = [pl.ds(low, high - low) for low, high in zip(bounds, bounds[1:])]

    def left_copy(step, cut, up):
        low, high, kind = cuts[cut]
        panel = col - step if up else col + step
        span = pl.ds(panel * slots + low, high - low)
        target = side.at[span] if kind == "side" else left_all.at[span]
        source = (packed_up if up else packed_down).at[pl.ds(low, high - low)]
        if kind == "lead" and step == 1:
            source = lead_up if up else lead_down
        send, recv = (up_send, up_recv) if up else (down_send, down_recv)
        return pltpu.make_async_remote_copy(
            src_ref=source if step == int(kind == "lead") else target, dst_ref=target,
            send_sem=send.at[step, cut], recv_sem=recv.at[step, cut],
            device_id={"col": col + 1 if up else col - 1}, device_id_type=MESH,
        )

    def left_sends(step, cut, up):
        mid = 0 if cuts[cut][2] in ("main", "lead") else 1
        if up:
            return (col + 1 < n_col - mid) & (col - step >= 0)
        return (col - 1 >= mid) & (col + step < n_col)

    def left_receives(step, cut, up):
        mid = 0 if cuts[cut][2] in ("main", "lead") else 1
        if up:
            return (col - 1 - step >= 0) & (col < n_col - mid)
        return (col + 1 + step < n_col) & (col >= mid)

    def start_left(step, cut):
        for up in (True, False):
            pl.when(left_sends(step, cut, up))(left_copy(step, cut, up).start)

    def steps_of(kind):
        if kind == "lead":
            return range(1, n_col - 1)
        return range(n_col - 1 if kind == "main" else n_col - 2)

    def spill_copy(up):
        return pltpu.make_async_remote_copy(
            src_ref=spill_up if up else spill_down,
            dst_ref=left_all.at[pl.ds(n_col * slots, spill)],
            send_sem=spill_send.at[int(up)], recv_sem=spill_recv.at[int(up)],
            device_id={"col": n_col - 1 if up else 0}, device_id_type=MESH,
        )

    def across(step, cut):
        span = right_cuts[cut]
        other = ((chip + step) % n_chip) * 2 + core
        return pltpu.make_async_remote_copy(
            src_ref=right_all.at[:, row, span], dst_ref=right_all.at[:, row, span],
            send_sem=x_send.at[step - 1, cut], recv_sem=x_recv.at[step - 1, cut],
            device_id={"row": other}, device_id_type=MESH,
        )

    def passed(step, cut):
        span = right_cuts[cut]
        panel = ((chip + n_chip - step) % n_chip) * 2 + core
        return pltpu.make_async_remote_copy(
            src_ref=right_all.at[:, panel, span], dst_ref=right_all.at[:, panel, span],
            send_sem=pass_send.at[step - 1, cut], recv_sem=pass_recv.at[step - 1, cut],
            device_id={"row": partner}, device_id_type=MESH,
        )

    own = pltpu.make_async_remote_copy(
        src_ref=right_all.at[:, row, pl.ds(0, limit)],
        dst_ref=right_all.at[:, row, pl.ds(0, limit)],
        send_sem=own_send, recv_sem=own_recv,
        device_id={"row": partner}, device_id_type=MESH,
    )

    def pack_left(low, high):
        @pl.loop(low, high)
        def _(at):
            packed_down[at] = own_left[perm[0, at]]
            packed_up[at] = own_left[perm[1, at]]

    pack_left(*cuts[0][:2])
    pl.semaphore_wait(
        barrier, len(others) + jnp.where(col > 0, 1, 0) + jnp.where(col + 1 < n_col, 1, 0)
    )
    start_left(0, 0)
    staged = pltpu.make_async_copy(right, own_right, right_sem)
    staged.start()
    pack_left(cuts[0][1], middle)
    for cut in range(1, len(cuts)):
        if cuts[cut][2] == "main":
            start_left(0, cut)
        elif cuts[cut][2] == "lead" and n_col > 2:
            start_left(1, cut)

    staged.wait()
    for which in range(sets):
        @pl.loop(0, limit)
        def _(at):
            right_all[which, row, at] = own_right[which, perm[4 + which, at]]

    for step in range(1, n_chip):
        for cut in range(RIGHT_CUTS):
            across(step, cut).start()
    own.start()
    if spill:
        @pl.loop(main, head)
        def _(at):
            side[col * slots + at] = packed_down[at]
            side[n_col * slots + at] = packed_up[at]

    def take_left(step, cut):
        for up in (True, False):
            pl.when(left_receives(step, cut, up))(left_copy(step, cut, up).wait_recv)
            if step + 1 < n_col - 1:
                pl.when(left_sends(step + 1, cut, up))(left_copy(step + 1, cut, up).start)

    def take_right(step, cut):
        across(step, cut).wait_recv()
        passed(step, cut).start()

    def take_order():
        for panel, there, found in (
            (col + 1, col + 1 < n_col, lead_down), (col - 1, col > 0, lead_up)
        ):
            @pl.when(there)
            def _():
                for at in range(LEAD):
                    left_all[panel * slots + at] = found[at]

        order_pairs(
            sizes, main, lax.axis_index("kpt"), col, tiles, left_meta, right_meta, order
        )

    def send_spill():
        for up in (False, True):
            target, line = (spill_up, 3) if up else (spill_down, 2)

            @pl.when(col == (n_col - 2 if up else 1))
            def _():
                @pl.loop(0, spill)
                def _(at):
                    target[at] = side[perm[line, at] + main]

                spill_copy(up).start()

    def take_sides():
        for step in range(1, n_col):
            for panel, there in (
                (col - step, (col - step >= 0) & (col < n_col - 1)),
                (col + step, (col + step < n_col) & (col > 0)),
            ):
                @pl.when(there)
                def _():
                    @pl.loop(main, head)
                    def _(at):
                        left_all[panel * slots + at] = side[panel * slots + at]

    mains, heads = (n_col - 2) * main - LEAD, (n_col - 2) * head - LEAD
    jobs = [(7, take_order)]
    if spill:
        jobs.append((heads + 0.02, send_spill))
    if head > main:
        jobs.append((heads + 0.03, take_sides))
    for cut, (low, high, kind) in enumerate(cuts):
        start = functools.partial(start_left, 0, cut)
        if kind == "side":
            jobs.append(((n_col - 3) * main - LEAD + 0.01, start))
        elif kind == "rest":
            jobs.append((mains + (n_col - 3) * (head - main) + 0.01, start))
        for step in steps_of(kind):
            when = step * main + high - LEAD
            if kind == "side":
                when = mains + (step + 1) * (high - low)
            elif kind == "rest":
                when = heads + (step + 1) * (high - low) + 0.04
            jobs.append((when, functools.partial(take_left, step, cut)))
    for step in range(1, n_chip):
        for cut in range(RIGHT_CUTS):
            when = ((step - 1) * RIGHT_CUTS + cut + 1) * limit * sets / RIGHT_CUTS + 2
            jobs.append((when, functools.partial(take_right, step, cut)))
    for _, job in sorted(jobs, key=lambda entry: entry[0]):
        job()

    kept.wait()
    if spill:
        for up in (False, True):
            pl.when(col == (n_col - 1 if up else 0))(spill_copy(up).wait_recv)
            pl.when(col == (n_col - 2 if up else 1))(spill_copy(up).wait_send)
    own.wait()
    for step in range(1, n_chip):
        for cut in range(RIGHT_CUTS):
            across(step, cut).wait_send()
            passed(step, cut).wait()
    for cut, entry in enumerate(cuts):
        for step in steps_of(entry[2]):
            for up in (True, False):
                pl.when(left_sends(step, cut, up))(left_copy(step, cut, up).wait_send)


def product_kernel(sizes, left, right, order, out, stage, partial, out_sem):
    n_row, n_col, sets, per, ma, mb, kb_cols = sizes
    blocks = GR * kb_cols
    lines = -(-n_col * per * ma * mb // 128)
    width = stage.shape[2]
    empty = jnp.zeros(stage.shape[1:], stage.dtype)

    @pl.loop(0, (order[2 * lines + 2, 0] + 3) // 4)
    def _(at):
        for lane in range(4):
            stage[order[2 * lines + 1, at * 4 + lane]] = empty

    def out_copy(line):
        span = pl.ds(line * kb_cols, kb_cols)
        return pltpu.make_async_copy(stage.at[span], out.at[span], out_sem.at[line])

    count = order[2 * lines, GR - 1]

    def group(at, carry):
        line, last = carry
        codes, targets, done = [], [], []
        for lane in range(GROUP):
            spot = at * GROUP + lane
            codes.append(order[spot // 128, spot % 128])
            targets.append(order[lines + spot // 128, spot % 128])
        for code in codes:
            block = left[code // 1024]
            wide = jnp.concatenate([block[:width], block[width:]], axis=1)
            other = right[code % 1024]
            real, imag = other[:width], other[width:]
            matrix = jnp.concatenate(
                [jnp.concatenate([real, imag], axis=1), jnp.concatenate([-imag, real], axis=1)],
                axis=0,
            )
            done.append(jnp.dot(wide, matrix, preferred_element_type=jnp.float32))
        held = partial[...]
        for target, product in zip(targets, done):
            held = jnp.where(target == last, held, 0.0) + product
            value = held.astype(stage.dtype)
            stage[target, :width] = value[:, :width]
            stage[target, width:] = value[:, width:]
            last = target
        partial[...] = held
        for _ in range(1 + GROUP // 12):
            ready = (line < GR) & (at * GROUP >= order[2 * lines, jnp.minimum(line, GR - 1)])
            pl.when(ready)(out_copy(jnp.minimum(line, GR - 1)).start)
            line = line + jnp.where(ready, 1, 0)
        return line, last

    partial[...] = jnp.zeros(partial.shape, partial.dtype)
    line, _ = lax.fori_loop(
        0, (count + GROUP - 1) // GROUP, group, (jnp.int32(0), jnp.int32(-1))
    )

    @pl.loop(line, GR)
    def _(line):
        out_copy(line).start()

    @pl.loop(0, GR)
    def _(line):
        out_copy(line).wait()


def body(
    n_kpt, n_row, n_col, left_blocks, left_rows, left_count, left_level,
    right_blocks, right_cols, right_count, right_level,
):
    _, per, ma, _, width, _ = left_blocks.shape
    sets, right_per, _, mb = right_blocks.shape[:4]
    assert right_per == per and sets * n_row == n_col and n_row % 2 == 0 and sets <= 2
    blocks = GR * (n_row * sets * per // n_col)
    assert n_col * per <= 128 and per * ma <= 128 and blocks <= 128 and ma * mb <= 8
    slots = per * ma
    left = left_blocks.reshape(slots, 2 * width, width)
    right = right_blocks.reshape(sets, per * mb, 2 * width, width)
    any_space = pl.BlockSpec(memory_space=pl.ANY)
    vmem = pl.BlockSpec(memory_space=pltpu.VMEM)
    smem = pl.BlockSpec(memory_space=pltpu.SMEM)
    dma = pltpu.SemaphoreType.DMA
    n_chip = n_row // 2
    total = n_kpt * n_row * n_col
    options = variants(slots, n_col, per * mb)
    sizes = (n_row, n_col, sets, per, ma, mb, n_row * sets * per // n_col)
    tile_rows = -(-(ma + sets) // 4) * 4
    meta_rows = -(-(3 * ma + 2 * mb * sets) // 8) * 8
    lines = -(-n_col * per * ma * mb // 128)
    order_rows = -(-(2 * lines + 3) // 8) * 8
    own_left, lead_down, lead_up, left_meta, right_meta, tiles, perm, choice = pl.pallas_call(
        functools.partial(plan_kernel, (n_kpt,) + sizes[:-1], options),
        out_shape=(
            pltpu.VMEM(left.shape, left.dtype),
            *[pltpu.VMEM((LEAD,) + left.shape[1:], left.dtype)] * 2,
            jax.ShapeDtypeStruct((n_col, meta_rows, 128), jnp.int32),
            jax.ShapeDtypeStruct((n_row, meta_rows, 128), jnp.int32),
            jax.ShapeDtypeStruct((total, tile_rows, 128), jnp.int32),
            jax.ShapeDtypeStruct((8, 128), jnp.int32),
            jax.ShapeDtypeStruct((1,), jnp.int32),
        ),
        in_specs=[any_space] + [vmem] * 6,
        out_specs=(vmem,) * 7 + (smem,),
        scratch_shapes=[
            pltpu.VMEM((LEAD,) + left.shape[1:], left.dtype),
            pltpu.VMEM((tile_rows, 128), jnp.int32),
            pltpu.VMEM((meta_rows, 128), jnp.int32),
            *[dma((total,))] * 2,
            *[dma((2,))] * 2,
            *[dma((n_col - 1,))] * 2,
            *[dma((n_row - 1,))] * 2,
            dma,
        ],
        compiler_params=pltpu.CompilerParams(collective_id=0, has_side_effects=True),
        name="plan",
    )(
        left, left_level[0].T, left_rows[0].T, left_count,
        right_level[:, :, 0].transpose(0, 2, 1), right_cols[:, :, 0].transpose(0, 2, 1),
        right_count.transpose(0, 2, 1),
    )

    kb_cols = sizes[-1]
    right_shape = (sets, n_row) + right.shape[1:]
    assert LEAD <= per
    most = (n_col + 1) * left.size + 2 * LEAD * left.size // slots + n_row * right.size + 24 * left.size // slots
    limit = VMEM_BYTES - most * left.dtype.itemsize

    def run(at, left, own_left, lead_down, lead_up, right, perm, left_meta, right_meta, tiles):
        cuts, spill = MAIN_CUTS + 3, max(options[at][1], 1)
        left_all, right_all, order = pl.pallas_call(
            functools.partial(gather_kernel, sizes, options[at]),
            out_shape=(
                pltpu.VMEM((n_col * slots + options[at][1],) + left.shape[1:], left.dtype),
                pltpu.VMEM(right_shape, right.dtype),
                jax.ShapeDtypeStruct((order_rows, 128), jnp.int32),
            ),
            in_specs=[any_space, vmem, vmem, vmem, any_space, smem, vmem, vmem, vmem],
            out_specs=(vmem, vmem, vmem),
            scratch_shapes=[
                pltpu.VMEM(right.shape, right.dtype),
                *[pltpu.VMEM(left.shape, left.dtype)] * 2,
                pltpu.VMEM(((n_col + 1) * slots,) + left.shape[1:], left.dtype),
                *[pltpu.VMEM((spill,) + left.shape[1:], left.dtype)] * 2,
                *[dma((n_col - 1, cuts))] * 4,
                *[dma((2,))] * 2,
                *[dma((n_chip - 1, RIGHT_CUTS))] * 2,
                *[dma] * 2,
                *[dma((n_chip - 1, RIGHT_CUTS))] * 2,
                *[dma] * 2,
            ],
            compiler_params=pltpu.CompilerParams(
                collective_id=1 + at, has_side_effects=True, vmem_limit_bytes=limit
            ),
            name=f"gather_panels_{at}",
        )(
            left, pltpu.with_memory_space_constraint(own_left, pltpu.VMEM),
            pltpu.with_memory_space_constraint(lead_down, pltpu.VMEM),
            pltpu.with_memory_space_constraint(lead_up, pltpu.VMEM),
            right, perm, left_meta, right_meta, tiles,
        )
        return pl.pallas_call(
            functools.partial(product_kernel, sizes),
            out_shape=jax.ShapeDtypeStruct((blocks, 2 * width, width), jnp.bfloat16),
            in_specs=[vmem, vmem, smem],
            out_specs=any_space,
            scratch_shapes=[
                pltpu.VMEM((blocks + 1, 2 * width, width), jnp.bfloat16),
                pltpu.VMEM((width, 2 * width), jnp.float32),
                dma((GR,)),
            ],
            compiler_params=pltpu.CompilerParams(vmem_limit_bytes=limit),
            name="pair_products",
        )(
            pltpu.with_memory_space_constraint(
                left_all, pltpu.VMEM
            ),
            pltpu.with_memory_space_constraint(
                right_all.reshape((-1,) + right.shape[2:]), pltpu.VMEM
            ),
            order,
        )

    out = lax.switch(
        choice[0], [functools.partial(run, at) for at in range(len(options))],
        left, own_left, lead_down, lead_up, right, perm, left_meta, right_meta, tiles,
    )
    return out.reshape(GR, kb_cols, 2, width, width)


def solution(mesh):
    in_specs = (
        P(("kpt", "row"), "col", None, None, None, None),
        P(("kpt", "row"), "col", None),
        P(("kpt", "row"), "col"),
        P(("kpt", "row"), "col", None),
        P("kpt", "row", "col", None, None, None, None),
        P("kpt", "row", "col", None),
        P("kpt", "row", "col"),
        P("kpt", "row", "col", None),
    )
    out_specs = P(("kpt", "row"), "col", None, None, None)
    return jax.shard_map(
        functools.partial(body, mesh.shape["kpt"], mesh.shape["row"], mesh.shape["col"]),
        mesh=mesh, in_specs=in_specs, out_specs=out_specs, check_vma=False,
    )
```

```python
import functools

import jax
import jax.numpy as jnp
from jax import lax
from jax.experimental import pallas as pl
from jax.experimental.pallas import tpu as pltpu
from jax.sharding import PartitionSpec as P

GR = 8
LEVEL_CUT = 7
DEAD = -1000
GROUP = 24
LEAD = 3
MAIN_CUTS = 2
RIGHT_CUTS = 8
VMEM_BYTES = 59 * 1024 * 1024
MESH = pl.DeviceIdType.MESH
FAR = 2.0 ** 17
FIRST = 1000


def variants(slots, n_col, right_slots):
    scale = slots * (n_col - 1) / 96
    found = []
    for spill, head, middle, rights in (
        (5, 26, 29, 54), (6, 26, 29, 55), (7, 26, 30, 56), (8, 26, 30, 56), (9, 26, 30, 58),
        (10, 27, 31, 58), (12, 27, 31, 60), (14, 28, 32, 60), (18, 28, 32, 60), (24, 32, 32, 64),
    ):
        found.append((
            slots * 18 // 32, max(1, int(spill * scale)), slots * head // 32,
            slots * middle // 32, right_slots * rights // 64,
        ))
    return found + [(slots, 0, slots, slots, right_slots)]


def ordered(levels, end, union, slots, lane_row):
    ma, per = levels.shape[0], slots // levels.shape[0]
    rows, columns = [], []
    lane = lax.broadcasted_iota(jnp.int32, (per, 128), 1)
    line = lax.broadcasted_iota(jnp.int32, (per, 128), 0)
    for m in range(ma):
        kind = jnp.where(
            levels[m:m + 1] + end >= LEVEL_CUT, 0.0,
            jnp.where(levels[m:m + 1] + union >= LEVEL_CUT, 1.0, 2.0),
        )
        level = levels[m:m + 1].astype(jnp.float32)
        key = jnp.where(level >= FIRST / 2, -level, kind * 128.0 + lane_row * ma + m)
        rows.append(jnp.where(lane_row < per, key, 1024.0))
        columns.append(jnp.sum(
            jnp.where(lane == line, jnp.broadcast_to(rows[-1], (per, 128)), 0.0),
            axis=1, keepdims=True,
        ))
    return rows, columns


def spilled(levels, end, main):
    hits = [
        jnp.where(levels[m:m + 1] + end >= LEVEL_CUT, 1.0, 0.0) for m in range(levels.shape[0])
    ]
    size = jnp.sum(functools.reduce(jnp.add, hits), axis=1, keepdims=True)
    return jnp.maximum(size - main, 0.0)


def placed(live, per, lane, line):
    padded = live if live.shape[1] == 128 else jnp.concatenate(
        [live, jnp.zeros((1, 128 - per), jnp.float32)], axis=1
    )
    wide = jnp.broadcast_to(padded, (per, 128))
    own = jnp.sum(jnp.where(lane == line, wide, 0.0), axis=1, keepdims=True)
    first = jnp.sum(jnp.where(lane < line, wide, 0.0), axis=1, keepdims=True)
    return own, first


def plan_kernel(
    sizes, options, left,
    left_level, left_rows, left_count, right_level, right_cols, right_count,
    own_left, lead_down, lead_up, left_meta, right_meta, tiles, perm, choice,
    lead, tile, meta, send, recv, lead_send, lead_recv, lm_send, lm_recv, rm_send, rm_recv, left_sem,
):
    n_kpt, n_row, n_col, sets, per, ma, mb = sizes
    slots = per * ma
    kpt, row, col = (lax.axis_index(name) for name in ("kpt", "row", "col"))
    total = n_kpt * n_row * n_col
    me = (kpt * n_row + row) * n_col + col

    groups = n_kpt * n_row
    group = kpt * n_row + row

    def place_of(far, side):
        other = (group + far) % groups
        return {"kpt": other // n_row, "row": other % n_row, "col": (col + side) % n_col}

    def copy_of(far, side):
        at = far * n_col + side
        return pltpu.make_async_remote_copy(
            src_ref=tile, dst_ref=tiles.at[me], send_sem=send.at[at], recv_sem=recv.at[at],
            device_id=place_of(far, side), device_id_type=MESH,
        )

    def for_others(act):
        @pl.loop(1, groups)
        def _(far):
            for side in range(n_col):
                act(far, side)

        for side in range(1, n_col):
            act(0, side)

    barrier = pltpu.get_barrier_semaphore()
    for_others(lambda far, side: pl.semaphore_signal(
        barrier, inc=1, device_id=place_of(far, side), device_id_type=MESH
    ))
    stages = (
        pltpu.make_async_copy(left, own_left, left_sem),
    )
    for copy in stages:
        copy.start()
    tile[...] = jnp.full(tile.shape, DEAD, jnp.int32)
    live = lax.broadcasted_iota(jnp.int32, (ma, per), 0) < left_count[...]
    levels = jnp.where(live, left_level[...], DEAD)
    tile[:ma, :per] = levels
    lane = lax.broadcasted_iota(jnp.int32, (per, 128), 1)
    line = lax.broadcasted_iota(jnp.int32, (per, 128), 0)
    keys, columns, ranks = [], [], []
    for m in range(ma):
        key = 256 * (8 - tile[m:m + 1, :]) + lane[:1] * ma + m
        keys.append(jnp.where(lane[:1] < per, key, 1024 ** 2))
        wide = jnp.broadcast_to(keys[-1], (per, 128))
        columns.append(jnp.sum(jnp.where(lane == line, wide, 0), axis=1, keepdims=True))
    for m in range(ma):
        before = [jnp.where(key < keys[m], 1, 0) for key in columns]
        rank = jnp.sum(functools.reduce(jnp.add, before), axis=0, keepdims=True)
        ranks.append(jnp.where(lane[:1] < per, rank, slots))
        tile[m:m + 1, :] = jnp.where(ranks[-1] < LEAD, FIRST - ranks[-1], tile[m:m + 1, :])
    marked = tile[:ma, :]
    rights = []
    for which in range(sets):
        live = lax.broadcasted_iota(jnp.int32, (mb, per), 0) < right_count[which]
        rights.append(jnp.where(live, right_level[which], DEAD))
        tile[ma + which:ma + which + 1, :per] = jnp.max(rights[-1], axis=0, keepdims=True)
        size = jnp.sum(right_count[which].astype(jnp.float32), axis=1, keepdims=True)
        tile[ma + which:ma + which + 1, 127:] = size.astype(jnp.int32)
    tiles[me] = tile[...]
    meta[...] = jnp.full(meta.shape, DEAD, jnp.int32)
    meta[:ma, :] = marked
    tail = 2 * ma + 2 * mb * sets
    meta[tail:tail + ma, :per] = levels
    meta[ma:2 * ma, :per] = left_rows[...]
    for which in range(sets):
        base = 2 * ma + which * 2 * mb
        meta[base:base + mb, :per] = right_cols[which]
        meta[base + mb:base + 2 * mb, :per] = rights[which]
    left_meta[col] = meta[...]
    right_meta[row] = meta[...]
    stages[0].wait()
    for at in range(LEAD):
        spots = [jnp.where(rank == at, lane[:1] * ma + m, 0) for m, rank in enumerate(ranks)]
        spot = jnp.max(functools.reduce(jnp.maximum, spots))
        lead[at] = own_left[jnp.minimum(jnp.maximum(spot, 0), slots - 1)]

    def lead_copy(up):
        return pltpu.make_async_remote_copy(
            src_ref=lead, dst_ref=lead_up if up else lead_down,
            send_sem=lead_send.at[int(up)], recv_sem=lead_recv.at[int(up)],
            device_id={"col": col + 1 if up else col - 1}, device_id_type=MESH,
        )

    pl.semaphore_wait(barrier, total - 1)

    for_others(lambda far, side: copy_of(far, side).start())

    def meta_copies():
        for step in range(1, n_col):
            yield pltpu.make_async_remote_copy(
                src_ref=meta, dst_ref=left_meta.at[col],
                send_sem=lm_send.at[step - 1], recv_sem=lm_recv.at[step - 1],
                device_id={"col": (col + step) % n_col}, device_id_type=MESH,
            )
        for step in range(1, n_row):
            yield pltpu.make_async_remote_copy(
                src_ref=meta, dst_ref=right_meta.at[row],
                send_sem=rm_send.at[step - 1], recv_sem=rm_recv.at[step - 1],
                device_id={"row": (row + step) % n_row}, device_id_type=MESH,
            )

    for copy in meta_copies():
        copy.start()
    for up in (False, True):
        pl.when(col + 1 < n_col if up else col > 0)(lead_copy(up).start)

    for_others(lambda far, side: copy_of(far, side).wait_recv())

    def at_device(k, r, c):
        return (k * n_row + r) * n_col + c

    def right_max(k, panel, q):
        return tiles[at_device(k, panel % n_row, q), pl.ds(ma + panel // n_row, 1), :]

    def measure_part(k, carry):
        most_end, most_mid, most_spill, most_right = carry
        spills = [zero, zero]
        for panel in range(n_col):
            levels = [
                jnp.concatenate(
                    [tiles[at_device(k, r, panel), pl.ds(m, 1), :] for r in range(n_row)], axis=0
                )
                for m in range(ma)
            ]

            def needed(most):
                hits = [jnp.where(level + most >= LEVEL_CUT, 1.0, 0.0) for level in levels]
                return jnp.sum(functools.reduce(jnp.add, hits), axis=1, keepdims=True)

            rights = [right_max(k, panel, q) for q in range(n_col)]
            for right in rights:
                most_right = jnp.maximum(most_right, right)
            for way, (taken, right) in enumerate(
                ((panel > 0, rights[0]), (panel < n_col - 1, rights[-1]))
            ):
                if taken:
                    wanted = needed(right)
                    most_end = jnp.maximum(most_end, wanted)
                    spills[way] = spills[way] + jnp.maximum(wanted - main, 0.0)
            if panel > 1:
                union = functools.reduce(jnp.maximum, rights[:panel])
                most_mid = jnp.maximum(most_mid, needed(union))
            if panel < n_col - 2:
                union = functools.reduce(jnp.maximum, rights[panel + 1:])
                most_mid = jnp.maximum(most_mid, needed(union))
        most_spill = jnp.maximum(most_spill, jnp.maximum(*spills))
        return most_end, most_mid, most_spill, most_right

    main = options[0][0]
    zero = jnp.zeros((n_row, 1), jnp.float32)
    most_end, most_mid, most_spill, most_right = lax.fori_loop(
        0, n_kpt, measure_part, (zero, zero, zero, jnp.zeros((1, 128), jnp.int32))
    )
    lanes = lax.broadcasted_iota(jnp.int32, (1, 128), 1)
    most_right = jnp.max(
        jnp.where(lanes == 127, most_right, 0).astype(jnp.float32), axis=1, keepdims=True
    )
    index = zero
    for _, spill, head, middle, limit in options[:-1]:
        over = (most_spill > spill) | (most_end > head) | (most_mid > middle)
        index = index + jnp.where(over | (most_right > limit), 1.0, 0.0)
    choice[0] = jnp.max(index).astype(jnp.int32)

    lane_row = lax.broadcasted_iota(jnp.int32, (1, 128), 1).astype(jnp.float32)
    line = lax.broadcasted_iota(jnp.int32, (per, 128), 0).astype(jnp.float32)
    mine = tiles[me, :ma, :]
    for at, up in enumerate((False, True)):
        which = ma + col // n_row
        near = [
            tiles[at_device(kpt, col % n_row, q), pl.ds(which, 1), :] for q in range(n_col)
        ]
        union = jnp.full((1, 128), DEAD, jnp.int32)
        for q in range(n_col):
            beyond = q > col if up else q < col
            union = jnp.maximum(union, jnp.where(beyond, near[q], DEAD))
        rows, columns = ordered(mine, near[-1] if up else near[0], union, slots, lane_row)
        found = jnp.zeros((1, 128), jnp.float32)
        for m in range(ma):
            before = [jnp.where(key < columns[m], 1.0, 0.0) for key in rows]
            rank = jnp.sum(functools.reduce(jnp.add, before), axis=1, keepdims=True)
            hit = jnp.where(rank == lane_row, line * ma + m, 0.0)
            found = found + jnp.sum(hit, axis=0, keepdims=True)
        perm[pl.ds(at, 1), :] = found.astype(jnp.int32)

    for at, up in ((2, False), (3, True)):
        panels = range(n_col - 2, -1, -1) if up else range(1, n_col)
        code, low = jnp.zeros((1, 128), jnp.float32), jnp.zeros((1, 1), jnp.float32)
        for panel in panels:
            levels = tiles[at_device(kpt, row, panel), :ma, :]
            end = right_max(kpt, panel, n_col - 1 if up else 0)
            high = low + spilled(levels, end, main)
            own = up and panel == n_col - 2
            base = (n_col if own else panel) * slots
            inside = (lane_row >= low) & (lane_row < high)
            code = code + jnp.where(inside, base + lane_row - low, 0.0)
            low = high
        perm[pl.ds(at, 1), :] = code.astype(jnp.int32)
    lane = lax.broadcasted_iota(jnp.int32, (per, 128), 1).astype(jnp.float32)
    for which in range(sets):
        live, first = placed(right_count[which].astype(jnp.float32), per, lane, line)
        found = jnp.zeros((1, 128), jnp.float32)
        for n in range(mb):
            hit = jnp.where((first + n == lane) & (live > n), line * mb + n, 0.0)
            found = found + jnp.sum(hit, axis=0, keepdims=True)
        perm[pl.ds(4 + which, 1), :] = found.astype(jnp.int32)

    for copy in meta_copies():
        copy.wait()
    for up in (False, True):
        pl.when(col + 1 < n_col if up else col > 0)(lead_copy(up).wait_send)
        pl.when(col > 0 if up else col + 1 < n_col)(lead_copy(up).wait_recv)

    for_others(lambda far, side: copy_of(far, side).wait_send())


def order_pairs(sizes, main, kpt, col, tiles, left_meta, right_meta, order):
    n_row, n_col, sets, per, ma, mb, kb_cols = sizes
    slots, high = per * ma, n_col * per
    blocks = GR * kb_cols
    lane_row = lax.broadcasted_iota(jnp.int32, (1, 128), 1).astype(jnp.float32)

    def right_max(panel, q):
        at = (kpt * n_row + panel % n_row) * n_col + q
        return tiles[at, pl.ds(ma + panel // n_row, 1), :]

    lefts = jnp.zeros((2 * ma, 128), jnp.float32)
    rights = jnp.zeros((2 * mb, 128), jnp.float32)
    places = jnp.zeros((8, 128), jnp.float32)
    spots = jnp.zeros((8, 128), jnp.float32)
    thin = lax.broadcasted_iota(jnp.int32, (per, 128), 1).astype(jnp.float32)
    thick = lax.broadcasted_iota(jnp.int32, (per, 128), 0).astype(jnp.float32)
    lows, low = [None] * n_col, jnp.zeros((1, 1), jnp.float32)
    for panel in range(1, n_col):
        lows[panel] = low
        low = low + spilled(left_meta[panel, :ma, :], right_max(panel, 0), main)
    low = jnp.zeros((1, 1), jnp.float32)
    for panel in range(n_col - 2, -1, -1):
        lows[panel] = low if lows[panel] is None else jnp.where(col == 0, lows[panel], low)
        low = low + spilled(left_meta[panel, :ma, :], right_max(panel, n_col - 1), main)
    for panel in range(n_col):
        levels = left_meta[panel, :ma, :]
        down, up = panel > col, panel < col
        end = jnp.where(down, right_max(panel, 0), right_max(panel, n_col - 1))
        union = jnp.full((1, 128), DEAD, jnp.int32)
        for q in range(n_col):
            beyond = down if q < panel else up
            if q != panel:
                union = jnp.maximum(union, jnp.where(beyond, right_max(panel, q), DEAD))
        rows, columns = ordered(levels, end, union, slots, lane_row)
        found = []
        for m in range(ma):
            before = [jnp.where(key < rows[m], 1.0, 0.0) for key in columns]
            rank = jnp.sum(functools.reduce(jnp.add, before), axis=0, keepdims=True)
            own = jnp.where(down | up, rank, lane_row * ma + m) + panel * slots
            far = (down | up) & ((col == 0) | (col == n_col - 1)) & (rank >= main)
            found.append(jnp.where(far, n_col * slots + lows[panel] + rank - main, own))
        found = jnp.concatenate(found + [jnp.zeros((8 - ma, 128), jnp.float32)], axis=0)
        base = 2 * ma + panel // n_row * 2 * mb
        here = (lane_row >= panel * per) & (lane_row < (panel + 1) * per)

        def moved(values):
            values = pltpu.roll(values, panel * per, 1) if panel else values
            return jnp.where(here, values, 0.0)

        tail = 2 * ma + 2 * mb * sets
        left = [left_meta[panel, tail:tail + ma, :], left_meta[panel, ma:2 * ma, :]]
        lefts = lefts + moved(jnp.concatenate(left, axis=0).astype(jnp.float32))
        right = right_meta[panel % n_row, base:base + 2 * mb, :].astype(jnp.float32)
        rights = rights + moved(right)
        places = places + moved(found)
        size = jnp.zeros((1, 128), jnp.float32)
        for n in range(mb):
            size = size + jnp.where((right[mb + n:mb + n + 1] > DEAD / 2) & (lane_row < per), 1.0, 0.0)
        live, _ = placed(size, per, thin, thick)
        first = jnp.sum(jnp.where(thick < thin, live, 0.0), axis=0, keepdims=True)
        spots = spots + moved(
            jnp.broadcast_to(jnp.where(lane_row < per, first, 0.0) + panel * per * mb, (8, 128))
        )

    lane = lax.broadcasted_iota(jnp.int32, (high, 128), 1)
    line = lax.broadcasted_iota(jnp.int32, (high, 128), 0)

    def column(values):
        wide = jnp.broadcast_to(values, (high, 128))
        return jnp.sum(jnp.where(lane == line, wide, 0.0), axis=1, keepdims=True)

    keys, key_columns, code_columns, target_columns = [], [], [], []
    for m in range(ma):
        for n in range(mb):
            kept = lefts[m:m + 1] + rights[mb + n:mb + n + 1] >= LEVEL_CUT
            target = lefts[ma + m:ma + m + 1] * kb_cols + rights[n:n + 1]
            spot = lane_row + (m * mb + n) * 128.0
            key = jnp.where(kept, target * 1024.0 + spot, FAR + spot)
            keys.append(jnp.where(lane_row < high, key, 2 * FAR))
            key_columns.append(column(keys[-1]))
            code = places[m:m + 1] * 1024.0 + spots[:1] + n
            code_columns.append(column(jnp.where(kept, code, 0.0)))
            target_columns.append(column(jnp.where(kept, target, 1.0 * blocks)))
    ranks = []
    for mine in key_columns:
        before = [jnp.where(key < mine, 1.0, 0.0) for key in keys]
        ranks.append(jnp.sum(functools.reduce(jnp.add, before), axis=1, keepdims=True))

    def gathered(hits):
        return jnp.sum(functools.reduce(jnp.add, hits), axis=0, keepdims=True)

    def write(at, values):
        order[pl.ds(at, 1), :] = values.astype(jnp.int32)

    lines = -(-high * ma * mb // 128)
    for at in range(lines):
        spot = lane_row + at * 128.0
        for base, columns in ((0, code_columns), (lines, target_columns)):
            write(base + at, gathered([
                jnp.where(rank == spot, values, 0.0) for rank, values in zip(ranks, columns)
            ]))
    bound = (lane_row + 1.0) * (kb_cols * 1024.0)
    write(2 * lines, gathered([jnp.where(mine < bound, 1.0, 0.0) for mine in key_columns]))
    filled = gathered([jnp.where(mine == lane_row, 1.0, 0.0) for mine in target_columns])
    empty = jnp.where((filled < 0.5) & (lane_row < blocks), 1.0, 0.0)
    lane = lax.broadcasted_iota(jnp.int32, (128, 128), 1).astype(jnp.float32)
    line = lax.broadcasted_iota(jnp.int32, (128, 128), 0).astype(jnp.float32)
    wide = jnp.broadcast_to(empty, (128, 128))
    rank = jnp.sum(jnp.where(lane < line, wide, 0.0), axis=1, keepdims=True)
    flag = jnp.sum(jnp.where(lane == line, wide, 0.0), axis=1, keepdims=True)
    size = jnp.broadcast_to(jnp.sum(empty, axis=1, keepdims=True), (1, 128))
    listed = gathered([jnp.where(rank == lane, line * flag, 0.0)])
    write(2 * lines + 1, jnp.where(lane_row < size, listed, 1.0 * blocks))
    write(2 * lines + 2, size)


def gather_kernel(
    sizes, option, left, own_left, lead_down, lead_up, right, perm, left_meta, right_meta, tiles,
    left_all, right_all, order,
    own_right, packed_down, packed_up, side, spill_down, spill_up,
    up_send, up_recv, down_send, down_recv, spill_send, spill_recv,
    x_send, x_recv, own_send, own_recv, pass_send, pass_recv,
    left_sem, right_sem,
):
    n_row, n_col, sets = sizes[:3]
    row = lax.axis_index("row")
    col = lax.axis_index("col")
    n_chip = n_row // 2
    chip, core = row // 2, row % 2
    partner = chip * 2 + 1 - core
    slots = left.shape[0]
    main, spill, head, middle, limit = option

    barrier = pltpu.get_barrier_semaphore()
    for there, step in ((col > 0, -1), (col + 1 < n_col, 1)):
        @pl.when(there)
        def _():
            pl.semaphore_signal(
                barrier, inc=1, device_id={"col": col + step}, device_id_type=MESH
            )
    others = [partner] + [((chip + step) % n_chip) * 2 + core for step in range(1, n_chip)]
    for other in others:
        pl.semaphore_signal(barrier, inc=1, device_id={"row": other}, device_id_type=MESH)
    kept = pltpu.make_async_copy(left, left_all.at[pl.ds(col * slots, slots)], left_sem)
    kept.start()

    bounds = [LEAD + (main - LEAD) * at // MAIN_CUTS for at in range(MAIN_CUTS + 1)]
    cuts = [(low, high, "main") for low, high in zip(bounds, bounds[1:])]
    cuts.append((0, LEAD, "lead"))
    if head > main:
        cuts.append((main, head, "side"))
    if middle > head:
        cuts.append((head, middle, "rest"))
    bounds = [limit * at // RIGHT_CUTS for at in range(RIGHT_CUTS + 1)]
    right_cuts = [pl.ds(low, high - low) for low, high in zip(bounds, bounds[1:])]

    def left_copy(step, cut, up):
        low, high, kind = cuts[cut]
        panel = col - step if up else col + step
        span = pl.ds(panel * slots + low, high - low)
        target = side.at[span] if kind == "side" else left_all.at[span]
        source = (packed_up if up else packed_down).at[pl.ds(low, high - low)]
        if kind == "lead" and step == 1:
            source = lead_up if up else lead_down
        send, recv = (up_send, up_recv) if up else (down_send, down_recv)
        return pltpu.make_async_remote_copy(
            src_ref=source if step == int(kind == "lead") else target, dst_ref=target,
            send_sem=send.at[step, cut], recv_sem=recv.at[step, cut],
            device_id={"col": col + 1 if up else col - 1}, device_id_type=MESH,
        )

    def left_sends(step, cut, up):
        mid = 0 if cuts[cut][2] in ("main", "lead") else 1
        if up:
            return (col + 1 < n_col - mid) & (col - step >= 0)
        return (col - 1 >= mid) & (col + step < n_col)

    def left_receives(step, cut, up):
        mid = 0 if cuts[cut][2] in ("main", "lead") else 1
        if up:
            return (col - 1 - step >= 0) & (col < n_col - mid)
        return (col + 1 + step < n_col) & (col >= mid)

    def start_left(step, cut):
        for up in (True, False):
            pl.when(left_sends(step, cut, up))(left_copy(step, cut, up).start)

    def steps_of(kind):
        if kind == "lead":
            return range(1, n_col - 1)
        return range(n_col - 1 if kind == "main" else n_col - 2)

    def spill_copy(up):
        return pltpu.make_async_remote_copy(
            src_ref=spill_up if up else spill_down,
            dst_ref=left_all.at[pl.ds(n_col * slots, spill)],
            send_sem=spill_send.at[int(up)], recv_sem=spill_recv.at[int(up)],
            device_id={"col": n_col - 1 if up else 0}, device_id_type=MESH,
        )

    def across(step, cut):
        span = right_cuts[cut]
        other = ((chip + step) % n_chip) * 2 + core
        return pltpu.make_async_remote_copy(
            src_ref=right_all.at[:, row, span], dst_ref=right_all.at[:, row, span],
            send_sem=x_send.at[step - 1, cut], recv_sem=x_recv.at[step - 1, cut],
            device_id={"row": other}, device_id_type=MESH,
        )

    def passed(step, cut):
        span = right_cuts[cut]
        panel = ((chip + n_chip - step) % n_chip) * 2 + core
        return pltpu.make_async_remote_copy(
            src_ref=right_all.at[:, panel, span], dst_ref=right_all.at[:, panel, span],
            send_sem=pass_send.at[step - 1, cut], recv_sem=pass_recv.at[step - 1, cut],
            device_id={"row": partner}, device_id_type=MESH,
        )

    own = pltpu.make_async_remote_copy(
        src_ref=right_all.at[:, row, pl.ds(0, limit)],
        dst_ref=right_all.at[:, row, pl.ds(0, limit)],
        send_sem=own_send, recv_sem=own_recv,
        device_id={"row": partner}, device_id_type=MESH,
    )

    def pack_left(low, high):
        @pl.loop(low, high)
        def _(at):
            packed_down[at] = own_left[perm[0, at]]
            packed_up[at] = own_left[perm[1, at]]

    pack_left(*cuts[0][:2])
    pl.semaphore_wait(
        barrier, len(others) + jnp.where(col > 0, 1, 0) + jnp.where(col + 1 < n_col, 1, 0)
    )
    start_left(0, 0)
    staged = pltpu.make_async_copy(right, own_right, right_sem)
    staged.start()
    pack_left(cuts[0][1], middle)
    for cut in range(1, len(cuts)):
        if cuts[cut][2] == "main":
            start_left(0, cut)
        elif cuts[cut][2] == "lead" and n_col > 2:
            start_left(1, cut)

    staged.wait()
    for which in range(sets):
        @pl.loop(0, limit)
        def _(at):
            right_all[which, row, at] = own_right[which, perm[4 + which, at]]

    for step in range(1, n_chip):
        for cut in range(RIGHT_CUTS):
            across(step, cut).start()
    own.start()
    if spill:
        @pl.loop(main, head)
        def _(at):
            side[col * slots + at] = packed_down[at]
            side[n_col * slots + at] = packed_up[at]

    def take_left(step, cut):
        for up in (True, False):
            pl.when(left_receives(step, cut, up))(left_copy(step, cut, up).wait_recv)
            if step + 1 < n_col - 1:
                pl.when(left_sends(step + 1, cut, up))(left_copy(step + 1, cut, up).start)

    def take_right(step, cut):
        across(step, cut).wait_recv()
        passed(step, cut).start()

    def take_order():
        for panel, there, found in (
            (col + 1, col + 1 < n_col, lead_down), (col - 1, col > 0, lead_up)
        ):
            @pl.when(there)
            def _():
                for at in range(LEAD):
                    left_all[panel * slots + at] = found[at]

        order_pairs(
            sizes, main, lax.axis_index("kpt"), col, tiles, left_meta, right_meta, order
        )

    def send_spill():
        for up in (False, True):
            target, line = (spill_up, 3) if up else (spill_down, 2)

            @pl.when(col == (n_col - 2 if up else 1))
            def _():
                @pl.loop(0, spill)
                def _(at):
                    target[at] = side[perm[line, at] + main]

                spill_copy(up).start()

    def take_sides():
        for step in range(1, n_col):
            for panel, there in (
                (col - step, (col - step >= 0) & (col < n_col - 1)),
                (col + step, (col + step < n_col) & (col > 0)),
            ):
                @pl.when(there)
                def _():
                    @pl.loop(main, head)
                    def _(at):
                        left_all[panel * slots + at] = side[panel * slots + at]

    mains, heads = (n_col - 2) * main - LEAD, (n_col - 2) * head - LEAD
    jobs = [(7, take_order)]
    if spill:
        jobs.append((heads + 0.02, send_spill))
    if head > main:
        jobs.append((heads + 0.03, take_sides))
    for cut, (low, high, kind) in enumerate(cuts):
        start = functools.partial(start_left, 0, cut)
        if kind == "side":
            jobs.append(((n_col - 3) * main - LEAD + 0.01, start))
        elif kind == "rest":
            jobs.append((mains + (n_col - 3) * (head - main) + 0.01, start))
        for step in steps_of(kind):
            when = step * main + high - LEAD
            if kind == "side":
                when = mains + (step + 1) * (high - low)
            elif kind == "rest":
                when = heads + (step + 1) * (high - low) + 0.04
            jobs.append((when, functools.partial(take_left, step, cut)))
    for step in range(1, n_chip):
        for cut in range(RIGHT_CUTS):
            when = ((step - 1) * RIGHT_CUTS + cut + 1) * limit * sets / RIGHT_CUTS + 2
            jobs.append((when, functools.partial(take_right, step, cut)))
    for _, job in sorted(jobs, key=lambda entry: entry[0]):
        job()

    kept.wait()
    if spill:
        for up in (False, True):
            pl.when(col == (n_col - 1 if up else 0))(spill_copy(up).wait_recv)
            pl.when(col == (n_col - 2 if up else 1))(spill_copy(up).wait_send)
    own.wait()
    for step in range(1, n_chip):
        for cut in range(RIGHT_CUTS):
            across(step, cut).wait_send()
            passed(step, cut).wait()
    for cut, entry in enumerate(cuts):
        for step in steps_of(entry[2]):
            for up in (True, False):
                pl.when(left_sends(step, cut, up))(left_copy(step, cut, up).wait_send)


def product_kernel(sizes, left, right, order, out, stage, partial, out_sem):
    n_row, n_col, sets, per, ma, mb, kb_cols = sizes
    blocks = GR * kb_cols
    lines = -(-n_col * per * ma * mb // 128)
    width = stage.shape[2]
    empty = jnp.zeros(stage.shape[1:], stage.dtype)

    @pl.loop(0, (order[2 * lines + 2, 0] + 3) // 4)
    def _(at):
        for lane in range(4):
            stage[order[2 * lines + 1, at * 4 + lane]] = empty

    def out_copy(line):
        span = pl.ds(line * kb_cols, kb_cols)
        return pltpu.make_async_copy(stage.at[span], out.at[span], out_sem.at[line])

    count = order[2 * lines, GR - 1]

    def group(at, carry):
        line, last = carry
        codes, targets, done = [], [], []
        for lane in range(GROUP):
            spot = at * GROUP + lane
            codes.append(order[spot // 128, spot % 128])
            targets.append(order[lines + spot // 128, spot % 128])
        for code in codes:
            block = left[code // 1024]
            wide = jnp.concatenate([block[:width], block[width:]], axis=1)
            other = right[code % 1024]
            real, imag = other[:width], other[width:]
            matrix = jnp.concatenate(
                [jnp.concatenate([real, imag], axis=1), jnp.concatenate([-imag, real], axis=1)],
                axis=0,
            )
            done.append(jnp.dot(wide, matrix, preferred_element_type=jnp.float32))
        held = partial[...]
        for target, product in zip(targets, done):
            held = jnp.where(target == last, held, 0.0) + product
            value = held.astype(stage.dtype)
            stage[target, :width] = value[:, :width]
            stage[target, width:] = value[:, width:]
            last = target
        partial[...] = held
        for _ in range(1 + GROUP // 12):
            ready = (line < GR) & (at * GROUP >= order[2 * lines, jnp.minimum(line, GR - 1)])
            pl.when(ready)(out_copy(jnp.minimum(line, GR - 1)).start)
            line = line + jnp.where(ready, 1, 0)
        return line, last

    partial[...] = jnp.zeros(partial.shape, partial.dtype)
    line, _ = lax.fori_loop(
        0, (count + GROUP - 1) // GROUP, group, (jnp.int32(0), jnp.int32(-1))
    )

    @pl.loop(line, GR)
    def _(line):
        out_copy(line).start()

    @pl.loop(0, GR)
    def _(line):
        out_copy(line).wait()


def body(
    n_kpt, n_row, n_col, left_blocks, left_rows, left_count, left_level,
    right_blocks, right_cols, right_count, right_level,
):
    _, per, ma, _, width, _ = left_blocks.shape
    sets, right_per, _, mb = right_blocks.shape[:4]
    assert right_per == per and sets * n_row == n_col and n_row % 2 == 0 and sets <= 2
    blocks = GR * (n_row * sets * per // n_col)
    assert n_col * per <= 128 and per * ma <= 128 and blocks <= 128 and ma * mb <= 8
    slots = per * ma
    left = left_blocks.reshape(slots, 2 * width, width)
    right = right_blocks.reshape(sets, per * mb, 2 * width, width)
    any_space = pl.BlockSpec(memory_space=pl.ANY)
    vmem = pl.BlockSpec(memory_space=pltpu.VMEM)
    smem = pl.BlockSpec(memory_space=pltpu.SMEM)
    dma = pltpu.SemaphoreType.DMA
    n_chip = n_row // 2
    total = n_kpt * n_row * n_col
    options = variants(slots, n_col, per * mb)
    sizes = (n_row, n_col, sets, per, ma, mb, n_row * sets * per // n_col)
    tile_rows = -(-(ma + sets) // 4) * 4
    meta_rows = -(-(3 * ma + 2 * mb * sets) // 8) * 8
    lines = -(-n_col * per * ma * mb // 128)
    order_rows = -(-(2 * lines + 3) // 8) * 8
    own_left, lead_down, lead_up, left_meta, right_meta, tiles, perm, choice = pl.pallas_call(
        functools.partial(plan_kernel, (n_kpt,) + sizes[:-1], options),
        out_shape=(
            pltpu.VMEM(left.shape, left.dtype),
            *[pltpu.VMEM((LEAD,) + left.shape[1:], left.dtype)] * 2,
            jax.ShapeDtypeStruct((n_col, meta_rows, 128), jnp.int32),
            jax.ShapeDtypeStruct((n_row, meta_rows, 128), jnp.int32),
            jax.ShapeDtypeStruct((total, tile_rows, 128), jnp.int32),
            jax.ShapeDtypeStruct((8, 128), jnp.int32),
            jax.ShapeDtypeStruct((1,), jnp.int32),
        ),
        in_specs=[any_space] + [vmem] * 6,
        out_specs=(vmem,) * 7 + (smem,),
        scratch_shapes=[
            pltpu.VMEM((LEAD,) + left.shape[1:], left.dtype),
            pltpu.VMEM((tile_rows, 128), jnp.int32),
            pltpu.VMEM((meta_rows, 128), jnp.int32),
            *[dma((total,))] * 2,
            *[dma((2,))] * 2,
            *[dma((n_col - 1,))] * 2,
            *[dma((n_row - 1,))] * 2,
            dma,
        ],
        compiler_params=pltpu.CompilerParams(collective_id=0, has_side_effects=True),
        name="plan",
    )(
        left, left_level[0].T, left_rows[0].T, left_count,
        right_level[:, :, 0].transpose(0, 2, 1), right_cols[:, :, 0].transpose(0, 2, 1),
        right_count.transpose(0, 2, 1),
    )

    kb_cols = sizes[-1]
    right_shape = (sets, n_row) + right.shape[1:]
    assert LEAD <= per
    most = (n_col + 1) * left.size + 2 * LEAD * left.size // slots + n_row * right.size + 24 * left.size // slots
    limit = VMEM_BYTES - most * left.dtype.itemsize

    def run(at, left, own_left, lead_down, lead_up, right, perm, left_meta, right_meta, tiles):
        cuts, spill = MAIN_CUTS + 3, max(options[at][1], 1)
        left_all, right_all, order = pl.pallas_call(
            functools.partial(gather_kernel, sizes, options[at]),
            out_shape=(
                pltpu.VMEM((n_col * slots + options[at][1],) + left.shape[1:], left.dtype),
                pltpu.VMEM(right_shape, right.dtype),
                jax.ShapeDtypeStruct((order_rows, 128), jnp.int32),
            ),
            in_specs=[any_space, vmem, vmem, vmem, any_space, smem, vmem, vmem, vmem],
            out_specs=(vmem, vmem, vmem),
            scratch_shapes=[
                pltpu.VMEM(right.shape, right.dtype),
                *[pltpu.VMEM(left.shape, left.dtype)] * 2,
                pltpu.VMEM(((n_col + 1) * slots,) + left.shape[1:], left.dtype),
                *[pltpu.VMEM((spill,) + left.shape[1:], left.dtype)] * 2,
                *[dma((n_col - 1, cuts))] * 4,
                *[dma((2,))] * 2,
                *[dma((n_chip - 1, RIGHT_CUTS))] * 2,
                *[dma] * 2,
                *[dma((n_chip - 1, RIGHT_CUTS))] * 2,
                *[dma] * 2,
            ],
            compiler_params=pltpu.CompilerParams(
                collective_id=1 + at, has_side_effects=True, vmem_limit_bytes=limit
            ),
            name=f"gather_panels_{at}",
        )(
            left, pltpu.with_memory_space_constraint(own_left, pltpu.VMEM),
            pltpu.with_memory_space_constraint(lead_down, pltpu.VMEM),
            pltpu.with_memory_space_constraint(lead_up, pltpu.VMEM),
            right, perm, left_meta, right_meta, tiles,
        )
        return pl.pallas_call(
            functools.partial(product_kernel, sizes),
            out_shape=jax.ShapeDtypeStruct((blocks, 2 * width, width), jnp.bfloat16),
            in_specs=[vmem, vmem, smem],
            out_specs=any_space,
            scratch_shapes=[
                pltpu.VMEM((blocks + 1, 2 * width, width), jnp.bfloat16),
                pltpu.VMEM((width, 2 * width), jnp.float32),
                dma((GR,)),
            ],
            compiler_params=pltpu.CompilerParams(vmem_limit_bytes=limit),
            name="pair_products",
        )(
            pltpu.with_memory_space_constraint(
                left_all, pltpu.VMEM
            ),
            pltpu.with_memory_space_constraint(
                right_all.reshape((-1,) + right.shape[2:]), pltpu.VMEM
            ),
            order,
        )

    out = lax.switch(
        choice[0], [functools.partial(run, at) for at in range(len(options))],
        left, own_left, lead_down, lead_up, right, perm, left_meta, right_meta, tiles,
    )
    return out.reshape(GR, kb_cols, 2, width, width)


def solution(mesh):
    in_specs = (
        P(("kpt", "row"), "col", None, None, None, None),
        P(("kpt", "row"), "col", None),
        P(("kpt", "row"), "col"),
        P(("kpt", "row"), "col", None),
        P("kpt", "row", "col", None, None, None, None),
        P("kpt", "row", "col", None),
        P("kpt", "row", "col"),
        P("kpt", "row", "col", None),
    )
    out_specs = P(("kpt", "row"), "col", None, None, None)
    return jax.shard_map(
        functools.partial(body, mesh.shape["kpt"], mesh.shape["row"], mesh.shape["col"]),
        mesh=mesh, in_specs=in_specs, out_specs=out_specs, check_vma=False,
    )
```

```python
import functools

import jax
import jax.numpy as jnp
from jax import lax
from jax.experimental import pallas as pl
from jax.experimental.pallas import tpu as pltpu
from jax.sharding import PartitionSpec as P

GR = 8
LEVEL_CUT = 7
DEAD = -1000
GROUP = 24
LEAD = 3
MAIN_CUTS = 2
RIGHT_CUTS = 8
VMEM_BYTES = 59 * 1024 * 1024
MESH = pl.DeviceIdType.MESH
FAR = 2.0 ** 17
FIRST = 1000


def variants(slots, n_col, right_slots):
    scale = slots * (n_col - 1) / 96
    found = []
    for spill, head, middle, rights in (
        (5, 26, 29, 54), (7, 26, 29, 55), (8, 26, 30, 55), (9, 26, 30, 56),
        (10, 27, 30, 56), (12, 27, 31, 58), (14, 28, 32, 60), (18, 28, 32, 60), (24, 32, 32, 64),
    ):
        found.append((
            slots * 18 // 32, max(1, int(spill * scale)), slots * head // 32,
            slots * middle // 32, right_slots * rights // 64,
        ))
    return found + [(slots, 0, slots, slots, right_slots)]


def ordered(levels, end, union, slots, lane_row):
    ma, per = levels.shape[0], slots // levels.shape[0]
    rows, columns = [], []
    lane = lax.broadcasted_iota(jnp.int32, (per, 128), 1)
    line = lax.broadcasted_iota(jnp.int32, (per, 128), 0)
    for m in range(ma):
        kind = jnp.where(
            levels[m:m + 1] + end >= LEVEL_CUT, 0.0,
            jnp.where(levels[m:m + 1] + union >= LEVEL_CUT, 1.0, 2.0),
        )
        level = levels[m:m + 1].astype(jnp.float32)
        key = jnp.where(level >= FIRST / 2, -level, kind * 128.0 + lane_row * ma + m)
        rows.append(jnp.where(lane_row < per, key, 1024.0))
        columns.append(jnp.sum(
            jnp.where(lane == line, jnp.broadcast_to(rows[-1], (per, 128)), 0.0),
            axis=1, keepdims=True,
        ))
    return rows, columns


def spilled(levels, end, main):
    hits = [
        jnp.where(levels[m:m + 1] + end >= LEVEL_CUT, 1.0, 0.0) for m in range(levels.shape[0])
    ]
    size = jnp.sum(functools.reduce(jnp.add, hits), axis=1, keepdims=True)
    return jnp.maximum(size - main, 0.0)


def placed(live, per, lane, line):
    padded = live if live.shape[1] == 128 else jnp.concatenate(
        [live, jnp.zeros((1, 128 - per), jnp.float32)], axis=1
    )
    wide = jnp.broadcast_to(padded, (per, 128))
    own = jnp.sum(jnp.where(lane == line, wide, 0.0), axis=1, keepdims=True)
    first = jnp.sum(jnp.where(lane < line, wide, 0.0), axis=1, keepdims=True)
    return own, first


def plan_kernel(
    sizes, options, left,
    left_level, left_rows, left_count, right_level, right_cols, right_count,
    own_left, lead_down, lead_up, left_meta, right_meta, tiles, perm, choice,
    lead, tile, meta, send, recv, lead_send, lead_recv, lm_send, lm_recv, rm_send, rm_recv, left_sem,
):
    n_kpt, n_row, n_col, sets, per, ma, mb = sizes
    slots = per * ma
    kpt, row, col = (lax.axis_index(name) for name in ("kpt", "row", "col"))
    total = n_kpt * n_row * n_col
    me = (kpt * n_row + row) * n_col + col

    groups = n_kpt * n_row
    group = kpt * n_row + row

    def place_of(far, side):
        other = (group + far) % groups
        return {"kpt": other // n_row, "row": other % n_row, "col": (col + side) % n_col}

    def copy_of(far, side):
        at = far * n_col + side
        return pltpu.make_async_remote_copy(
            src_ref=tile, dst_ref=tiles.at[me], send_sem=send.at[at], recv_sem=recv.at[at],
            device_id=place_of(far, side), device_id_type=MESH,
        )

    def for_others(act):
        @pl.loop(1, groups)
        def _(far):
            for side in range(n_col):
                act(far, side)

        for side in range(1, n_col):
            act(0, side)

    barrier = pltpu.get_barrier_semaphore()
    for_others(lambda far, side: pl.semaphore_signal(
        barrier, inc=1, device_id=place_of(far, side), device_id_type=MESH
    ))
    stages = (
        pltpu.make_async_copy(left, own_left, left_sem),
    )
    for copy in stages:
        copy.start()
    tile[...] = jnp.full(tile.shape, DEAD, jnp.int32)
    live = lax.broadcasted_iota(jnp.int32, (ma, per), 0) < left_count[...]
    levels = jnp.where(live, left_level[...], DEAD)
    tile[:ma, :per] = levels
    lane = lax.broadcasted_iota(jnp.int32, (per, 128), 1)
    line = lax.broadcasted_iota(jnp.int32, (per, 128), 0)
    keys, columns, ranks = [], [], []
    for m in range(ma):
        key = 256 * (8 - tile[m:m + 1, :]) + lane[:1] * ma + m
        keys.append(jnp.where(lane[:1] < per, key, 1024 ** 2))
        wide = jnp.broadcast_to(keys[-1], (per, 128))
        columns.append(jnp.sum(jnp.where(lane == line, wide, 0), axis=1, keepdims=True))
    for m in range(ma):
        before = [jnp.where(key < keys[m], 1, 0) for key in columns]
        rank = jnp.sum(functools.reduce(jnp.add, before), axis=0, keepdims=True)
        ranks.append(jnp.where(lane[:1] < per, rank, slots))
        tile[m:m + 1, :] = jnp.where(ranks[-1] < LEAD, FIRST - ranks[-1], tile[m:m + 1, :])
    marked = tile[:ma, :]
    rights = []
    for which in range(sets):
        live = lax.broadcasted_iota(jnp.int32, (mb, per), 0) < right_count[which]
        rights.append(jnp.where(live, right_level[which], DEAD))
        tile[ma + which:ma + which + 1, :per] = jnp.max(rights[-1], axis=0, keepdims=True)
        size = jnp.sum(right_count[which].astype(jnp.float32), axis=1, keepdims=True)
        tile[ma + which:ma + which + 1, 127:] = size.astype(jnp.int32)
    tiles[me] = tile[...]
    meta[...] = jnp.full(meta.shape, DEAD, jnp.int32)
    meta[:ma, :] = marked
    tail = 2 * ma + 2 * mb * sets
    meta[tail:tail + ma, :per] = levels
    meta[ma:2 * ma, :per] = left_rows[...]
    for which in range(sets):
        base = 2 * ma + which * 2 * mb
        meta[base:base + mb, :per] = right_cols[which]
        meta[base + mb:base + 2 * mb, :per] = rights[which]
    left_meta[col] = meta[...]
    right_meta[row] = meta[...]
    stages[0].wait()
    for at in range(LEAD):
        spots = [jnp.where(rank == at, lane[:1] * ma + m, 0) for m, rank in enumerate(ranks)]
        spot = jnp.max(functools.reduce(jnp.maximum, spots))
        lead[at] = own_left[jnp.minimum(jnp.maximum(spot, 0), slots - 1)]

    def lead_copy(up):
        return pltpu.make_async_remote_copy(
            src_ref=lead, dst_ref=lead_up if up else lead_down,
            send_sem=lead_send.at[int(up)], recv_sem=lead_recv.at[int(up)],
            device_id={"col": col + 1 if up else col - 1}, device_id_type=MESH,
        )

    pl.semaphore_wait(barrier, total - 1)

    for_others(lambda far, side: copy_of(far, side).start())

    def meta_copies():
        for step in range(1, n_col):
            yield pltpu.make_async_remote_copy(
                src_ref=meta, dst_ref=left_meta.at[col],
                send_sem=lm_send.at[step - 1], recv_sem=lm_recv.at[step - 1],
                device_id={"col": (col + step) % n_col}, device_id_type=MESH,
            )
        for step in range(1, n_row):
            yield pltpu.make_async_remote_copy(
                src_ref=meta, dst_ref=right_meta.at[row],
                send_sem=rm_send.at[step - 1], recv_sem=rm_recv.at[step - 1],
                device_id={"row": (row + step) % n_row}, device_id_type=MESH,
            )

    for copy in meta_copies():
        copy.start()
    for up in (False, True):
        pl.when(col + 1 < n_col if up else col > 0)(lead_copy(up).start)

    for_others(lambda far, side: copy_of(far, side).wait_recv())

    def at_device(k, r, c):
        return (k * n_row + r) * n_col + c

    def right_max(k, panel, q):
        return tiles[at_device(k, panel % n_row, q), pl.ds(ma + panel // n_row, 1), :]

    def measure_part(k, carry):
        most_end, most_mid, most_spill, most_right = carry
        spills = [zero, zero]
        for panel in range(n_col):
            levels = [
                jnp.concatenate(
                    [tiles[at_device(k, r, panel), pl.ds(m, 1), :] for r in range(n_row)], axis=0
                )
                for m in range(ma)
            ]

            def needed(most):
                hits = [jnp.where(level + most >= LEVEL_CUT, 1.0, 0.0) for level in levels]
                return jnp.sum(functools.reduce(jnp.add, hits), axis=1, keepdims=True)

            rights = [right_max(k, panel, q) for q in range(n_col)]
            for right in rights:
                most_right = jnp.maximum(most_right, right)
            for way, (taken, right) in enumerate(
                ((panel > 0, rights[0]), (panel < n_col - 1, rights[-1]))
            ):
                if taken:
                    wanted = needed(right)
                    most_end = jnp.maximum(most_end, wanted)
                    spills[way] = spills[way] + jnp.maximum(wanted - main, 0.0)
            if panel > 1:
                union = functools.reduce(jnp.maximum, rights[:panel])
                most_mid = jnp.maximum(most_mid, needed(union))
            if panel < n_col - 2:
                union = functools.reduce(jnp.maximum, rights[panel + 1:])
                most_mid = jnp.maximum(most_mid, needed(union))
        most_spill = jnp.maximum(most_spill, jnp.maximum(*spills))
        return most_end, most_mid, most_spill, most_right

    main = options[0][0]
    zero = jnp.zeros((n_row, 1), jnp.float32)
    most_end, most_mid, most_spill, most_right = lax.fori_loop(
        0, n_kpt, measure_part, (zero, zero, zero, jnp.zeros((1, 128), jnp.int32))
    )
    lanes = lax.broadcasted_iota(jnp.int32, (1, 128), 1)
    most_right = jnp.max(
        jnp.where(lanes == 127, most_right, 0).astype(jnp.float32), axis=1, keepdims=True
    )
    index = zero
    for _, spill, head, middle, limit in options[:-1]:
        over = (most_spill > spill) | (most_end > head) | (most_mid > middle)
        index = index + jnp.where(over | (most_right > limit), 1.0, 0.0)
    choice[0] = jnp.max(index).astype(jnp.int32)

    lane_row = lax.broadcasted_iota(jnp.int32, (1, 128), 1).astype(jnp.float32)
    line = lax.broadcasted_iota(jnp.int32, (per, 128), 0).astype(jnp.float32)
    mine = tiles[me, :ma, :]
    for at, up in enumerate((False, True)):
        which = ma + col // n_row
        near = [
            tiles[at_device(kpt, col % n_row, q), pl.ds(which, 1), :] for q in range(n_col)
        ]
        union = jnp.full((1, 128), DEAD, jnp.int32)
        for q in range(n_col):
            beyond = q > col if up else q < col
            union = jnp.maximum(union, jnp.where(beyond, near[q], DEAD))
        rows, columns = ordered(mine, near[-1] if up else near[0], union, slots, lane_row)
        found = jnp.zeros((1, 128), jnp.float32)
        for m in range(ma):
            before = [jnp.where(key < columns[m], 1.0, 0.0) for key in rows]
            rank = jnp.sum(functools.reduce(jnp.add, before), axis=1, keepdims=True)
            hit = jnp.where(rank == lane_row, line * ma + m, 0.0)
            found = found + jnp.sum(hit, axis=0, keepdims=True)
        perm[pl.ds(at, 1), :] = found.astype(jnp.int32)

    for at, up in ((2, False), (3, True)):
        panels = range(n_col - 2, -1, -1) if up else range(1, n_col)
        code, low = jnp.zeros((1, 128), jnp.float32), jnp.zeros((1, 1), jnp.float32)
        for panel in panels:
            levels = tiles[at_device(kpt, row, panel), :ma, :]
            end = right_max(kpt, panel, n_col - 1 if up else 0)
            high = low + spilled(levels, end, main)
            own = up and panel == n_col - 2
            base = (n_col if own else panel) * slots
            inside = (lane_row >= low) & (lane_row < high)
            code = code + jnp.where(inside, base + lane_row - low, 0.0)
            low = high
        perm[pl.ds(at, 1), :] = code.astype(jnp.int32)
    lane = lax.broadcasted_iota(jnp.int32, (per, 128), 1).astype(jnp.float32)
    for which in range(sets):
        live, first = placed(right_count[which].astype(jnp.float32), per, lane, line)
        found = jnp.zeros((1, 128), jnp.float32)
        for n in range(mb):
            hit = jnp.where((first + n == lane) & (live > n), line * mb + n, 0.0)
            found = found + jnp.sum(hit, axis=0, keepdims=True)
        perm[pl.ds(4 + which, 1), :] = found.astype(jnp.int32)

    for copy in meta_copies():
        copy.wait()
    for up in (False, True):
        pl.when(col + 1 < n_col if up else col > 0)(lead_copy(up).wait_send)
        pl.when(col > 0 if up else col + 1 < n_col)(lead_copy(up).wait_recv)

    for_others(lambda far, side: copy_of(far, side).wait_send())


def order_pairs(sizes, main, kpt, col, tiles, left_meta, right_meta, order):
    n_row, n_col, sets, per, ma, mb, kb_cols = sizes
    slots, high = per * ma, n_col * per
    blocks = GR * kb_cols
    lane_row = lax.broadcasted_iota(jnp.int32, (1, 128), 1).astype(jnp.float32)

    def right_max(panel, q):
        at = (kpt * n_row + panel % n_row) * n_col + q
        return tiles[at, pl.ds(ma + panel // n_row, 1), :]

    lefts = jnp.zeros((2 * ma, 128), jnp.float32)
    rights = jnp.zeros((2 * mb, 128), jnp.float32)
    places = jnp.zeros((8, 128), jnp.float32)
    spots = jnp.zeros((8, 128), jnp.float32)
    thin = lax.broadcasted_iota(jnp.int32, (per, 128), 1).astype(jnp.float32)
    thick = lax.broadcasted_iota(jnp.int32, (per, 128), 0).astype(jnp.float32)
    lows, low = [None] * n_col, jnp.zeros((1, 1), jnp.float32)
    for panel in range(1, n_col):
        lows[panel] = low
        low = low + spilled(left_meta[panel, :ma, :], right_max(panel, 0), main)
    low = jnp.zeros((1, 1), jnp.float32)
    for panel in range(n_col - 2, -1, -1):
        lows[panel] = low if lows[panel] is None else jnp.where(col == 0, lows[panel], low)
        low = low + spilled(left_meta[panel, :ma, :], right_max(panel, n_col - 1), main)
    for panel in range(n_col):
        levels = left_meta[panel, :ma, :]
        down, up = panel > col, panel < col
        end = jnp.where(down, right_max(panel, 0), right_max(panel, n_col - 1))
        union = jnp.full((1, 128), DEAD, jnp.int32)
        for q in range(n_col):
            beyond = down if q < panel else up
            if q != panel:
                union = jnp.maximum(union, jnp.where(beyond, right_max(panel, q), DEAD))
        rows, columns = ordered(levels, end, union, slots, lane_row)
        found = []
        for m in range(ma):
            before = [jnp.where(key < rows[m], 1.0, 0.0) for key in columns]
            rank = jnp.sum(functools.reduce(jnp.add, before), axis=0, keepdims=True)
            own = jnp.where(down | up, rank, lane_row * ma + m) + panel * slots
            far = (down | up) & ((col == 0) | (col == n_col - 1)) & (rank >= main)
            found.append(jnp.where(far, n_col * slots + lows[panel] + rank - main, own))
        found = jnp.concatenate(found + [jnp.zeros((8 - ma, 128), jnp.float32)], axis=0)
        base = 2 * ma + panel // n_row * 2 * mb
        here = (lane_row >= panel * per) & (lane_row < (panel + 1) * per)

        def moved(values):
            values = pltpu.roll(values, panel * per, 1) if panel else values
            return jnp.where(here, values, 0.0)

        tail = 2 * ma + 2 * mb * sets
        left = [left_meta[panel, tail:tail + ma, :], left_meta[panel, ma:2 * ma, :]]
        lefts = lefts + moved(jnp.concatenate(left, axis=0).astype(jnp.float32))
        right = right_meta[panel % n_row, base:base + 2 * mb, :].astype(jnp.float32)
        rights = rights + moved(right)
        places = places + moved(found)
        size = jnp.zeros((1, 128), jnp.float32)
        for n in range(mb):
            size = size + jnp.where((right[mb + n:mb + n + 1] > DEAD / 2) & (lane_row < per), 1.0, 0.0)
        live, _ = placed(size, per, thin, thick)
        first = jnp.sum(jnp.where(thick < thin, live, 0.0), axis=0, keepdims=True)
        spots = spots + moved(
            jnp.broadcast_to(jnp.where(lane_row < per, first, 0.0) + panel * per * mb, (8, 128))
        )

    lane = lax.broadcasted_iota(jnp.int32, (high, 128), 1)
    line = lax.broadcasted_iota(jnp.int32, (high, 128), 0)

    def column(values):
        wide = jnp.broadcast_to(values, (high, 128))
        return jnp.sum(jnp.where(lane == line, wide, 0.0), axis=1, keepdims=True)

    keys, key_columns, code_columns, target_columns = [], [], [], []
    for m in range(ma):
        for n in range(mb):
            kept = lefts[m:m + 1] + rights[mb + n:mb + n + 1] >= LEVEL_CUT
            target = lefts[ma + m:ma + m + 1] * kb_cols + rights[n:n + 1]
            spot = lane_row + (m * mb + n) * 128.0
            key = jnp.where(kept, target * 1024.0 + spot, FAR + spot)
            keys.append(jnp.where(lane_row < high, key, 2 * FAR))
            key_columns.append(column(keys[-1]))
            code = places[m:m + 1] * 1024.0 + spots[:1] + n
            code_columns.append(column(jnp.where(kept, code, 0.0)))
            target_columns.append(column(jnp.where(kept, target, 1.0 * blocks)))
    ranks = []
    for mine in key_columns:
        before = [jnp.where(key < mine, 1.0, 0.0) for key in keys]
        ranks.append(jnp.sum(functools.reduce(jnp.add, before), axis=1, keepdims=True))

    def gathered(hits):
        return jnp.sum(functools.reduce(jnp.add, hits), axis=0, keepdims=True)

    def write(at, values):
        order[pl.ds(at, 1), :] = values.astype(jnp.int32)

    lines = -(-high * ma * mb // 128)
    for at in range(lines):
        spot = lane_row + at * 128.0
        for base, columns in ((0, code_columns), (lines, target_columns)):
            write(base + at, gathered([
                jnp.where(rank == spot, values, 0.0) for rank, values in zip(ranks, columns)
            ]))
    bound = (lane_row + 1.0) * (kb_cols * 1024.0)
    write(2 * lines, gathered([jnp.where(mine < bound, 1.0, 0.0) for mine in key_columns]))
    filled = gathered([jnp.where(mine == lane_row, 1.0, 0.0) for mine in target_columns])
    empty = jnp.where((filled < 0.5) & (lane_row < blocks), 1.0, 0.0)
    lane = lax.broadcasted_iota(jnp.int32, (128, 128), 1).astype(jnp.float32)
    line = lax.broadcasted_iota(jnp.int32, (128, 128), 0).astype(jnp.float32)
    wide = jnp.broadcast_to(empty, (128, 128))
    rank = jnp.sum(jnp.where(lane < line, wide, 0.0), axis=1, keepdims=True)
    flag = jnp.sum(jnp.where(lane == line, wide, 0.0), axis=1, keepdims=True)
    size = jnp.broadcast_to(jnp.sum(empty, axis=1, keepdims=True), (1, 128))
    listed = gathered([jnp.where(rank == lane, line * flag, 0.0)])
    write(2 * lines + 1, jnp.where(lane_row < size, listed, 1.0 * blocks))
    write(2 * lines + 2, size)


def gather_kernel(
    sizes, option, left, own_left, lead_down, lead_up, right, perm, left_meta, right_meta, tiles,
    left_all, right_all, order,
    own_right, packed_down, packed_up, side, spill_down, spill_up,
    up_send, up_recv, down_send, down_recv, spill_send, spill_recv,
    x_send, x_recv, own_send, own_recv, pass_send, pass_recv,
    left_sem, right_sem,
):
    n_row, n_col, sets = sizes[:3]
    row = lax.axis_index("row")
    col = lax.axis_index("col")
    n_chip = n_row // 2
    chip, core = row // 2, row % 2
    partner = chip * 2 + 1 - core
    slots = left.shape[0]
    main, spill, head, middle, limit = option

    barrier = pltpu.get_barrier_semaphore()
    for there, step in ((col > 0, -1), (col + 1 < n_col, 1)):
        @pl.when(there)
        def _():
            pl.semaphore_signal(
                barrier, inc=1, device_id={"col": col + step}, device_id_type=MESH
            )
    others = [partner] + [((chip + step) % n_chip) * 2 + core for step in range(1, n_chip)]
    for other in others:
        pl.semaphore_signal(barrier, inc=1, device_id={"row": other}, device_id_type=MESH)
    staged = pltpu.make_async_copy(right, own_right, right_sem)
    staged.start()
    kept = pltpu.make_async_copy(left, left_all.at[pl.ds(col * slots, slots)], left_sem)

    bounds = [LEAD + (main - LEAD) * at // MAIN_CUTS for at in range(MAIN_CUTS + 1)]
    cuts = [(low, high, "main") for low, high in zip(bounds, bounds[1:])]
    cuts.append((0, LEAD, "lead"))
    if head > main:
        cuts.append((main, head, "side"))
    if middle > head:
        cuts.append((head, middle, "rest"))
    bounds = [limit * at // RIGHT_CUTS for at in range(RIGHT_CUTS + 1)]
    right_cuts = [pl.ds(low, high - low) for low, high in zip(bounds, bounds[1:])]

    def left_copy(step, cut, up):
        low, high, kind = cuts[cut]
        panel = col - step if up else col + step
        span = pl.ds(panel * slots + low, high - low)
        target = side.at[span] if kind == "side" else left_all.at[span]
        source = (packed_up if up else packed_down).at[pl.ds(low, high - low)]
        if kind == "lead" and step == 1:
            source = lead_up if up else lead_down
        send, recv = (up_send, up_recv) if up else (down_send, down_recv)
        return pltpu.make_async_remote_copy(
            src_ref=source if step == int(kind == "lead") else target, dst_ref=target,
            send_sem=send.at[step, cut], recv_sem=recv.at[step, cut],
            device_id={"col": col + 1 if up else col - 1}, device_id_type=MESH,
        )

    def left_sends(step, cut, up):
        mid = 0 if cuts[cut][2] in ("main", "lead") else 1
        if up:
            return (col + 1 < n_col - mid) & (col - step >= 0)
        return (col - 1 >= mid) & (col + step < n_col)

    def left_receives(step, cut, up):
        mid = 0 if cuts[cut][2] in ("main", "lead") else 1
        if up:
            return (col - 1 - step >= 0) & (col < n_col - mid)
        return (col + 1 + step < n_col) & (col >= mid)

    def start_left(step, cut):
        for up in (True, False):
            pl.when(left_sends(step, cut, up))(left_copy(step, cut, up).start)

    def steps_of(kind):
        if kind == "lead":
            return range(1, n_col - 1)
        return range(n_col - 1 if kind == "main" else n_col - 2)

    def spill_copy(up):
        return pltpu.make_async_remote_copy(
            src_ref=spill_up if up else spill_down,
            dst_ref=left_all.at[pl.ds(n_col * slots, spill)],
            send_sem=spill_send.at[int(up)], recv_sem=spill_recv.at[int(up)],
            device_id={"col": n_col - 1 if up else 0}, device_id_type=MESH,
        )

    def across(step, cut):
        span = right_cuts[cut]
        other = ((chip + step) % n_chip) * 2 + core
        return pltpu.make_async_remote_copy(
            src_ref=right_all.at[:, row, span], dst_ref=right_all.at[:, row, span],
            send_sem=x_send.at[step - 1, cut], recv_sem=x_recv.at[step - 1, cut],
            device_id={"row": other}, device_id_type=MESH,
        )

    def passed(step, cut):
        span = right_cuts[cut]
        panel = ((chip + n_chip - step) % n_chip) * 2 + core
        return pltpu.make_async_remote_copy(
            src_ref=right_all.at[:, panel, span], dst_ref=right_all.at[:, panel, span],
            send_sem=pass_send.at[step - 1, cut], recv_sem=pass_recv.at[step - 1, cut],
            device_id={"row": partner}, device_id_type=MESH,
        )

    own = pltpu.make_async_remote_copy(
        src_ref=right_all.at[:, row, pl.ds(0, limit)],
        dst_ref=right_all.at[:, row, pl.ds(0, limit)],
        send_sem=own_send, recv_sem=own_recv,
        device_id={"row": partner}, device_id_type=MESH,
    )

    def pack_left(low, high):
        @pl.loop(low, high)
        def _(at):
            packed_down[at] = own_left[perm[0, at]]
            packed_up[at] = own_left[perm[1, at]]

    pack_left(*cuts[0][:2])
    pl.semaphore_wait(
        barrier, len(others) + jnp.where(col > 0, 1, 0) + jnp.where(col + 1 < n_col, 1, 0)
    )
    start_left(0, 0)
    pack_left(cuts[0][1], main)
    for cut in range(len(cuts)):
        if cuts[cut][2] == "main" and cut:
            start_left(0, cut)
        elif cuts[cut][2] == "lead" and n_col > 2:
            start_left(1, cut)

    staged.wait()
    for cut in range(RIGHT_CUTS):
        for which in range(sets):
            @pl.loop(bounds[cut], bounds[cut + 1])
            def _(at):
                right_all[which, row, at] = own_right[which, perm[4 + which, at]]

        for step in range(1, n_chip):
            across(step, cut).start()
    kept.start()
    pack_left(main, middle)
    own.start()
    if spill:
        @pl.loop(main, head)
        def _(at):
            side[col * slots + at] = packed_down[at]
            side[n_col * slots + at] = packed_up[at]

    def take_left(step, cut):
        for up in (True, False):
            pl.when(left_receives(step, cut, up))(left_copy(step, cut, up).wait_recv)
            if step + 1 < n_col - 1:
                pl.when(left_sends(step + 1, cut, up))(left_copy(step + 1, cut, up).start)

    def take_right(step, cut):
        across(step, cut).wait_recv()
        passed(step, cut).start()

    def take_order():
        for panel, there, found in (
            (col + 1, col + 1 < n_col, lead_down), (col - 1, col > 0, lead_up)
        ):
            @pl.when(there)
            def _():
                for at in range(LEAD):
                    left_all[panel * slots + at] = found[at]

        order_pairs(
            sizes, main, lax.axis_index("kpt"), col, tiles, left_meta, right_meta, order
        )

    def send_spill():
        for up in (False, True):
            target, line = (spill_up, 3) if up else (spill_down, 2)

            @pl.when(col == (n_col - 2 if up else 1))
            def _():
                @pl.loop(0, spill)
                def _(at):
                    target[at] = side[perm[line, at] + main]

                spill_copy(up).start()

    def take_sides():
        for step in range(1, n_col):
            for panel, there in (
                (col - step, (col - step >= 0) & (col < n_col - 1)),
                (col + step, (col + step < n_col) & (col > 0)),
            ):
                @pl.when(there)
                def _():
                    @pl.loop(main, head)
                    def _(at):
                        left_all[panel * slots + at] = side[panel * slots + at]

    mains, heads = (n_col - 2) * main - LEAD, (n_col - 2) * head - LEAD
    jobs = [(7, take_order)]
    if spill:
        jobs.append((heads + 0.02, send_spill))
    if head > main:
        jobs.append((heads + 0.03, take_sides))
    for cut, (low, high, kind) in enumerate(cuts):
        start = functools.partial(start_left, 0, cut)
        if kind == "side":
            jobs.append(((n_col - 3) * main - LEAD + 0.01, start))
        elif kind == "rest":
            jobs.append((mains + (n_col - 3) * (head - main) + 0.01, start))
        for step in steps_of(kind):
            when = step * main + high - LEAD
            if kind == "side":
                when = mains + (step + 1) * (high - low)
            elif kind == "rest":
                when = heads + (step + 1) * (high - low) + 0.04
            jobs.append((when, functools.partial(take_left, step, cut)))
    for step in range(1, n_chip):
        for cut in range(RIGHT_CUTS):
            when = ((step - 1) * RIGHT_CUTS + cut + 1) * limit * sets / RIGHT_CUTS + 2
            jobs.append((when, functools.partial(take_right, step, cut)))
    for _, job in sorted(jobs, key=lambda entry: entry[0]):
        job()

    kept.wait()
    if spill:
        for up in (False, True):
            pl.when(col == (n_col - 1 if up else 0))(spill_copy(up).wait_recv)
            pl.when(col == (n_col - 2 if up else 1))(spill_copy(up).wait_send)
    own.wait()
    for step in range(1, n_chip):
        for cut in range(RIGHT_CUTS):
            across(step, cut).wait_send()
            passed(step, cut).wait()
    for cut, entry in enumerate(cuts):
        for step in steps_of(entry[2]):
            for up in (True, False):
                pl.when(left_sends(step, cut, up))(left_copy(step, cut, up).wait_send)


def product_kernel(sizes, left, right, order, out, stage, partial, out_sem):
    n_row, n_col, sets, per, ma, mb, kb_cols = sizes
    blocks = GR * kb_cols
    lines = -(-n_col * per * ma * mb // 128)
    width = stage.shape[2]
    empty = jnp.zeros(stage.shape[1:], stage.dtype)

    @pl.loop(0, (order[2 * lines + 2, 0] + 3) // 4)
    def _(at):
        for lane in range(4):
            stage[order[2 * lines + 1, at * 4 + lane]] = empty

    def out_copy(line):
        span = pl.ds(line * kb_cols, kb_cols)
        return pltpu.make_async_copy(stage.at[span], out.at[span], out_sem.at[line])

    count = order[2 * lines, GR - 1]

    def group(at, carry):
        line, last = carry
        codes, targets, done = [], [], []
        for lane in range(GROUP):
            spot = at * GROUP + lane
            codes.append(order[spot // 128, spot % 128])
            targets.append(order[lines + spot // 128, spot % 128])
        for code in codes:
            block = left[code // 1024]
            wide = jnp.concatenate([block[:width], block[width:]], axis=1)
            other = right[code % 1024]
            real, imag = other[:width], other[width:]
            matrix = jnp.concatenate(
                [jnp.concatenate([real, imag], axis=1), jnp.concatenate([-imag, real], axis=1)],
                axis=0,
            )
            done.append(jnp.dot(wide, matrix, preferred_element_type=jnp.float32))
        held = partial[...]
        for target, product in zip(targets, done):
            held = jnp.where(target == last, held, 0.0) + product
            value = held.astype(stage.dtype)
            stage[target, :width] = value[:, :width]
            stage[target, width:] = value[:, width:]
            last = target
        partial[...] = held
        for _ in range(1 + GROUP // 12):
            ready = (line < GR) & (at * GROUP >= order[2 * lines, jnp.minimum(line, GR - 1)])
            pl.when(ready)(out_copy(jnp.minimum(line, GR - 1)).start)
            line = line + jnp.where(ready, 1, 0)
        return line, last

    partial[...] = jnp.zeros(partial.shape, partial.dtype)
    line, _ = lax.fori_loop(
        0, (count + GROUP - 1) // GROUP, group, (jnp.int32(0), jnp.int32(-1))
    )

    @pl.loop(line, GR)
    def _(line):
        out_copy(line).start()

    @pl.loop(0, GR)
    def _(line):
        out_copy(line).wait()


def body(
    n_kpt, n_row, n_col, left_blocks, left_rows, left_count, left_level,
    right_blocks, right_cols, right_count, right_level,
):
    _, per, ma, _, width, _ = left_blocks.shape
    sets, right_per, _, mb = right_blocks.shape[:4]
    assert right_per == per and sets * n_row == n_col and n_row % 2 == 0 and sets <= 2
    blocks = GR * (n_row * sets * per // n_col)
    assert n_col * per <= 128 and per * ma <= 128 and blocks <= 128 and ma * mb <= 8
    slots = per * ma
    left = left_blocks.reshape(slots, 2 * width, width)
    right = right_blocks.reshape(sets, per * mb, 2 * width, width)
    any_space = pl.BlockSpec(memory_space=pl.ANY)
    vmem = pl.BlockSpec(memory_space=pltpu.VMEM)
    smem = pl.BlockSpec(memory_space=pltpu.SMEM)
    dma = pltpu.SemaphoreType.DMA
    n_chip = n_row // 2
    total = n_kpt * n_row * n_col
    options = variants(slots, n_col, per * mb)
    sizes = (n_row, n_col, sets, per, ma, mb, n_row * sets * per // n_col)
    tile_rows = -(-(ma + sets) // 4) * 4
    meta_rows = -(-(3 * ma + 2 * mb * sets) // 8) * 8
    lines = -(-n_col * per * ma * mb // 128)
    order_rows = -(-(2 * lines + 3) // 8) * 8
    own_left, lead_down, lead_up, left_meta, right_meta, tiles, perm, choice = pl.pallas_call(
        functools.partial(plan_kernel, (n_kpt,) + sizes[:-1], options),
        out_shape=(
            pltpu.VMEM(left.shape, left.dtype),
            *[pltpu.VMEM((LEAD,) + left.shape[1:], left.dtype)] * 2,
            jax.ShapeDtypeStruct((n_col, meta_rows, 128), jnp.int32),
            jax.ShapeDtypeStruct((n_row, meta_rows, 128), jnp.int32),
            jax.ShapeDtypeStruct((total, tile_rows, 128), jnp.int32),
            jax.ShapeDtypeStruct((8, 128), jnp.int32),
            jax.ShapeDtypeStruct((1,), jnp.int32),
        ),
        in_specs=[any_space] + [vmem] * 6,
        out_specs=(vmem,) * 7 + (smem,),
        scratch_shapes=[
            pltpu.VMEM((LEAD,) + left.shape[1:], left.dtype),
            pltpu.VMEM((tile_rows, 128), jnp.int32),
            pltpu.VMEM((meta_rows, 128), jnp.int32),
            *[dma((total,))] * 2,
            *[dma((2,))] * 2,
            *[dma((n_col - 1,))] * 2,
            *[dma((n_row - 1,))] * 2,
            dma,
        ],
        compiler_params=pltpu.CompilerParams(collective_id=0, has_side_effects=True),
        name="plan",
    )(
        left, left_level[0].T, left_rows[0].T, left_count,
        right_level[:, :, 0].transpose(0, 2, 1), right_cols[:, :, 0].transpose(0, 2, 1),
        right_count.transpose(0, 2, 1),
    )

    kb_cols = sizes[-1]
    right_shape = (sets, n_row) + right.shape[1:]
    assert LEAD <= per
    most = (n_col + 1) * left.size + 2 * LEAD * left.size // slots + n_row * right.size + 24 * left.size // slots
    limit = VMEM_BYTES - most * left.dtype.itemsize

    def run(at, left, own_left, lead_down, lead_up, right, perm, left_meta, right_meta, tiles):
        cuts, spill = MAIN_CUTS + 3, max(options[at][1], 1)
        left_all, right_all, order = pl.pallas_call(
            functools.partial(gather_kernel, sizes, options[at]),
            out_shape=(
                pltpu.VMEM((n_col * slots + options[at][1],) + left.shape[1:], left.dtype),
                pltpu.VMEM(right_shape, right.dtype),
                jax.ShapeDtypeStruct((order_rows, 128), jnp.int32),
            ),
            in_specs=[any_space, vmem, vmem, vmem, any_space, smem, vmem, vmem, vmem],
            out_specs=(vmem, vmem, vmem),
            scratch_shapes=[
                pltpu.VMEM(right.shape, right.dtype),
                *[pltpu.VMEM(left.shape, left.dtype)] * 2,
                pltpu.VMEM(((n_col + 1) * slots,) + left.shape[1:], left.dtype),
                *[pltpu.VMEM((spill,) + left.shape[1:], left.dtype)] * 2,
                *[dma((n_col - 1, cuts))] * 4,
                *[dma((2,))] * 2,
                *[dma((n_chip - 1, RIGHT_CUTS))] * 2,
                *[dma] * 2,
                *[dma((n_chip - 1, RIGHT_CUTS))] * 2,
                *[dma] * 2,
            ],
            compiler_params=pltpu.CompilerParams(
                collective_id=1 + at, has_side_effects=True, vmem_limit_bytes=limit
            ),
            name=f"gather_panels_{at}",
        )(
            left, pltpu.with_memory_space_constraint(own_left, pltpu.VMEM),
            pltpu.with_memory_space_constraint(lead_down, pltpu.VMEM),
            pltpu.with_memory_space_constraint(lead_up, pltpu.VMEM),
            right, perm, left_meta, right_meta, tiles,
        )
        return pl.pallas_call(
            functools.partial(product_kernel, sizes),
            out_shape=jax.ShapeDtypeStruct((blocks, 2 * width, width), jnp.bfloat16),
            in_specs=[vmem, vmem, smem],
            out_specs=any_space,
            scratch_shapes=[
                pltpu.VMEM((blocks + 1, 2 * width, width), jnp.bfloat16),
                pltpu.VMEM((width, 2 * width), jnp.float32),
                dma((GR,)),
            ],
            compiler_params=pltpu.CompilerParams(vmem_limit_bytes=limit),
            name="pair_products",
        )(
            pltpu.with_memory_space_constraint(
                left_all, pltpu.VMEM
            ),
            pltpu.with_memory_space_constraint(
                right_all.reshape((-1,) + right.shape[2:]), pltpu.VMEM
            ),
            order,
        )

    out = lax.switch(
        choice[0], [functools.partial(run, at) for at in range(len(options))],
        left, own_left, lead_down, lead_up, right, perm, left_meta, right_meta, tiles,
    )
    return out.reshape(GR, kb_cols, 2, width, width)


def solution(mesh):
    in_specs = (
        P(("kpt", "row"), "col", None, None, None, None),
        P(("kpt", "row"), "col", None),
        P(("kpt", "row"), "col"),
        P(("kpt", "row"), "col", None),
        P("kpt", "row", "col", None, None, None, None),
        P("kpt", "row", "col", None),
        P("kpt", "row", "col"),
        P("kpt", "row", "col", None),
    )
    out_specs = P(("kpt", "row"), "col", None, None, None)
    return jax.shard_map(
        functools.partial(body, mesh.shape["kpt"], mesh.shape["row"], mesh.shape["col"]),
        mesh=mesh, in_specs=in_specs, out_specs=out_specs, check_vma=False,
    )
```
